32 devices in a mesh: shard: 4 (over z), width: 2 (over core), shift: 4 (over y, x).
Axes of the slice: x: 2, y: 2, z: 4, core: 2. Of those that a mesh axis runs over, the one named last changes fastest.
Arguments:
- w_query: bfloat16 [8192, 2048], P(('shift', 'shard'), 'width'), parts along dimension 0, may hold values from -0.125 to 0.125
- low_query: bfloat16 [8192, 16], P(('shift', 'shard')), parts along dimension 0, may hold values from -0.125 to 0.125
- high_query: bfloat16 [64, 2048], P('shift', 'width'), parts along dimension 0, may hold values from -1.5 to 1.5
- w_key: bfloat16 [8192, 512], P(('shift', 'shard'), 'width'), parts along dimension 0, may hold values from -0.125 to 0.125
- low_key: bfloat16 [8192, 16], P(('shift', 'shard')), parts along dimension 0, may hold values from -0.125 to 0.125
- high_key: bfloat16 [64, 512], P('shift', 'width'), parts along dimension 0, may hold values from -1.5 to 1.5
- w_value: bfloat16 [8192, 512], P(('shift', 'shard'), 'width'), parts along dimension 0, may hold values from -0.125 to 0.125
- low_value: bfloat16 [8192, 16], P(('shift', 'shard')), parts along dimension 0, may hold values from -0.125 to 0.125
- high_value: bfloat16 [64, 512], P('shift', 'width'), parts along dimension 0, may hold values from -1.5 to 1.5
- w_mixed: bfloat16 [8192, 2048], P(('shift', 'width'), 'shard'), parts along dimension 0, may hold values from -0.125 to 0.125
- low_mixed: bfloat16 [8192, 16], P(('shift', 'width')), parts along dimension 0, may hold values from -0.125 to 0.125
- high_mixed: bfloat16 [64, 2048], P('shift', 'shard'), parts along dimension 0, may hold values from -1.5 to 1.5
- norm_train: float32 [8192], P(('shift', 'shard', 'width')), parts along dimension 0, may hold values from 0.25 to 1.75
- norm_step: float32 [8192], P(('shift', 'shard', 'width')), parts along dimension 0, may hold values from -0.3 to 0.3
Outputs:
- final_query: bfloat16 [8192, 2048], P(('shift', 'width')), parts along dimension 0
- final_key: bfloat16 [2048, 2048], P(('shift', 'width')), parts along dimension 0
- final_value: bfloat16 [2048, 2048], P(('shift', 'width')), parts along dimension 0
- final_mixed: bfloat16 [8192, 2048], P('shift', 'width'), parts along dimension 0
- serve_norm: bfloat16 [8192], P('shift'), parts along dimension 0
The draws below stay inside these ranges and needn't reach their ends.
There are 4 independent parts, one for each index of `shift`. The reference program is written for one: setup_inputs(seed, part) draws one part's arguments, and reference() takes and returns one part's arrays. A program takes and returns all parts, laid end to end along the dimension named above; each array names one. Nothing has to cross between parts.
All inputs are finite; a program needn't handle non-finite values.
Results may differ from the reference program's by a relative error of at most 0.001.
Values may be sent and summed in bfloat16 or wider, within the bound.
A program may use at most 64 MiB of HBM per device.

```python
import jax
import jax.numpy as jnp

D_MODEL = 2048
Q_DIM = 2048
KV_DIM = 512
RANK = 16


def levels(key, shape, pieces, low, top_value):
    gain, own = 1.0, jax.random.fold_in(key, 6)
    for dim, shards_of in pieces:
        heights = jnp.exp(jax.random.uniform(jax.random.fold_in(own, dim), (shards_of,), jnp.float32, low / len(pieces), top_value / len(pieces)))
        gain = gain * jnp.repeat(heights, shape[dim] // shards_of).reshape([-1 if axis == dim else 1 for axis in range(len(shape))])
    return gain


def noise(own_key, shape, width, bound, shards=(), dtype=jnp.bfloat16):
    array = width * jax.random.normal(own_key, shape, jnp.float32)
    if shards:
        array = array * levels(own_key, shape, shards, -0.22, 0.18)
    return jnp.clip(array, -bound, bound).astype(dtype)


def setup_inputs(seed: int = 0, part: int = 0) -> dict:
    keys = jax.random.split(jax.random.key(seed), 15)
    own_keys = jax.random.split(jax.random.fold_in(keys[14], part), 15)
    w_query = noise(own_keys[0], (D_MODEL, Q_DIM), D_MODEL ** -0.5, 0.125, ((0, 4), (1, 2)))
    low_query = noise(own_keys[1], (D_MODEL, RANK), D_MODEL ** -0.5, 0.125, ((0, 4),))
    high_query = noise(own_keys[2], (RANK, Q_DIM), RANK ** -0.5, 1.5, ((1, 2),))
    w_key = noise(own_keys[3], (D_MODEL, KV_DIM), D_MODEL ** -0.5, 0.125, ((0, 4), (1, 2)))
    low_key = noise(own_keys[4], (D_MODEL, RANK), D_MODEL ** -0.5, 0.125, ((0, 4),))
    high_key = noise(own_keys[5], (RANK, KV_DIM), RANK ** -0.5, 1.5, ((1, 2),))
    w_value = noise(own_keys[6], (D_MODEL, KV_DIM), D_MODEL ** -0.5, 0.125, ((0, 4), (1, 2)))
    low_value = noise(own_keys[7], (D_MODEL, RANK), D_MODEL ** -0.5, 0.125, ((0, 4),))
    high_value = noise(own_keys[8], (RANK, KV_DIM), RANK ** -0.5, 1.5, ((1, 2),))
    w_mixed = noise(own_keys[9], (Q_DIM, D_MODEL), Q_DIM ** -0.5, 0.125, ((0, 2), (1, 4)))
    low_mixed = noise(own_keys[10], (Q_DIM, RANK), Q_DIM ** -0.5, 0.125, ((0, 2),))
    high_mixed = noise(own_keys[11], (RANK, D_MODEL), RANK ** -0.5, 1.5, ((1, 4),))
    norm_train = jnp.clip(1.0 + 0.15 * jax.random.normal(own_keys[12], (D_MODEL,), jnp.float32), 0.25, 1.75)
    norm_step = jnp.clip(jax.random.uniform(own_keys[13], (D_MODEL,), jnp.float32, -0.3, 0.3) * levels(own_keys[13], (D_MODEL,), ((0, 8),), -0.4, 0.0), -0.3, 0.3)
    return dict(w_query=w_query, low_query=low_query, high_query=high_query, w_key=w_key, low_key=low_key, high_key=high_key, w_value=w_value, low_value=low_value, high_value=high_value, w_mixed=w_mixed, low_mixed=low_mixed, high_mixed=high_mixed, norm_train=norm_train, norm_step=norm_step)


mix_rate = 0.5


def reference(w_query, low_query, high_query, w_key, low_key, high_key, w_value, low_value, high_value, w_mixed, low_mixed, high_mixed, norm_train, norm_step):
    result_query = w_query.astype(jnp.float32) + mix_rate * jnp.dot(low_query, high_query, preferred_element_type=jnp.float32)
    result_key = w_key.astype(jnp.float32) + mix_rate * jnp.dot(low_key, high_key, preferred_element_type=jnp.float32)
    result_value = w_value.astype(jnp.float32) + mix_rate * jnp.dot(low_value, high_value, preferred_element_type=jnp.float32)
    result_mixed = w_mixed.astype(jnp.float32) + mix_rate * jnp.dot(low_mixed, high_mixed, preferred_element_type=jnp.float32)
    final_query = result_query.T.astype(jnp.bfloat16)
    final_key = result_key.T.astype(jnp.bfloat16)
    final_value = result_value.T.astype(jnp.bfloat16)
    final_mixed = result_mixed.T.astype(jnp.bfloat16)
    serve_norm = (norm_train + norm_step).astype(jnp.bfloat16)
    return final_query, final_key, final_value, final_mixed, serve_norm
```

```python
import functools

import jax
import jax.numpy as jnp
from jax import lax
from jax.experimental import pallas as pl
from jax.experimental.pallas import tpu as pltpu
from jax.sharding import PartitionSpec as P

mix_rate = 0.5
MESH = pl.DeviceIdType.MESH
LANES = 128
COPY_ROWS = 256
LATE_STEPS = 8
LATE_CORE = 1
LATE_PIECES = 2


def plain(
    w_query,
    low_query,
    high_query,
    w_key,
    low_key,
    high_key,
    w_value,
    low_value,
    high_value,
    w_mixed,
    low_mixed,
    high_mixed,
    norm_train,
    norm_step,
):
    def merged(w, low, high):
        low_rank = jnp.dot(low, high, preferred_element_type=jnp.float32)
        return (w.astype(jnp.float32) + mix_rate * low_rank).astype(jnp.bfloat16)

    query = lax.all_gather(merged(w_query, low_query, high_query), "shard", axis=0, tiled=True)
    key = lax.all_gather(merged(w_key, low_key, high_key), "shard", axis=0, tiled=True)
    value = lax.all_gather(merged(w_value, low_value, high_value), "shard", axis=0, tiled=True)
    mixed = lax.all_gather(merged(w_mixed, low_mixed, high_mixed), "shard", axis=1, tiled=True)
    norm = lax.all_gather(
        (norm_train + norm_step).astype(jnp.bfloat16), ("shard", "width"), axis=0, tiled=True
    )
    return query.T, key.T, value.T, mixed.T, norm


def late_pieces(block):
    return min(LATE_PIECES, block // LANES)


def kernel(
    n,
    given,
    outs,
    norm_out,
    copied,
    load_sem,
    send_sem,
    back_sem,
    recv_sem,
    pair_sem,
):
    me = lax.axis_index("shard")
    core = lax.axis_index("width")
    has_left, has_right = me > 0, me < n - 1
    left, right = {"shard": me - 1}, {"shard": me + 1}
    partner = {"width": 1 - core}

    held, low_refs, high_refs = copied[0:12:3], copied[1:12:3], copied[2:12:3]
    width = held[0].shape[1]
    first, rest = pl.ds(0, LANES), pl.ds(LANES, width - LANES)
    loads = [pltpu.make_async_copy(given[0].at[:, first], held[0].at[:, first], load_sem.at[0])]
    loads += [
        pltpu.make_async_copy(given[i], copied[i], load_sem.at[i]) for i in range(1, len(given))
    ]
    others = []
    if width > LANES:
        others.append(
            pltpu.make_async_copy(
                given[0].at[:, rest], held[0].at[:, rest], load_sem.at[len(loads)]
            )
        )
    for load in loads[:3] + others + loads[3:]:
        load.start()

    barrier = pltpu.get_barrier_semaphore()
    pl.semaphore_signal(barrier, inc=1, device_id=partner, device_id_type=MESH)

    @pl.when(has_left)
    def _():
        pl.semaphore_signal(barrier, inc=1, device_id=left, device_id_type=MESH)

    @pl.when(has_right)
    def _():
        pl.semaphore_signal(barrier, inc=1, device_id=right, device_id_type=MESH)

    def piece(array, c, origin):
        if array == len(outs):
            return norm_out.at[origin]
        out, w = outs[array], held[array]
        if array < len(outs) - 1:
            block = w.shape[0]
            start = pl.multiple_of(origin * block, LANES)
            return out.at[pl.ds(pl.multiple_of(c * LANES, LANES), LANES), pl.ds(start, block)]
        start = pl.multiple_of(origin * w.shape[1] + c * LANES, LANES)
        return out.at[pl.ds(start, LANES)]

    counts = [w.shape[1] // LANES for w in held] + [1]
    kept = counts[len(outs) - 1] - late_pieces(held[-1].shape[1])
    moved = list(counts)
    moved[len(outs) - 1] = jnp.where(core == LATE_CORE, kept, counts[len(outs) - 1])
    firsts = [sum(counts[:i]) for i in range(len(counts))]

    def forward(array, c, origin):
        slot = firsts[array] + c
        return pltpu.make_async_remote_copy(
            src_ref=piece(array, c, origin),
            dst_ref=piece(array, c, origin),
            send_sem=send_sem.at[origin, slot],
            recv_sem=recv_sem.at[origin, slot],
            device_id=right,
            device_id_type=MESH,
        )

    def backward(array, c, origin, own=False):
        slot = firsts[array] + c
        return pltpu.make_async_remote_copy(
            src_ref=piece(array, c, origin),
            dst_ref=piece(array, c, origin),
            send_sem=back_sem.at[slot] if own else send_sem.at[origin, slot],
            recv_sem=recv_sem.at[origin, slot],
            device_id=left,
            device_id_type=MESH,
        )

    def compute(array, c):
        columns = pl.ds(pl.multiple_of(c * LANES, LANES), LANES)
        low_rank = lax.dot_general(
            high_refs[array][:, columns],
            low_refs[array][...],
            (((0,), (0,)), ((), ())),
            preferred_element_type=jnp.float32,
        )
        base = held[array][:, columns].astype(jnp.float32).T
        piece(array, c, me)[...] = (base + mix_rate * low_rank).astype(jnp.bfloat16)

    def send(array, c):
        ready = c < moved[array]

        @pl.when(jnp.logical_and(has_right, ready))
        def _():
            forward(array, c, me).start()

        @pl.when(jnp.logical_and(has_left, ready))
        def _():
            backward(array, c, me, own=True).start()

    for load in loads[:3]:
        load.wait()
    compute(0, 0)

    pl.semaphore_wait(barrier, 1 + has_left.astype(jnp.int32) + has_right.astype(jnp.int32))

    def exchange(side):
        return pltpu.make_async_remote_copy(
            src_ref=norm_out.at[me, side],
            dst_ref=norm_out.at[me, side],
            send_sem=pair_sem.at[0],
            recv_sem=pair_sem.at[1],
            device_id=partner,
            device_id_type=MESH,
        )

    for array in range(len(outs)):
        for load in loads[3 * array : 3 * array + 3] if array else others:
            load.wait()
        if array:
            compute(array, 0)
            send(array - 1, counts[array - 1] - 1)
        if array == 1:
            for load in loads[12:]:
                load.wait()
            norm_out[me, core] = copied[12][...] + copied[13][...]

        def step(c, carry, array=array):
            compute(array, c)
            send(array, c - 1)
            return carry

        lax.fori_loop(1, counts[array], step, 0)
    exchange(core).start()

    send(len(outs) - 1, counts[len(outs) - 1] - 1)

    exchange(core).wait_send()
    exchange(1 - core).wait_recv()
    send(len(outs), 0)

    for k in range(1, n):
        from_left, from_right = me - k, me + k
        for array in range(len(counts)):

            def relay(c, carry, array=array, from_left=from_left, from_right=from_right):
                @pl.when(from_left >= 0)
                def _():
                    forward(array, c, from_left).wait_recv()

                    @pl.when(has_right)
                    def _():
                        forward(array, c, from_left).start()

                @pl.when(from_right < n)
                def _():
                    backward(array, c, from_right).wait_recv()

                    @pl.when(has_left)
                    def _():
                        backward(array, c, from_right).start()

                return carry

            lax.fori_loop(0, moved[array], relay, 0)

    for array in range(len(counts)):

        def drain(c, carry, array=array):
            @pl.when(has_right)
            def _():
                forward(array, c, me).wait_send()

            @pl.when(has_left)
            def _():
                backward(array, c, me, own=True).wait_send()

            for k in range(1, n):

                @pl.when(jnp.logical_and(me - k >= 0, has_right))
                def _(k=k):
                    forward(array, c, me - k).wait_send()

                @pl.when(jnp.logical_and(me + k < n, has_left))
                def _(k=k):
                    backward(array, c, me + k).wait_send()

            return carry

        lax.fori_loop(0, moved[array], drain, 0)


def body(n, *refs):
    kernel(n, refs[:14], refs[14:18], refs[18], refs[19:33], *refs[33:])


def store(n, cores, *refs):
    gathered, norm_ref, outs, norm_out, flat, sem, mixed_sem = refs[:4], refs[4], refs[5:9], *refs[9:]
    me, core = lax.axis_index("shard"), lax.axis_index("width")
    copies = []
    for source, out in zip(gathered[:3], outs[:3]):
        for row in range(0, source.shape[0], COPY_ROWS):
            rows = pl.ds(row, min(COPY_ROWS, source.shape[0] - row))
            copies.append(
                pltpu.make_async_copy(source.at[rows], out.at[rows], sem.at[len(copies)])
            )

    block = gathered[3].shape[0] // n
    tail = late_pieces(block) * LANES

    def mixed(origin, row, size, part):
        rows = pl.ds(origin * block + row, size)
        return pltpu.make_async_copy(
            gathered[3].at[rows], outs[3].at[rows], mixed_sem.at[origin, part]
        )

    if block > tail:
        copies += [mixed(origin, 0, block - tail, 0) for origin in range(n)]

    def each_last(act):
        for origin in range(n):

            @pl.when(jnp.logical_or(core != LATE_CORE, me == origin))
            def _(origin=origin):
                act(mixed(origin, block - tail, tail, 1))

    for copy in copies:
        copy.start()
    each_last(lambda copy: copy.start())
    rows = norm_ref.shape[2]
    for origin in range(n):
        for side in range(cores):
            flat[pl.ds((origin * cores + side) * rows, rows)] = norm_ref[origin, side]
    norm_out[...] = flat[...].astype(norm_out.dtype)
    for copy in copies:
        copy.wait()
    each_last(lambda copy: copy.wait())


def late(n, mixed, after, out, send_sem, back_sem, recv_sem):
    me = lax.axis_index("shard")
    core = lax.axis_index("width")
    has_left, has_right = me > 0, me < n - 1
    left, right = {"shard": me - 1}, {"shard": me + 1}
    block = mixed.shape[0] // n
    tail = late_pieces(block) * LANES
    size = tail // LATE_STEPS

    def copy(origin, step, device, semaphore, own):
        rows = pl.ds(pl.multiple_of(step * size, size), size)
        first = pl.multiple_of(me * block + block - tail + step * size, size)
        return pltpu.make_async_remote_copy(
            src_ref=mixed.at[pl.ds(first, size)] if own else out.at[origin, rows],
            dst_ref=out.at[origin, rows],
            send_sem=semaphore,
            recv_sem=recv_sem.at[origin, step],
            device_id=device,
            device_id_type=MESH,
        )

    def forward(origin, step, own=False):
        return copy(origin, step, right, send_sem.at[origin, step], own)

    def backward(origin, step, own=False):
        semaphore = back_sem.at[step] if own else send_sem.at[origin, step]
        return copy(origin, step, left, semaphore, own)

    @pl.when(core == LATE_CORE)
    def _():
        barrier = pltpu.get_barrier_semaphore()

        @pl.when(has_left)
        def _():
            pl.semaphore_signal(barrier, inc=1, device_id=left, device_id_type=MESH)

        @pl.when(has_right)
        def _():
            pl.semaphore_signal(barrier, inc=1, device_id=right, device_id_type=MESH)

        pl.semaphore_wait(barrier, has_left.astype(jnp.int32) + has_right.astype(jnp.int32))

        for step in range(LATE_STEPS):

            @pl.when(has_right)
            def _(step=step):
                forward(me, step, own=True).start()

            @pl.when(has_left)
            def _(step=step):
                backward(me, step, own=True).start()

        for k in range(1, n):

            def relay(step, carry, k=k):
                @pl.when(me - k >= 0)
                def _():
                    forward(me - k, step).wait_recv()

                    @pl.when(has_right)
                    def _():
                        forward(me - k, step).start()

                @pl.when(me + k < n)
                def _():
                    backward(me + k, step).wait_recv()

                    @pl.when(has_left)
                    def _():
                        backward(me + k, step).start()

                return carry

            lax.fori_loop(0, LATE_STEPS, relay, 0)

        def drain(step, carry):
            @pl.when(has_right)
            def _():
                forward(me, step, own=True).wait_send()

            @pl.when(has_left)
            def _():
                backward(me, step, own=True).wait_send()

            for k in range(1, n):

                @pl.when(jnp.logical_and(me - k >= 0, has_right))
                def _(k=k):
                    forward(me - k, step).wait_send()

                @pl.when(jnp.logical_and(me + k < n, has_left))
                def _(k=k):
                    backward(me + k, step).wait_send()

            return carry

        lax.fori_loop(0, LATE_STEPS, drain, 0)


def store_late(n, pieces, given, out, sem):
    me, core = lax.axis_index("shard"), lax.axis_index("width")
    block = out.shape[0] // n
    tail = late_pieces(block) * LANES

    def each(act):
        for origin in range(n):

            @pl.when(jnp.logical_and(core == LATE_CORE, me != origin))
            def _(origin=origin):
                rows = pl.ds((origin + 1) * block - tail, tail)
                act(pltpu.make_async_copy(pieces.at[origin], out.at[rows], sem.at[origin]))

    each(lambda copy: copy.start())
    each(lambda copy: copy.wait())


def on_device(n, cores, *args):
    weights, (norm_train, norm_step) = list(args[:12]), args[12:]
    bases = weights[0::3]
    (size,) = norm_train.shape
    sizes = [size, *(size for w in bases for size in w.shape)]
    if cores != 2 or any(size % LANES for size in sizes):
        return plain(*args)
    rows = size // LANES
    shapes = [(w.shape[1], w.shape[0] * n) for w in bases[:3]]
    shapes.append((bases[3].shape[1] * n, bases[3].shape[0]))
    slots = sum(w.shape[1] // LANES for w in bases) + 1
    in_hbm = pl.BlockSpec(memory_space=pltpu.HBM)
    in_vmem = pl.BlockSpec(memory_space=pltpu.VMEM)
    weights[1::3] = [low.T for low in weights[1::3]]
    norms = [norm_train.reshape(rows, LANES), norm_step.reshape(rows, LANES)]
    given = [pltpu.with_memory_space_constraint(array, pltpu.HBM) for array in weights + norms]
    gathered = pl.pallas_call(
        functools.partial(body, n),
        out_shape=[pltpu.VMEM(shape, jnp.bfloat16) for shape in shapes]
        + [pltpu.VMEM((n, cores, rows, LANES), jnp.float32)],
        in_specs=[in_hbm] * 14,
        out_specs=[in_vmem] * 5,
        scratch_shapes=[pltpu.VMEM(array.shape, array.dtype) for array in given]
        + [
            pltpu.SemaphoreType.DMA((15,)),
            pltpu.SemaphoreType.DMA((n, slots)),
            pltpu.SemaphoreType.DMA((slots,)),
            pltpu.SemaphoreType.DMA((n, slots)),
            pltpu.SemaphoreType.DMA((2,)),
        ],
        compiler_params=pltpu.CompilerParams(
            collective_id=0, has_side_effects=True, vmem_limit_bytes=40 * 2**20
        ),
        name="merge_gather",
    )(*given)
    norm_rows = n * cores * rows
    *finals, norm = pl.pallas_call(
        functools.partial(store, n, cores),
        out_shape=[jax.ShapeDtypeStruct(shape, jnp.bfloat16) for shape in shapes]
        + [jax.ShapeDtypeStruct((norm_rows, LANES), jnp.bfloat16)],
        in_specs=[in_vmem] * 5,
        out_specs=[in_hbm] * 4 + [in_vmem],
        scratch_shapes=[
            pltpu.VMEM((norm_rows, LANES), jnp.float32),
            pltpu.SemaphoreType.DMA((sum(-(-shape[0] // COPY_ROWS) for shape in shapes[:3]),)),
            pltpu.SemaphoreType.DMA((n, 2)),
        ],
        compiler_params=pltpu.CompilerParams(vmem_limit_bytes=20 * 2**20),
        name="store",
    )(*gathered)
    columns = shapes[3][1]
    tail = late_pieces(bases[3].shape[1]) * LANES
    pieces = pl.pallas_call(
        functools.partial(late, n),
        out_shape=pltpu.VMEM((n, tail, columns), jnp.bfloat16),
        in_specs=[in_vmem, in_hbm],
        out_specs=in_vmem,
        scratch_shapes=[
            pltpu.SemaphoreType.DMA((n, LATE_STEPS)),
            pltpu.SemaphoreType.DMA((LATE_STEPS,)),
            pltpu.SemaphoreType.DMA((n, LATE_STEPS)),
        ],
        compiler_params=pltpu.CompilerParams(
            collective_id=1, has_side_effects=True, vmem_limit_bytes=20 * 2**20
        ),
        name="late",
    )(gathered[3], pltpu.with_memory_space_constraint(finals[3], pltpu.HBM))
    finals[3] = pl.pallas_call(
        functools.partial(store_late, n),
        out_shape=jax.ShapeDtypeStruct(shapes[3], jnp.bfloat16),
        in_specs=[in_vmem, in_hbm],
        out_specs=in_hbm,
        input_output_aliases={1: 0},
        scratch_shapes=[pltpu.SemaphoreType.DMA((n,))],
        compiler_params=pltpu.CompilerParams(vmem_limit_bytes=20 * 2**20),
        name="store_late",
    )(pieces, finals[3])
    return (*finals, norm.reshape(-1))


def solution(mesh):
    placed = (
        P(("shift", "shard"), "width"),
        P(("shift", "shard"), None),
        P("shift", "width"),
        P(("shift", "shard"), "width"),
        P(("shift", "shard"), None),
        P("shift", "width"),
        P(("shift", "shard"), "width"),
        P(("shift", "shard"), None),
        P("shift", "width"),
        P(("shift", "width"), "shard"),
        P(("shift", "width"), None),
        P("shift", "shard"),
        P(("shift", "shard", "width")),
        P(("shift", "shard", "width")),
    )
    return jax.shard_map(
        functools.partial(on_device, mesh.shape["shard"], mesh.shape["width"]),
        mesh=mesh,
        in_specs=placed,
        out_specs=(
            P(("shift", "width"), None),
            P(("shift", "width"), None),
            P(("shift", "width"), None),
            P("shift", "width"),
            P("shift"),
        ),
        check_vma=False,
    )
```

```python
import functools

import jax
import jax.numpy as jnp
from jax import lax
from jax.experimental import pallas as pl
from jax.experimental.pallas import tpu as pltpu
from jax.sharding import PartitionSpec as P

mix_rate = 0.5
MESH = pl.DeviceIdType.MESH
LANES = 128
COPY_ROWS = 256
LATE_STEPS = 3
LATE_CORE = 1
LATE_ROWS = 192
ROW_UNIT = 64
STORE_ROWS = 32


def plain(
    w_query,
    low_query,
    high_query,
    w_key,
    low_key,
    high_key,
    w_value,
    low_value,
    high_value,
    w_mixed,
    low_mixed,
    high_mixed,
    norm_train,
    norm_step,
):
    def merged(w, low, high):
        low_rank = jnp.dot(low, high, preferred_element_type=jnp.float32)
        return (w.astype(jnp.float32) + mix_rate * low_rank).astype(jnp.bfloat16)

    query = lax.all_gather(merged(w_query, low_query, high_query), "shard", axis=0, tiled=True)
    key = lax.all_gather(merged(w_key, low_key, high_key), "shard", axis=0, tiled=True)
    value = lax.all_gather(merged(w_value, low_value, high_value), "shard", axis=0, tiled=True)
    mixed = lax.all_gather(merged(w_mixed, low_mixed, high_mixed), "shard", axis=1, tiled=True)
    norm = lax.all_gather(
        (norm_train + norm_step).astype(jnp.bfloat16), ("shard", "width"), axis=0, tiled=True
    )
    return query.T, key.T, value.T, mixed.T, norm


def late_rows(block):
    return LATE_ROWS if block > LATE_ROWS else 0


def kernel(
    n,
    given,
    outs,
    norm_out,
    copied,
    load_sem,
    send_sem,
    back_sem,
    recv_sem,
    pair_sem,
    told_sem,
):
    me = lax.axis_index("shard")
    core = lax.axis_index("width")
    has_left, has_right = me > 0, me < n - 1
    left, right = {"shard": me - 1}, {"shard": me + 1}
    partner = {"width": 1 - core}
    leftward = core == LATE_CORE
    has_near = jnp.where(leftward, has_left.astype(jnp.int32), has_right.astype(jnp.int32))
    has_far = jnp.where(leftward, has_right.astype(jnp.int32), has_left.astype(jnp.int32))
    near = {"shard": jnp.where(leftward, me - 1, me + 1)}
    far = {"shard": jnp.where(leftward, me + 1, me - 1)}

    barrier = pltpu.get_barrier_semaphore()
    pl.semaphore_signal(barrier, inc=1, device_id=partner, device_id_type=MESH)

    @pl.when(has_far > 0)
    def _():
        pl.semaphore_signal(barrier, inc=1, device_id=far, device_id_type=MESH)

    held, low_refs, high_refs = copied[0:12:3], copied[1:12:3], copied[2:12:3]
    width = held[0].shape[1]
    first, rest = pl.ds(0, LANES), pl.ds(LANES, width - LANES)
    loads = [pltpu.make_async_copy(given[0].at[:, first], held[0].at[:, first], load_sem.at[0])]
    loads += [
        pltpu.make_async_copy(given[i], copied[i], load_sem.at[i]) for i in range(1, len(given))
    ]
    others = []
    if width > LANES:
        others.append(
            pltpu.make_async_copy(
                given[0].at[:, rest], held[0].at[:, rest], load_sem.at[len(loads)]
            )
        )
    for load in loads[:3] + others:
        load.start()

    last = len(outs) - 1
    block = held[last].shape[1]
    tail = late_rows(block)
    groups = [(array, 0, w.shape[1]) for array, w in enumerate(held[:last])]
    groups.append((last, 0, block - tail))
    if tail:
        groups.append((last, block - tail, tail))
    groups.append((len(outs), 0, 0))
    late_group = len(groups) - 2 if tail else -1

    def part(array, row, rows, origin, columns=None):
        if array == len(outs):
            return norm_out.at[origin]
        out, w = outs[array], held[array]
        if array < last:
            size = w.shape[0]
            begin, size = columns or (0, size)
            begin = pl.multiple_of(origin * w.shape[0] + begin, LANES)
            return out.at[pl.ds(pl.multiple_of(row, LANES), rows), pl.ds(begin, size)]
        begin = pl.multiple_of(origin * block + row, ROW_UNIT)
        return out.at[pl.ds(begin, rows)]

    def copy(ref, device, semaphore, origin, group):
        return pltpu.make_async_remote_copy(
            src_ref=ref,
            dst_ref=ref,
            send_sem=semaphore,
            recv_sem=recv_sem.at[origin, group],
            device_id=device,
            device_id_type=MESH,
        )

    def forward(group, origin):
        ref = part(*groups[group], origin)
        return copy(ref, right, send_sem.at[origin, group], origin, group)

    def backward(group, origin, own=False):
        ref = part(*groups[group], origin)
        semaphore = back_sem.at[group] if own else send_sem.at[origin, group]
        return copy(ref, left, semaphore, origin, group)

    def compute(array, c, columns=None):
        rows = pl.ds(pl.multiple_of(c * LANES, LANES), LANES)
        taken = pl.ds(*(columns or (0, held[array].shape[0])))
        low_rank = lax.dot_general(
            high_refs[array][:, rows],
            low_refs[array][:, taken],
            (((0,), (0,)), ((), ())),
            preferred_element_type=jnp.float32,
        )
        base = held[array][taken, rows].T.astype(jnp.float32)
        part(array, c * LANES, LANES, me, columns)[...] = (base + mix_rate * low_rank).astype(
            jnp.bfloat16
        )

    def send_near(ref, group):
        @pl.when(jnp.logical_and(leftward, has_left))
        def _():
            copy(ref, left, back_sem.at[group], me, group).start()

        @pl.when(jnp.logical_and(jnp.logical_not(leftward), has_right))
        def _():
            copy(ref, right, send_sem.at[me, group], me, group).start()

    def send_far(ref, group):
        @pl.when(jnp.logical_and(jnp.logical_not(leftward), has_left))
        def _():
            copy(ref, left, back_sem.at[group], me, group).start()

        @pl.when(jnp.logical_and(leftward, has_right))
        def _():
            copy(ref, right, send_sem.at[me, group], me, group).start()

    def send_both(ref, group):
        @pl.when(has_left)
        def _():
            copy(ref, left, back_sem.at[group], me, group).start()

        @pl.when(has_right)
        def _():
            copy(ref, right, send_sem.at[me, group], me, group).start()

    def finish(array):
        if array == 0:
            row = held[0].shape[1] - LANES
            send_near(part(0, row, LANES, me), 0)

            @pl.when(has_far > 0)
            def _():
                pl.semaphore_wait(told_sem, 1)

            send_far(part(*groups[0], me), 0)
        else:
            send_both(part(*groups[array], me), array)

    for load in loads[:3]:
        load.wait()
    for load in loads[3:]:
        load.start()
    half = held[0].shape[0] // 2
    halves = [(0, half), (half, half)] if half % LANES == 0 else [(0, 2 * half)]
    for columns in halves:
        compute(0, 0, columns)

    pl.semaphore_wait(barrier, 1 + has_near)

    @pl.when(has_near > 0)
    def _():
        pl.semaphore_signal(told_sem, inc=1, device_id=near, device_id_type=MESH)

    for columns in halves[:-1]:
        send_near(part(0, 0, LANES, me, columns), 0)

    def exchange(side):
        return pltpu.make_async_remote_copy(
            src_ref=norm_out.at[me, side],
            dst_ref=norm_out.at[me, side],
            send_sem=pair_sem.at[0],
            recv_sem=pair_sem.at[1],
            device_id=partner,
            device_id_type=MESH,
        )

    for array in range(len(outs)):
        for load in loads[3 * array : 3 * array + 3] if array else others:
            load.wait()
        count = held[array].shape[1] // LANES
        if array:
            compute(array, 0)
            finish(array - 1)
        if array == 1:
            for load in loads[12:]:
                load.wait()
            norm_out[me, core] = copied[12][...] + copied[13][...]
        if array == 0 and count > 1:
            compute(0, 1)
            send_near(part(0, 0, LANES, me, halves[-1]), 0)

        def step(c, carry, array=array):
            compute(array, c)
            if array == 0:
                send_near(part(0, (c - 1) * LANES, LANES, me), 0)
            return carry

        lax.fori_loop(1 if array else 2, count, step, 0)
    exchange(core).start()
    if tail >= LANES:
        finish(last)
    exchange(core).wait_send()
    exchange(1 - core).wait_recv()
    if tail < LANES:
        finish(last)
    if tail:

        @pl.when(core != LATE_CORE)
        def _():
            send_both(part(*groups[late_group], me), late_group)

    send_both(part(*groups[-1], me), len(groups) - 1)

    def each_group(act):
        for group in range(len(groups)):
            if group == late_group:

                @pl.when(core != LATE_CORE)
                def _(group=group):
                    act(group)
            else:
                act(group)

    def relay(k, carry):
        from_left, from_right = me - k, me + k

        def pass_on(group):
            @pl.when(from_left >= 0)
            def _():
                forward(group, from_left).wait_recv()

                @pl.when(has_right)
                def _():
                    forward(group, from_left).start()

            @pl.when(from_right < n)
            def _():
                backward(group, from_right).wait_recv()

                @pl.when(has_left)
                def _():
                    backward(group, from_right).start()

        each_group(pass_on)
        return carry

    lax.fori_loop(1, n, relay, 0)

    def own_sent(group):
        @pl.when(has_right)
        def _():
            forward(group, me).wait_send()

        @pl.when(has_left)
        def _():
            backward(group, me, own=True).wait_send()

    each_group(own_sent)

    def drain(k, carry):
        def sent(group):
            @pl.when(jnp.logical_and(me - k >= 0, has_right))
            def _():
                forward(group, me - k).wait_send()

            @pl.when(jnp.logical_and(me + k < n, has_left))
            def _():
                backward(group, me + k).wait_send()

        each_group(sent)
        return carry

    lax.fori_loop(1, n, drain, 0)


def body(n, *refs):
    kernel(n, refs[:14], refs[14:18], refs[18], refs[19:33], *refs[33:])


def store(n, cores, *refs):
    gathered, norm_ref, outs, norm_out, flat, sem, mixed_sem = refs[:4], refs[4], refs[5:9], *refs[9:]
    me, core = lax.axis_index("shard"), lax.axis_index("width")
    copies = []
    for source, out in zip(gathered[:3], outs[:3]):
        for row in range(0, source.shape[0], COPY_ROWS):
            rows = pl.ds(row, min(COPY_ROWS, source.shape[0] - row))
            copies.append(
                pltpu.make_async_copy(source.at[rows], out.at[rows], sem.at[len(copies)])
            )

    block = gathered[3].shape[0] // n
    tail = late_rows(block)

    def mixed(origin, row, size, part):
        rows = pl.ds(origin * block + row, size)
        return pltpu.make_async_copy(
            gathered[3].at[rows], outs[3].at[rows], mixed_sem.at[origin, part]
        )

    copies += [mixed(origin, 0, block - tail, 0) for origin in range(n)]

    def each_last(act):
        for origin in range(n if tail else 0):

            @pl.when(jnp.logical_or(core != LATE_CORE, me == origin))
            def _(origin=origin):
                act(mixed(origin, block - tail, tail, 1))

    for copy in copies:
        copy.start()
    each_last(lambda copy: copy.start())
    rows = norm_ref.shape[2]
    for origin in range(n):
        for side in range(cores):
            flat[pl.ds((origin * cores + side) * rows, rows)] = norm_ref[origin, side]
    norm_out[...] = flat[...].astype(norm_out.dtype)
    for copy in copies:
        copy.wait()
    each_last(lambda copy: copy.wait())


def late(n, mixed, after, out, send_sem, recv_sem, told_sem):
    me = lax.axis_index("shard")
    core = lax.axis_index("width")
    has_left, has_right = me > 0, me < n - 1
    left, right = {"shard": me - 1}, {"shard": me + 1}
    block = mixed.shape[0] // n
    tail = late_rows(block)
    size = tail // LATE_STEPS

    def copy(origin, begin, rows, step, device, semaphore, own):
        first = pl.multiple_of(me * block + block - tail + begin, 16)
        dst = out.at[origin, pl.ds(pl.multiple_of(begin, 16), rows)]
        return pltpu.make_async_remote_copy(
            src_ref=mixed.at[pl.ds(first, rows)] if own else dst,
            dst_ref=dst,
            send_sem=send_sem.at[semaphore],
            recv_sem=recv_sem.at[origin, step],
            device_id=device,
            device_id_type=MESH,
        )

    def forward(origin, step, own=False):
        return copy(origin, step * size, size, step, right, origin, own)

    def backward(origin, step, own=False):
        return copy(origin, step * size, size, step, left, n if own else origin, own)

    def sent(origin, semaphore):
        copy(origin, 0, tail, 0, right, semaphore, True).wait_send()

    @pl.when(core == LATE_CORE)
    def _():
        barrier = pltpu.get_barrier_semaphore()
        half = n // 2
        to_left, middle = me < half, me == half

        def signal(semaphore, condition, device):
            @pl.when(condition)
            def _():
                pl.semaphore_signal(semaphore, inc=1, device_id=device, device_id_type=MESH)

        signal(barrier, jnp.logical_and(has_right, me < half), right)
        signal(barrier, me > half, left)
        known = jnp.where(to_left, has_left, has_right).astype(jnp.int32)
        known += jnp.logical_and(middle, has_left).astype(jnp.int32)

        @pl.when(known > 0)
        def _():
            pl.semaphore_wait(barrier, known)

        def own(direction, condition):
            for step in range(LATE_STEPS):

                @pl.when(condition)
                def _(step=step):
                    direction(me, step, own=True).start()

        own(backward, jnp.logical_and(to_left, has_left))
        own(forward, jnp.logical_and(jnp.logical_not(to_left), has_right))
        signal(told_sem, jnp.logical_and(has_left, me <= half), left)
        signal(told_sem, jnp.logical_and(has_right, me >= half), right)
        unknown = jnp.logical_or(jnp.logical_and(to_left, has_right), me > half)

        @pl.when(unknown)
        def _():
            pl.semaphore_wait(told_sem, 1)
        own(backward, jnp.logical_and(jnp.logical_not(to_left), has_left))
        own(forward, jnp.logical_and(to_left, has_right))

        def relay(k, carry):
            for step in range(LATE_STEPS):

                @pl.when(me - k >= 0)
                def _(step=step):
                    forward(me - k, step).wait_recv()

                    @pl.when(has_right)
                    def _():
                        forward(me - k, step).start()

                @pl.when(me + k < n)
                def _(step=step):
                    backward(me + k, step).wait_recv()

                    @pl.when(has_left)
                    def _():
                        backward(me + k, step).start()

            return carry

        lax.fori_loop(1, n, relay, 0)

        @pl.when(has_right)
        def _():
            sent(me, me)

        @pl.when(has_left)
        def _():
            sent(me, n)

        def drain(k, carry):
            @pl.when(jnp.logical_and(me - k >= 0, has_right))
            def _():
                sent(me - k, me - k)

            @pl.when(jnp.logical_and(me + k < n, has_left))
            def _():
                sent(me + k, me + k)

            return carry

        lax.fori_loop(1, n, drain, 0)


def store_late(n, pieces, given, out, sem):
    me, core = lax.axis_index("shard"), lax.axis_index("width")
    block = out.shape[0] // n
    tail = late_rows(block)

    def each(act):
        for origin in range(n):

            @pl.when(jnp.logical_and(core == LATE_CORE, me != origin))
            def _(origin=origin):
                act(origin)

    def begin(origin):
        for row in range(0, tail, STORE_ROWS):
            rows = pl.ds((origin + 1) * block - tail + row, STORE_ROWS)
            source = pieces.at[origin, pl.ds(row, STORE_ROWS)]
            pltpu.make_async_copy(source, out.at[rows], sem.at[origin]).start()

    def end(origin):
        rows = pl.ds((origin + 1) * block - tail, tail)
        pltpu.make_async_copy(pieces.at[origin], out.at[rows], sem.at[origin]).wait()

    each(begin)
    each(end)


def on_device(n, cores, *args):
    weights, (norm_train, norm_step) = list(args[:12]), args[12:]
    bases = weights[0::3]
    (size,) = norm_train.shape
    sizes = [size, *(size for w in bases for size in w.shape)]
    if cores != 2 or any(size % LANES for size in sizes):
        return plain(*args)
    rows = size // LANES
    shapes = [(w.shape[1], w.shape[0] * n) for w in bases[:3]]
    shapes.append((bases[3].shape[1] * n, bases[3].shape[0]))
    in_hbm = pl.BlockSpec(memory_space=pltpu.HBM)
    in_vmem = pl.BlockSpec(memory_space=pltpu.VMEM)
    tail = late_rows(bases[3].shape[1])
    groups = len(bases) + (2 if tail else 1)
    weights[1::3] = [low.T for low in weights[1::3]]
    norms = [norm_train.reshape(rows, LANES), norm_step.reshape(rows, LANES)]
    given = [pltpu.with_memory_space_constraint(array, pltpu.HBM) for array in weights + norms]
    gathered = pl.pallas_call(
        functools.partial(body, n),
        out_shape=[pltpu.VMEM(shape, jnp.bfloat16) for shape in shapes]
        + [pltpu.VMEM((n, cores, rows, LANES), jnp.float32)],
        in_specs=[in_hbm] * 14,
        out_specs=[in_vmem] * 5,
        scratch_shapes=[pltpu.VMEM(array.shape, array.dtype) for array in given]
        + [
            pltpu.SemaphoreType.DMA((15,)),
            pltpu.SemaphoreType.DMA((n, groups)),
            pltpu.SemaphoreType.DMA((groups,)),
            pltpu.SemaphoreType.DMA((n, groups)),
            pltpu.SemaphoreType.DMA((2,)),
            pltpu.SemaphoreType.REGULAR,
        ],
        compiler_params=pltpu.CompilerParams(
            collective_id=0, has_side_effects=True, vmem_limit_bytes=40 * 2**20
        ),
        name="merge_gather",
    )(*given)
    norm_rows = n * cores * rows
    *finals, norm = pl.pallas_call(
        functools.partial(store, n, cores),
        out_shape=[jax.ShapeDtypeStruct(shape, jnp.bfloat16) for shape in shapes]
        + [jax.ShapeDtypeStruct((norm_rows, LANES), jnp.bfloat16)],
        in_specs=[in_vmem] * 5,
        out_specs=[in_hbm] * 4 + [in_vmem],
        scratch_shapes=[
            pltpu.VMEM((norm_rows, LANES), jnp.float32),
            pltpu.SemaphoreType.DMA((sum(-(-shape[0] // COPY_ROWS) for shape in shapes[:3]),)),
            pltpu.SemaphoreType.DMA((n, 2)),
        ],
        compiler_params=pltpu.CompilerParams(vmem_limit_bytes=20 * 2**20),
        name="store",
    )(*gathered)
    norm = norm.reshape(-1)
    if not tail:
        return (*finals, norm)
    columns = shapes[3][1]
    pieces = pl.pallas_call(
        functools.partial(late, n),
        out_shape=pltpu.VMEM((n, tail, columns), jnp.bfloat16),
        in_specs=[in_vmem, in_hbm],
        out_specs=in_vmem,
        scratch_shapes=[
            pltpu.SemaphoreType.DMA((n + 1,)),
            pltpu.SemaphoreType.DMA((n, LATE_STEPS)),
            pltpu.SemaphoreType.REGULAR,
        ],
        compiler_params=pltpu.CompilerParams(
            collective_id=1, has_side_effects=True, vmem_limit_bytes=20 * 2**20
        ),
        name="late",
    )(gathered[3], pltpu.with_memory_space_constraint(finals[3], pltpu.HBM))
    finals[3] = pl.pallas_call(
        functools.partial(store_late, n),
        out_shape=jax.ShapeDtypeStruct(shapes[3], jnp.bfloat16),
        in_specs=[in_vmem, in_hbm],
        out_specs=in_hbm,
        input_output_aliases={1: 0},
        scratch_shapes=[pltpu.SemaphoreType.DMA((n,))],
        compiler_params=pltpu.CompilerParams(vmem_limit_bytes=20 * 2**20),
        name="store_late",
    )(pieces, finals[3])
    return (*finals, norm)


def solution(mesh):
    placed = (
        P(("shift", "shard"), "width"),
        P(("shift", "shard"), None),
        P("shift", "width"),
        P(("shift", "shard"), "width"),
        P(("shift", "shard"), None),
        P("shift", "width"),
        P(("shift", "shard"), "width"),
        P(("shift", "shard"), None),
        P("shift", "width"),
        P(("shift", "width"), "shard"),
        P(("shift", "width"), None),
        P("shift", "shard"),
        P(("shift", "shard", "width")),
        P(("shift", "shard", "width")),
    )
    return jax.shard_map(
        functools.partial(on_device, mesh.shape["shard"], mesh.shape["width"]),
        mesh=mesh,
        in_specs=placed,
        out_specs=(
            P(("shift", "width"), None),
            P(("shift", "width"), None),
            P(("shift", "width"), None),
            P("shift", "width"),
            P("shift"),
        ),
        check_vma=False,
    )
```

```python
import functools

import jax
import jax.numpy as jnp
from jax import lax
from jax.experimental import pallas as pl
from jax.experimental.pallas import tpu as pltpu
from jax.sharding import PartitionSpec as P

mix_rate = 0.5
MESH = pl.DeviceIdType.MESH
LANES = 128
COPY_ROWS = 256
LATE_STEPS = 3
LATE_CORE = 1
LATE_ROWS = 192
ROW_UNIT = 64
EARLY_PIECES = 4
STORE_ROWS = 32


def plain(
    w_query,
    low_query,
    high_query,
    w_key,
    low_key,
    high_key,
    w_value,
    low_value,
    high_value,
    w_mixed,
    low_mixed,
    high_mixed,
    norm_train,
    norm_step,
):
    def merged(w, low, high):
        low_rank = jnp.dot(low, high, preferred_element_type=jnp.float32)
        return (w.astype(jnp.float32) + mix_rate * low_rank).astype(jnp.bfloat16)

    query = lax.all_gather(merged(w_query, low_query, high_query), "shard", axis=0, tiled=True)
    key = lax.all_gather(merged(w_key, low_key, high_key), "shard", axis=0, tiled=True)
    value = lax.all_gather(merged(w_value, low_value, high_value), "shard", axis=0, tiled=True)
    mixed = lax.all_gather(merged(w_mixed, low_mixed, high_mixed), "shard", axis=1, tiled=True)
    norm = lax.all_gather(
        (norm_train + norm_step).astype(jnp.bfloat16), ("shard", "width"), axis=0, tiled=True
    )
    return query.T, key.T, value.T, mixed.T, norm


def late_rows(block):
    return LATE_ROWS if block > LATE_ROWS else 0


def kernel(
    n,
    given,
    outs,
    norm_out,
    copied,
    load_sem,
    send_sem,
    back_sem,
    recv_sem,
    pair_sem,
    told_sem,
):
    me = lax.axis_index("shard")
    core = lax.axis_index("width")
    has_left, has_right = me > 0, me < n - 1
    left, right = {"shard": me - 1}, {"shard": me + 1}
    partner = {"width": 1 - core}
    leftward = core == LATE_CORE
    has_near = jnp.where(leftward, has_left.astype(jnp.int32), has_right.astype(jnp.int32))
    has_far = jnp.where(leftward, has_right.astype(jnp.int32), has_left.astype(jnp.int32))
    near = {"shard": jnp.where(leftward, me - 1, me + 1)}
    far = {"shard": jnp.where(leftward, me + 1, me - 1)}

    held, low_refs, high_refs = copied[0:12:3], copied[1:12:3], copied[2:12:3]
    depth, width = held[0].shape
    first, rest = pl.ds(0, LANES), pl.ds(LANES, width - LANES)
    bands = [pl.ds(row, LANES) for row in range(0, depth, LANES)]
    loads = []

    def load(source, target):
        loads.append(pltpu.make_async_copy(source, target, load_sem.at[len(loads)]))
        return loads[-1]

    opening = [load(given[1], copied[1]), load(given[2].at[:, first], copied[2].at[:, first])]
    opening += [load(given[0].at[rows, first], held[0].at[rows, first]) for rows in bands]
    others = []
    if width > LANES:
        others = [load(given[i].at[:, rest], copied[i].at[:, rest]) for i in (2, 0)]
    rest_of = [others] + [
        [load(given[i], copied[i]) for i in range(array, array + 3)] for array in (3, 6, 9)
    ]
    norm_loads = [load(given[i], copied[i]) for i in (12, 13)]
    for one in opening:
        one.start()

    barrier = pltpu.get_barrier_semaphore()
    pl.semaphore_signal(barrier, inc=1, device_id=partner, device_id_type=MESH)

    @pl.when(has_far > 0)
    def _():
        pl.semaphore_signal(barrier, inc=1, device_id=far, device_id_type=MESH)

    for one in loads[len(opening) :]:
        one.start()

    last = len(outs) - 1
    block = held[last].shape[1]
    tail = late_rows(block)
    groups = [(array, 0, w.shape[1]) for array, w in enumerate(held[:last])]
    groups.append((last, 0, block - tail))
    if tail:
        groups.append((last, block - tail, tail))
    groups.append((len(outs), 0, 0))
    late_group = len(groups) - 2 if tail else -1

    def part(array, row, rows, origin):
        if array == len(outs):
            return norm_out.at[origin]
        out, w = outs[array], held[array]
        if array < last:
            size = w.shape[0]
            begin = pl.multiple_of(origin * size, LANES)
            return out.at[pl.ds(pl.multiple_of(row, LANES), rows), pl.ds(begin, size)]
        begin = pl.multiple_of(origin * block + row, ROW_UNIT)
        return out.at[pl.ds(begin, rows)]

    def copy(ref, device, semaphore, origin, group):
        return pltpu.make_async_remote_copy(
            src_ref=ref,
            dst_ref=ref,
            send_sem=semaphore,
            recv_sem=recv_sem.at[origin, group],
            device_id=device,
            device_id_type=MESH,
        )

    def forward(group, origin):
        ref = part(*groups[group], origin)
        return copy(ref, right, send_sem.at[origin, group], origin, group)

    def backward(group, origin, own=False):
        ref = part(*groups[group], origin)
        semaphore = back_sem.at[group] if own else send_sem.at[origin, group]
        return copy(ref, left, semaphore, origin, group)

    def compute(array, c):
        rows = pl.ds(pl.multiple_of(c * LANES, LANES), LANES)
        low_rank = lax.dot_general(
            high_refs[array][:, rows],
            low_refs[array][...],
            (((0,), (0,)), ((), ())),
            preferred_element_type=jnp.float32,
        )
        base = held[array][:, rows].T.astype(jnp.float32)
        part(array, c * LANES, LANES, me)[...] = (base + mix_rate * low_rank).astype(
            jnp.bfloat16
        )

    def send_near(ref, group):
        @pl.when(jnp.logical_and(leftward, has_left))
        def _():
            copy(ref, left, back_sem.at[group], me, group).start()

        @pl.when(jnp.logical_and(jnp.logical_not(leftward), has_right))
        def _():
            copy(ref, right, send_sem.at[me, group], me, group).start()

    def send_far(ref, group):
        @pl.when(jnp.logical_and(jnp.logical_not(leftward), has_left))
        def _():
            copy(ref, left, back_sem.at[group], me, group).start()

        @pl.when(jnp.logical_and(leftward, has_right))
        def _():
            copy(ref, right, send_sem.at[me, group], me, group).start()

    def send_both(ref, group):
        @pl.when(has_left)
        def _():
            copy(ref, left, back_sem.at[group], me, group).start()

        @pl.when(has_right)
        def _():
            copy(ref, right, send_sem.at[me, group], me, group).start()

    def open_far(rows):
        @pl.when(has_far > 0)
        def _():
            pl.semaphore_wait(told_sem, 1)

        send_far(part(0, 0, rows, me), 0)

    def finish(array):
        if array == 0:
            rows = held[0].shape[1]
            if rows > LANES:
                send_near(part(0, rows - LANES, LANES, me), 0)
            if early:
                send_far(part(0, early, rows - early, me), 0)
            else:
                open_far(rows)
        else:
            send_both(part(*groups[array], me), array)

    for one in opening:
        one.wait()
    compute(0, 0)

    pl.semaphore_wait(barrier, 1 + has_near)

    @pl.when(has_near > 0)
    def _():
        pl.semaphore_signal(told_sem, inc=1, device_id=near, device_id_type=MESH)

    send_near(part(0, 0, LANES, me), 0)

    def exchange(side):
        return pltpu.make_async_remote_copy(
            src_ref=norm_out.at[me, side],
            dst_ref=norm_out.at[me, side],
            send_sem=pair_sem.at[0],
            recv_sem=pair_sem.at[1],
            device_id=partner,
            device_id_type=MESH,
        )

    early = (EARLY_PIECES - 1) * LANES if width > EARLY_PIECES * LANES else 0

    for array in range(len(outs)):
        for one in rest_of[array]:
            one.wait()
        count = held[array].shape[1] // LANES
        if array:
            compute(array, 0)
            finish(array - 1)
        if array == 1:
            for one in norm_loads:
                one.wait()
            norm_out[me, core] = copied[12][...] + copied[13][...]
        begin = 1
        if array == 0 and count > 1:
            compute(0, 1)
            begin = 2

        def step(c, carry, array=array):
            compute(array, c)
            if array == 0:
                send_near(part(0, (c - 1) * LANES, LANES, me), 0)
            return carry

        if array == 0 and early:
            lax.fori_loop(begin, EARLY_PIECES, step, 0)
            open_far(early)
            begin = EARLY_PIECES
        lax.fori_loop(begin, count, step, 0)
    exchange(core).start()
    if tail >= LANES:
        finish(last)
    exchange(core).wait_send()
    exchange(1 - core).wait_recv()
    if tail < LANES:
        finish(last)
    if tail:

        @pl.when(core != LATE_CORE)
        def _():
            send_both(part(*groups[late_group], me), late_group)

    send_both(part(*groups[-1], me), len(groups) - 1)

    def each_group(act):
        for group in range(len(groups)):
            if group == late_group:

                @pl.when(core != LATE_CORE)
                def _(group=group):
                    act(group)
            else:
                act(group)

    def relay(k, carry):
        from_left, from_right = me - k, me + k

        def pass_on(group):
            @pl.when(from_left >= 0)
            def _():
                forward(group, from_left).wait_recv()

                @pl.when(has_right)
                def _():
                    forward(group, from_left).start()

            @pl.when(from_right < n)
            def _():
                backward(group, from_right).wait_recv()

                @pl.when(has_left)
                def _():
                    backward(group, from_right).start()

        each_group(pass_on)
        return carry

    lax.fori_loop(1, n, relay, 0)

    def own_sent(group):
        @pl.when(has_right)
        def _():
            forward(group, me).wait_send()

        @pl.when(has_left)
        def _():
            backward(group, me, own=True).wait_send()

    each_group(own_sent)

    def drain(k, carry):
        def sent(group):
            @pl.when(jnp.logical_and(me - k >= 0, has_right))
            def _():
                forward(group, me - k).wait_send()

            @pl.when(jnp.logical_and(me + k < n, has_left))
            def _():
                backward(group, me + k).wait_send()

        each_group(sent)
        return carry

    lax.fori_loop(1, n, drain, 0)


def body(n, *refs):
    kernel(n, refs[:14], refs[14:18], refs[18], refs[19:33], *refs[33:])


def store(n, cores, *refs):
    gathered, norm_ref, outs, norm_out, flat, rounded, sem, mixed_sem, norm_sem = (
        refs[:4],
        refs[4],
        refs[5:9],
        *refs[9:],
    )
    me, core = lax.axis_index("shard"), lax.axis_index("width")
    copies = []
    for source, out in zip(gathered[:3], outs[:3]):
        for row in range(0, source.shape[0], COPY_ROWS):
            rows = pl.ds(row, min(COPY_ROWS, source.shape[0] - row))
            copies.append(
                pltpu.make_async_copy(source.at[rows], out.at[rows], sem.at[len(copies)])
            )

    block = gathered[3].shape[0] // n
    tail = late_rows(block)

    def mixed(origin, row, size, part):
        rows = pl.ds(origin * block + row, size)
        return pltpu.make_async_copy(
            gathered[3].at[rows], outs[3].at[rows], mixed_sem.at[origin, part]
        )

    copies += [mixed(origin, 0, block - tail, 0) for origin in range(n)]

    def each_last(act):
        for origin in range(n if tail else 0):

            @pl.when(jnp.logical_or(core != LATE_CORE, me == origin))
            def _(origin=origin):
                act(mixed(origin, block - tail, tail, 1))

    for copy in copies:
        copy.start()
    each_last(lambda copy: copy.start())
    rows = norm_ref.shape[2]
    for origin in range(n):
        for side in range(cores):
            flat[pl.ds((origin * cores + side) * rows, rows)] = norm_ref[origin, side]
    rounded[...] = flat[...].astype(norm_out.dtype)
    norm_copy = pltpu.make_async_copy(rounded, norm_out, norm_sem)
    norm_copy.start()
    for copy in copies:
        copy.wait()
    each_last(lambda copy: copy.wait())
    norm_copy.wait()


def late(n, mixed, after, out, send_sem, recv_sem, told_sem):
    me = lax.axis_index("shard")
    core = lax.axis_index("width")
    has_left, has_right = me > 0, me < n - 1
    left, right = {"shard": me - 1}, {"shard": me + 1}
    block = mixed.shape[0] // n
    tail = late_rows(block)
    size = tail // LATE_STEPS

    def copy(origin, begin, rows, step, device, semaphore, own):
        first = pl.multiple_of(me * block + block - tail + begin, 16)
        dst = out.at[origin, pl.ds(pl.multiple_of(begin, 16), rows)]
        return pltpu.make_async_remote_copy(
            src_ref=mixed.at[pl.ds(first, rows)] if own else dst,
            dst_ref=dst,
            send_sem=send_sem.at[semaphore],
            recv_sem=recv_sem.at[origin, step],
            device_id=device,
            device_id_type=MESH,
        )

    def forward(origin, step, own=False):
        return copy(origin, step * size, size, step, right, origin, own)

    def backward(origin, step, own=False):
        return copy(origin, step * size, size, step, left, n if own else origin, own)

    def sent(origin, semaphore):
        copy(origin, 0, tail, 0, right, semaphore, True).wait_send()

    @pl.when(core == LATE_CORE)
    def _():
        barrier = pltpu.get_barrier_semaphore()
        half = n // 2
        to_left, middle = me < half, me == half

        def signal(semaphore, condition, device):
            @pl.when(condition)
            def _():
                pl.semaphore_signal(semaphore, inc=1, device_id=device, device_id_type=MESH)

        signal(barrier, jnp.logical_and(has_right, me < half), right)
        signal(barrier, me > half, left)
        known = jnp.where(to_left, has_left, has_right).astype(jnp.int32)
        known += jnp.logical_and(middle, has_left).astype(jnp.int32)

        @pl.when(known > 0)
        def _():
            pl.semaphore_wait(barrier, known)

        def own(direction, condition):
            for step in range(LATE_STEPS):

                @pl.when(condition)
                def _(step=step):
                    direction(me, step, own=True).start()

        own(backward, jnp.logical_and(to_left, has_left))
        own(forward, jnp.logical_and(jnp.logical_not(to_left), has_right))
        signal(told_sem, jnp.logical_and(has_left, me <= half), left)
        signal(told_sem, jnp.logical_and(has_right, me >= half), right)
        unknown = jnp.logical_or(jnp.logical_and(to_left, has_right), me > half)

        @pl.when(unknown)
        def _():
            pl.semaphore_wait(told_sem, 1)
        own(backward, jnp.logical_and(jnp.logical_not(to_left), has_left))
        own(forward, jnp.logical_and(to_left, has_right))

        def relay(k, carry):
            for step in range(LATE_STEPS):

                @pl.when(me - k >= 0)
                def _(step=step):
                    forward(me - k, step).wait_recv()

                    @pl.when(has_right)
                    def _():
                        forward(me - k, step).start()

                @pl.when(me + k < n)
                def _(step=step):
                    backward(me + k, step).wait_recv()

                    @pl.when(has_left)
                    def _():
                        backward(me + k, step).start()

            return carry

        lax.fori_loop(1, n, relay, 0)

        @pl.when(has_right)
        def _():
            sent(me, me)

        @pl.when(has_left)
        def _():
            sent(me, n)

        def drain(k, carry):
            @pl.when(jnp.logical_and(me - k >= 0, has_right))
            def _():
                sent(me - k, me - k)

            @pl.when(jnp.logical_and(me + k < n, has_left))
            def _():
                sent(me + k, me + k)

            return carry

        lax.fori_loop(1, n, drain, 0)


def store_late(n, pieces, given, out, sem):
    me, core = lax.axis_index("shard"), lax.axis_index("width")
    block = out.shape[0] // n
    tail = late_rows(block)

    def each(act):
        for origin in range(n):

            @pl.when(jnp.logical_and(core == LATE_CORE, me != origin))
            def _(origin=origin):
                act(origin)

    def begin(origin):
        for row in range(0, tail, STORE_ROWS):
            rows = pl.ds((origin + 1) * block - tail + row, STORE_ROWS)
            source = pieces.at[origin, pl.ds(row, STORE_ROWS)]
            pltpu.make_async_copy(source, out.at[rows], sem.at[origin]).start()

    def end(origin):
        rows = pl.ds((origin + 1) * block - tail, tail)
        pltpu.make_async_copy(pieces.at[origin], out.at[rows], sem.at[origin]).wait()

    each(begin)
    each(end)


def on_device(n, cores, *args):
    weights, (norm_train, norm_step) = list(args[:12]), args[12:]
    bases = weights[0::3]
    (size,) = norm_train.shape
    sizes = [size, *(size for w in bases for size in w.shape)]
    if cores != 2 or any(size % LANES for size in sizes):
        return plain(*args)
    rows = size // LANES
    shapes = [(w.shape[1], w.shape[0] * n) for w in bases[:3]]
    shapes.append((bases[3].shape[1] * n, bases[3].shape[0]))
    in_hbm = pl.BlockSpec(memory_space=pltpu.HBM)
    in_vmem = pl.BlockSpec(memory_space=pltpu.VMEM)
    tail = late_rows(bases[3].shape[1])
    groups = len(bases) + (2 if tail else 1)
    weights[1::3] = [low.T for low in weights[1::3]]
    norms = [norm_train.reshape(rows, LANES), norm_step.reshape(rows, LANES)]
    given = [pltpu.with_memory_space_constraint(array, pltpu.HBM) for array in weights + norms]
    gathered = pl.pallas_call(
        functools.partial(body, n),
        out_shape=[pltpu.VMEM(shape, jnp.bfloat16) for shape in shapes]
        + [pltpu.VMEM((n, cores, rows, LANES), jnp.float32)],
        in_specs=[in_hbm] * 14,
        out_specs=[in_vmem] * 5,
        scratch_shapes=[pltpu.VMEM(array.shape, array.dtype) for array in given]
        + [
            pltpu.SemaphoreType.DMA((15 + bases[0].shape[0] // LANES,)),
            pltpu.SemaphoreType.DMA((n, groups)),
            pltpu.SemaphoreType.DMA((groups,)),
            pltpu.SemaphoreType.DMA((n, groups)),
            pltpu.SemaphoreType.DMA((2,)),
            pltpu.SemaphoreType.REGULAR,
        ],
        compiler_params=pltpu.CompilerParams(
            collective_id=0, has_side_effects=True, vmem_limit_bytes=40 * 2**20
        ),
        name="merge_gather",
    )(*given)
    norm_rows = n * cores * rows
    *finals, norm = pl.pallas_call(
        functools.partial(store, n, cores),
        out_shape=[jax.ShapeDtypeStruct(shape, jnp.bfloat16) for shape in shapes]
        + [jax.ShapeDtypeStruct((norm_rows, LANES), jnp.bfloat16)],
        in_specs=[in_vmem] * 5,
        out_specs=[in_hbm] * 5,
        scratch_shapes=[
            pltpu.VMEM((norm_rows, LANES), jnp.float32),
            pltpu.VMEM((norm_rows, LANES), jnp.bfloat16),
            pltpu.SemaphoreType.DMA((sum(-(-shape[0] // COPY_ROWS) for shape in shapes[:3]),)),
            pltpu.SemaphoreType.DMA((n, 2)),
            pltpu.SemaphoreType.DMA,
        ],
        compiler_params=pltpu.CompilerParams(vmem_limit_bytes=20 * 2**20),
        name="store",
    )(*gathered)
    norm = norm.reshape(-1)
    if not tail:
        return (*finals, norm)
    columns = shapes[3][1]
    pieces = pl.pallas_call(
        functools.partial(late, n),
        out_shape=pltpu.VMEM((n, tail, columns), jnp.bfloat16),
        in_specs=[in_vmem, in_hbm],
        out_specs=in_vmem,
        scratch_shapes=[
            pltpu.SemaphoreType.DMA((n + 1,)),
            pltpu.SemaphoreType.DMA((n, LATE_STEPS)),
            pltpu.SemaphoreType.REGULAR,
        ],
        compiler_params=pltpu.CompilerParams(
            collective_id=1, has_side_effects=True, vmem_limit_bytes=20 * 2**20
        ),
        name="late",
    )(gathered[3], pltpu.with_memory_space_constraint(finals[3], pltpu.HBM))
    finals[3] = pl.pallas_call(
        functools.partial(store_late, n),
        out_shape=jax.ShapeDtypeStruct(shapes[3], jnp.bfloat16),
        in_specs=[in_vmem, in_hbm],
        out_specs=in_hbm,
        input_output_aliases={1: 0},
        scratch_shapes=[pltpu.SemaphoreType.DMA((n,))],
        compiler_params=pltpu.CompilerParams(vmem_limit_bytes=20 * 2**20),
        name="store_late",
    )(pieces, finals[3])
    return (*finals, norm)


def solution(mesh):
    placed = (
        P(("shift", "shard"), "width"),
        P(("shift", "shard"), None),
        P("shift", "width"),
        P(("shift", "shard"), "width"),
        P(("shift", "shard"), None),
        P("shift", "width"),
        P(("shift", "shard"), "width"),
        P(("shift", "shard"), None),
        P("shift", "width"),
        P(("shift", "width"), "shard"),
        P(("shift", "width"), None),
        P("shift", "shard"),
        P(("shift", "shard", "width")),
        P(("shift", "shard", "width")),
    )
    return jax.shard_map(
        functools.partial(on_device, mesh.shape["shard"], mesh.shape["width"]),
        mesh=mesh,
        in_specs=placed,
        out_specs=(
            P(("shift", "width"), None),
            P(("shift", "width"), None),
            P(("shift", "width"), None),
            P("shift", "width"),
            P("shift"),
        ),
        check_vma=False,
    )
```

```python
import functools

import jax
import jax.numpy as jnp
from jax import lax
from jax.experimental import pallas as pl
from jax.experimental.pallas import tpu as pltpu
from jax.sharding import PartitionSpec as P

mix_rate = 0.5
MESH = pl.DeviceIdType.MESH
LANES = 128
COPY_ROWS = 256
LATE_STEPS = 2
LATE_CORE = 1
LATE_ROWS = 128
ROW_UNIT = 64
EARLY_PIECES = 3
STORE_ROWS = 64


def plain(
    w_query,
    low_query,
    high_query,
    w_key,
    low_key,
    high_key,
    w_value,
    low_value,
    high_value,
    w_mixed,
    low_mixed,
    high_mixed,
    norm_train,
    norm_step,
):
    def merged(w, low, high):
        low_rank = jnp.dot(low, high, preferred_element_type=jnp.float32)
        return (w.astype(jnp.float32) + mix_rate * low_rank).astype(jnp.bfloat16)

    query = lax.all_gather(merged(w_query, low_query, high_query), "shard", axis=0, tiled=True)
    key = lax.all_gather(merged(w_key, low_key, high_key), "shard", axis=0, tiled=True)
    value = lax.all_gather(merged(w_value, low_value, high_value), "shard", axis=0, tiled=True)
    mixed = lax.all_gather(merged(w_mixed, low_mixed, high_mixed), "shard", axis=1, tiled=True)
    norm = lax.all_gather(
        (norm_train + norm_step).astype(jnp.bfloat16), ("shard", "width"), axis=0, tiled=True
    )
    return query.T, key.T, value.T, mixed.T, norm


def late_rows(block):
    return LATE_ROWS if block > LATE_ROWS else 0


def kernel(
    n,
    given,
    outs,
    norm_out,
    copied,
    load_sem,
    send_sem,
    back_sem,
    recv_sem,
    pair_sem,
    told_sem,
):
    me = lax.axis_index("shard")
    core = lax.axis_index("width")
    has_left, has_right = me > 0, me < n - 1
    left, right = {"shard": me - 1}, {"shard": me + 1}
    partner = {"width": 1 - core}
    held, low_refs, high_refs = copied[0:12:3], copied[1:12:3], copied[2:12:3]
    depth, width = held[0].shape
    first, rest = pl.ds(0, LANES), pl.ds(LANES, width - LANES)
    bands = [pl.ds(row, LANES) for row in range(0, depth, LANES)]
    loads = []

    def load(source, target):
        loads.append(pltpu.make_async_copy(source, target, load_sem.at[len(loads)]))
        return loads[-1]

    opening = [load(given[1], copied[1]), load(given[2].at[:, first], copied[2].at[:, first])]
    opening += [load(given[0].at[rows, first], held[0].at[rows, first]) for rows in bands]
    others = []
    if width > LANES:
        others = [load(given[i].at[:, rest], copied[i].at[:, rest]) for i in (2, 0)]
    rest_of = [others] + [
        [load(given[i], copied[i]) for i in range(array, array + 3)] for array in (3, 6, 9)
    ]
    norm_loads = [load(given[i], copied[i]) for i in (12, 13)]
    for one in opening:
        one.start()

    barrier = pltpu.get_barrier_semaphore()
    pl.semaphore_signal(barrier, inc=1, device_id=partner, device_id_type=MESH)

    @pl.when(has_right)
    def _():
        pl.semaphore_signal(barrier, inc=1, device_id=right, device_id_type=MESH)

    for one in loads[len(opening) :]:
        one.start()
    pl.semaphore_wait(barrier, 1 + has_left.astype(jnp.int32))

    @pl.when(has_left)
    def _():
        pl.semaphore_signal(told_sem, inc=1, device_id=left, device_id_type=MESH)

    last = len(outs) - 1
    block = held[last].shape[1]
    tail = late_rows(block)
    groups = [(array, 0, w.shape[1]) for array, w in enumerate(held[:last])]
    groups.append((last, 0, block - tail))
    if tail:
        groups.append((last, block - tail, tail))
    groups.append((len(outs), 0, 0))
    late_group = len(groups) - 2 if tail else -1

    def part(array, row, rows, origin):
        if array == len(outs):
            return norm_out.at[origin]
        out, w = outs[array], held[array]
        if array < last:
            size = w.shape[0]
            begin = pl.multiple_of(origin * size, LANES)
            return out.at[pl.ds(pl.multiple_of(row, LANES), rows), pl.ds(begin, size)]
        begin = pl.multiple_of(origin * block + row, ROW_UNIT)
        return out.at[pl.ds(begin, rows)]

    def copy(ref, device, semaphore, origin, group):
        return pltpu.make_async_remote_copy(
            src_ref=ref,
            dst_ref=ref,
            send_sem=semaphore,
            recv_sem=recv_sem.at[origin, group],
            device_id=device,
            device_id_type=MESH,
        )

    def forward(group, origin):
        ref = part(*groups[group], origin)
        return copy(ref, right, send_sem.at[origin, group], origin, group)

    def backward(group, origin, own=False):
        ref = part(*groups[group], origin)
        semaphore = back_sem.at[group] if own else send_sem.at[origin, group]
        return copy(ref, left, semaphore, origin, group)

    def compute(array, c):
        rows = pl.ds(pl.multiple_of(c * LANES, LANES), LANES)
        low_rank = lax.dot_general(
            high_refs[array][:, rows],
            low_refs[array][...],
            (((0,), (0,)), ((), ())),
            preferred_element_type=jnp.float32,
        )
        base = held[array][:, rows].T.astype(jnp.float32)
        part(array, c * LANES, LANES, me)[...] = (base + mix_rate * low_rank).astype(
            jnp.bfloat16
        )

    def send_left(ref, group):
        @pl.when(has_left)
        def _():
            copy(ref, left, back_sem.at[group], me, group).start()

    def send_right(ref, group):
        @pl.when(has_right)
        def _():
            copy(ref, right, send_sem.at[me, group], me, group).start()

    def send_both(ref, group):
        send_left(ref, group)
        send_right(ref, group)

    def open_right(rows):
        @pl.when(has_right)
        def _():
            pl.semaphore_wait(told_sem, 1)

        send_right(part(0, 0, rows, me), 0)

    def finish(array):
        if array == 0:
            rows = held[0].shape[1]
            if rows > LANES:
                send_left(part(0, rows - LANES, LANES, me), 0)
            if early:
                send_right(part(0, early, rows - early, me), 0)
            else:
                open_right(rows)
        else:
            send_both(part(*groups[array], me), array)

    for one in opening:
        one.wait()
    compute(0, 0)

    send_left(part(0, 0, LANES, me), 0)

    def exchange(side):
        return pltpu.make_async_remote_copy(
            src_ref=norm_out.at[me, side],
            dst_ref=norm_out.at[me, side],
            send_sem=pair_sem.at[0],
            recv_sem=pair_sem.at[1],
            device_id=partner,
            device_id_type=MESH,
        )

    early = (EARLY_PIECES - 1) * LANES if width > EARLY_PIECES * LANES else 0

    for array in range(len(outs)):
        for one in rest_of[array]:
            one.wait()
        count = held[array].shape[1] // LANES
        if array:
            compute(array, 0)
            finish(array - 1)
        if array == 1:
            for one in norm_loads:
                one.wait()
            norm_out[me, core] = copied[12][...] + copied[13][...]
        begin = 1
        if array == 0 and count > 1:
            compute(0, 1)
            begin = 2

        def step(c, carry, array=array):
            compute(array, c)
            if array == 0:
                send_left(part(0, (c - 1) * LANES, LANES, me), 0)
            return carry

        if array == 0 and early:
            lax.fori_loop(begin, EARLY_PIECES, step, 0)
            open_right(early)
            begin = EARLY_PIECES
        lax.fori_loop(begin, count, step, 0)
    exchange(core).start()
    if tail >= LANES:
        finish(last)
    exchange(core).wait_send()
    exchange(1 - core).wait_recv()
    if tail < LANES:
        finish(last)
    if tail:

        @pl.when(core != LATE_CORE)
        def _():
            send_both(part(*groups[late_group], me), late_group)

    send_both(part(*groups[-1], me), len(groups) - 1)

    def each_group(act):
        for group in range(len(groups)):
            if group == late_group:

                @pl.when(core != LATE_CORE)
                def _(group=group):
                    act(group)
            else:
                act(group)

    def relay(k, carry):
        from_left, from_right = me - k, me + k

        def pass_on(group):
            @pl.when(from_left >= 0)
            def _():
                forward(group, from_left).wait_recv()

                @pl.when(has_right)
                def _():
                    forward(group, from_left).start()

            @pl.when(from_right < n)
            def _():
                backward(group, from_right).wait_recv()

                @pl.when(has_left)
                def _():
                    backward(group, from_right).start()

        each_group(pass_on)
        return carry

    lax.fori_loop(1, n, relay, 0)

    def own_sent(group):
        @pl.when(has_right)
        def _():
            forward(group, me).wait_send()

        @pl.when(has_left)
        def _():
            backward(group, me, own=True).wait_send()

    each_group(own_sent)

    def drain(k, carry):
        def sent(group):
            @pl.when(jnp.logical_and(me - k >= 0, has_right))
            def _():
                forward(group, me - k).wait_send()

            @pl.when(jnp.logical_and(me + k < n, has_left))
            def _():
                backward(group, me + k).wait_send()

        each_group(sent)
        return carry

    lax.fori_loop(1, n, drain, 0)


def body(n, *refs):
    kernel(n, refs[:14], refs[14:18], refs[18], refs[19:33], *refs[33:])


def store(n, cores, *refs):
    gathered, norm_ref, outs, norm_out, flat, rounded, sem, mixed_sem, norm_sem = (
        refs[:4],
        refs[4],
        refs[5:9],
        *refs[9:],
    )
    me, core = lax.axis_index("shard"), lax.axis_index("width")
    copies = []
    for source, out in zip(gathered[:3], outs[:3]):
        for row in range(0, source.shape[0], COPY_ROWS):
            rows = pl.ds(row, min(COPY_ROWS, source.shape[0] - row))
            copies.append(
                pltpu.make_async_copy(source.at[rows], out.at[rows], sem.at[len(copies)])
            )

    block = gathered[3].shape[0] // n
    tail = late_rows(block)

    def mixed(origin, row, size, part):
        rows = pl.ds(origin * block + row, size)
        return pltpu.make_async_copy(
            gathered[3].at[rows], outs[3].at[rows], mixed_sem.at[origin, part]
        )

    copies += [mixed(origin, 0, block - tail, 0) for origin in range(n)]

    def each_last(act):
        for origin in range(n if tail else 0):

            @pl.when(jnp.logical_or(core != LATE_CORE, me == origin))
            def _(origin=origin):
                act(mixed(origin, block - tail, tail, 1))

    for copy in copies:
        copy.start()
    each_last(lambda copy: copy.start())
    rows = norm_ref.shape[2]
    for origin in range(n):
        for side in range(cores):
            flat[pl.ds((origin * cores + side) * rows, rows)] = norm_ref[origin, side]
    rounded[...] = flat[...].astype(norm_out.dtype)
    norm_copy = pltpu.make_async_copy(rounded, norm_out, norm_sem)
    norm_copy.start()
    for copy in copies:
        copy.wait()
    each_last(lambda copy: copy.wait())
    norm_copy.wait()


def late(n, mixed, after, out, send_sem, recv_sem, told_sem):
    me = lax.axis_index("shard")
    core = lax.axis_index("width")
    has_left, has_right = me > 0, me < n - 1
    left, right = {"shard": me - 1}, {"shard": me + 1}
    block = mixed.shape[0] // n
    tail = late_rows(block)
    size = tail // LATE_STEPS

    def copy(origin, begin, rows, step, device, semaphore, own):
        first = pl.multiple_of(me * block + block - tail + begin, 16)
        dst = out.at[origin, pl.ds(pl.multiple_of(begin, 16), rows)]
        return pltpu.make_async_remote_copy(
            src_ref=mixed.at[pl.ds(first, rows)] if own else dst,
            dst_ref=dst,
            send_sem=send_sem.at[semaphore],
            recv_sem=recv_sem.at[origin, step],
            device_id=device,
            device_id_type=MESH,
        )

    def forward(origin, step, own=False):
        return copy(origin, step * size, size, step, right, origin, own)

    def backward(origin, step, own=False):
        return copy(origin, step * size, size, step, left, n if own else origin, own)

    def sent(origin, semaphore):
        copy(origin, 0, tail, 0, right, semaphore, True).wait_send()

    @pl.when(core == LATE_CORE)
    def _():
        barrier = pltpu.get_barrier_semaphore()

        @pl.when(has_right)
        def _():
            pl.semaphore_signal(barrier, inc=1, device_id=right, device_id_type=MESH)

        @pl.when(has_left)
        def _():
            pl.semaphore_wait(barrier, 1)
            for step in range(LATE_STEPS):
                backward(me, step, own=True).start()
            pl.semaphore_signal(told_sem, inc=1, device_id=left, device_id_type=MESH)

        @pl.when(has_right)
        def _():
            pl.semaphore_wait(told_sem, 1)
            for step in range(LATE_STEPS):
                forward(me, step, own=True).start()

        def relay(k, carry):
            for step in range(LATE_STEPS):

                @pl.when(me - k >= 0)
                def _(step=step):
                    forward(me - k, step).wait_recv()

                    @pl.when(has_right)
                    def _():
                        forward(me - k, step).start()

                @pl.when(me + k < n)
                def _(step=step):
                    backward(me + k, step).wait_recv()

                    @pl.when(has_left)
                    def _():
                        backward(me + k, step).start()

            return carry

        lax.fori_loop(1, n, relay, 0)

        @pl.when(has_right)
        def _():
            sent(me, me)

        @pl.when(has_left)
        def _():
            sent(me, n)

        def drain(k, carry):
            @pl.when(jnp.logical_and(me - k >= 0, has_right))
            def _():
                sent(me - k, me - k)

            @pl.when(jnp.logical_and(me + k < n, has_left))
            def _():
                sent(me + k, me + k)

            return carry

        lax.fori_loop(1, n, drain, 0)


def store_late(n, pieces, given, out, sem):
    me, core = lax.axis_index("shard"), lax.axis_index("width")
    block = out.shape[0] // n
    tail = late_rows(block)

    def each(act):
        for origin in range(n):

            @pl.when(jnp.logical_and(core == LATE_CORE, me != origin))
            def _(origin=origin):
                act(origin)

    def begin(origin):
        for row in range(0, tail, STORE_ROWS):
            rows = pl.ds((origin + 1) * block - tail + row, STORE_ROWS)
            source = pieces.at[origin, pl.ds(row, STORE_ROWS)]
            pltpu.make_async_copy(source, out.at[rows], sem.at[origin]).start()

    def end(origin):
        rows = pl.ds((origin + 1) * block - tail, tail)
        pltpu.make_async_copy(pieces.at[origin], out.at[rows], sem.at[origin]).wait()

    each(begin)
    each(end)


def on_device(n, cores, *args):
    weights, (norm_train, norm_step) = list(args[:12]), args[12:]
    bases = weights[0::3]
    (size,) = norm_train.shape
    sizes = [size, *(size for w in bases for size in w.shape)]
    if cores != 2 or any(size % LANES for size in sizes):
        return plain(*args)
    rows = size // LANES
    shapes = [(w.shape[1], w.shape[0] * n) for w in bases[:3]]
    shapes.append((bases[3].shape[1] * n, bases[3].shape[0]))
    in_hbm = pl.BlockSpec(memory_space=pltpu.HBM)
    in_vmem = pl.BlockSpec(memory_space=pltpu.VMEM)
    tail = late_rows(bases[3].shape[1])
    groups = len(bases) + (2 if tail else 1)
    weights[1::3] = [low.T for low in weights[1::3]]
    norms = [norm_train.reshape(rows, LANES), norm_step.reshape(rows, LANES)]
    given = [pltpu.with_memory_space_constraint(array, pltpu.HBM) for array in weights + norms]
    gathered = pl.pallas_call(
        functools.partial(body, n),
        out_shape=[pltpu.VMEM(shape, jnp.bfloat16) for shape in shapes]
        + [pltpu.VMEM((n, cores, rows, LANES), jnp.float32)],
        in_specs=[in_hbm] * 14,
        out_specs=[in_vmem] * 5,
        scratch_shapes=[pltpu.VMEM(array.shape, array.dtype) for array in given]
        + [
            pltpu.SemaphoreType.DMA((15 + bases[0].shape[0] // LANES,)),
            pltpu.SemaphoreType.DMA((n, groups)),
            pltpu.SemaphoreType.DMA((groups,)),
            pltpu.SemaphoreType.DMA((n, groups)),
            pltpu.SemaphoreType.DMA((2,)),
            pltpu.SemaphoreType.REGULAR,
        ],
        compiler_params=pltpu.CompilerParams(
            collective_id=0, has_side_effects=True, vmem_limit_bytes=40 * 2**20
        ),
        name="merge_gather",
    )(*given)
    norm_rows = n * cores * rows
    *finals, norm = pl.pallas_call(
        functools.partial(store, n, cores),
        out_shape=[jax.ShapeDtypeStruct(shape, jnp.bfloat16) for shape in shapes]
        + [jax.ShapeDtypeStruct((norm_rows, LANES), jnp.bfloat16)],
        in_specs=[in_vmem] * 5,
        out_specs=[in_hbm] * 5,
        scratch_shapes=[
            pltpu.VMEM((norm_rows, LANES), jnp.float32),
            pltpu.VMEM((norm_rows, LANES), jnp.bfloat16),
            pltpu.SemaphoreType.DMA((sum(-(-shape[0] // COPY_ROWS) for shape in shapes[:3]),)),
            pltpu.SemaphoreType.DMA((n, 2)),
            pltpu.SemaphoreType.DMA,
        ],
        compiler_params=pltpu.CompilerParams(vmem_limit_bytes=20 * 2**20),
        name="store",
    )(*gathered)
    norm = norm.reshape(-1)
    if not tail:
        return (*finals, norm)
    columns = shapes[3][1]
    pieces = pl.pallas_call(
        functools.partial(late, n),
        out_shape=pltpu.VMEM((n, tail, columns), jnp.bfloat16),
        in_specs=[in_vmem, in_hbm],
        out_specs=in_vmem,
        scratch_shapes=[
            pltpu.SemaphoreType.DMA((n + 1,)),
            pltpu.SemaphoreType.DMA((n, LATE_STEPS)),
            pltpu.SemaphoreType.REGULAR,
        ],
        compiler_params=pltpu.CompilerParams(
            collective_id=1, has_side_effects=True, vmem_limit_bytes=20 * 2**20
        ),
        name="late",
    )(gathered[3], pltpu.with_memory_space_constraint(finals[3], pltpu.HBM))
    finals[3] = pl.pallas_call(
        functools.partial(store_late, n),
        out_shape=jax.ShapeDtypeStruct(shapes[3], jnp.bfloat16),
        in_specs=[in_vmem, in_hbm],
        out_specs=in_hbm,
        input_output_aliases={1: 0},
        scratch_shapes=[pltpu.SemaphoreType.DMA((n,))],
        compiler_params=pltpu.CompilerParams(vmem_limit_bytes=20 * 2**20),
        name="store_late",
    )(pieces, finals[3])
    return (*finals, norm)


def solution(mesh):
    placed = (
        P(("shift", "shard"), "width"),
        P(("shift", "shard"), None),
        P("shift", "width"),
        P(("shift", "shard"), "width"),
        P(("shift", "shard"), None),
        P("shift", "width"),
        P(("shift", "shard"), "width"),
        P(("shift", "shard"), None),
        P("shift", "width"),
        P(("shift", "width"), "shard"),
        P(("shift", "width"), None),
        P("shift", "shard"),
        P(("shift", "shard", "width")),
        P(("shift", "shard", "width")),
    )
    return jax.shard_map(
        functools.partial(on_device, mesh.shape["shard"], mesh.shape["width"]),
        mesh=mesh,
        in_specs=placed,
        out_specs=(
            P(("shift", "width"), None),
            P(("shift", "width"), None),
            P(("shift", "width"), None),
            P("shift", "width"),
            P("shift"),
        ),
        check_vma=False,
    )
```

```python
import functools

import jax
import jax.numpy as jnp
from jax import lax
from jax.experimental import pallas as pl
from jax.experimental.pallas import tpu as pltpu
from jax.sharding import PartitionSpec as P

mix_rate = 0.5
MESH = pl.DeviceIdType.MESH
LANES = 128
COPY_ROWS = 256
LATE_STEPS = 2
LATE_CORE = 1
LATE_ROWS = 128
ROW_UNIT = 16
DETOURS = 2
DETOUR_ROWS = 16
EARLY_PIECES = 3
STORE_ROWS = 64


def plain(
    w_query,
    low_query,
    high_query,
    w_key,
    low_key,
    high_key,
    w_value,
    low_value,
    high_value,
    w_mixed,
    low_mixed,
    high_mixed,
    norm_train,
    norm_step,
):
    def merged(w, low, high):
        low_rank = jnp.dot(low, high, preferred_element_type=jnp.float32)
        return (w.astype(jnp.float32) + mix_rate * low_rank).astype(jnp.bfloat16)

    query = lax.all_gather(merged(w_query, low_query, high_query), "shard", axis=0, tiled=True)
    key = lax.all_gather(merged(w_key, low_key, high_key), "shard", axis=0, tiled=True)
    value = lax.all_gather(merged(w_value, low_value, high_value), "shard", axis=0, tiled=True)
    mixed = lax.all_gather(merged(w_mixed, low_mixed, high_mixed), "shard", axis=1, tiled=True)
    norm = lax.all_gather(
        (norm_train + norm_step).astype(jnp.bfloat16), ("shard", "width"), axis=0, tiled=True
    )
    return query.T, key.T, value.T, mixed.T, norm


def detours(shifts):
    return min(DETOURS, shifts - 1)


def late_rows(block):
    return LATE_ROWS if block > LATE_ROWS else 0


def kernel(
    n,
    shifts,
    given,
    outs,
    norm_out,
    copied,
    load_sem,
    send_sem,
    back_sem,
    recv_sem,
    pair_sem,
    told_sem,
    detour,
    detour_send,
    detour_recv,
):
    me, shift = lax.axis_index("shard"), lax.axis_index("shift")
    core = lax.axis_index("width")
    has_left, has_right = me > 0, me < n - 1
    left, right = {"shard": me - 1}, {"shard": me + 1}
    partner = {"width": 1 - core}
    helpers = range(1, 1 + detours(shifts))
    aside = len(helpers) * DETOUR_ROWS

    def on_early(*conditions):
        return functools.reduce(jnp.logical_and, conditions, core != LATE_CORE)

    helps = jnp.logical_and(shift >= 1, shift <= len(helpers))
    leads, ends = on_early(shift == 0, me == 1), on_early(shift == 0, me == 0)
    lifts, lands = on_early(helps, me == 1), on_early(helps, me == 0)
    held, low_refs, high_refs = copied[0:12:3], copied[1:12:3], copied[2:12:3]
    depth, width = held[0].shape
    first, rest = pl.ds(0, LANES), pl.ds(LANES, width - LANES)
    bands = [pl.ds(row, LANES) for row in range(0, depth, LANES)]
    loads = []

    def load(source, target):
        loads.append(pltpu.make_async_copy(source, target, load_sem.at[len(loads)]))
        return loads[-1]

    opening = [load(given[1], copied[1]), load(given[2].at[:, first], copied[2].at[:, first])]
    opening += [load(given[0].at[rows, first], held[0].at[rows, first]) for rows in bands]
    others = []
    if width > LANES:
        others = [load(given[i].at[:, rest], copied[i].at[:, rest]) for i in (2, 0)]
    rest_of = [others] + [
        [load(given[i], copied[i]) for i in range(array, array + 3)] for array in (3, 6, 9)
    ]
    norm_loads = [load(given[i], copied[i]) for i in (12, 13)]
    for one in opening:
        one.start()

    barrier = pltpu.get_barrier_semaphore()
    pl.semaphore_signal(barrier, inc=1, device_id=partner, device_id_type=MESH)

    @pl.when(has_right)
    def _():
        pl.semaphore_signal(barrier, inc=1, device_id=right, device_id_type=MESH)

    if aside:

        @pl.when(lifts)
        def _():
            line = {"shift": 0 * shift}
            pl.semaphore_signal(barrier, inc=1, device_id=line, device_id_type=MESH)

        @pl.when(ends)
        def _():
            for helper in helpers:
                line = {"shift": 0 * shift + helper}
                pl.semaphore_signal(barrier, inc=1, device_id=line, device_id_type=MESH)

    for one in loads[len(opening) :]:
        one.start()
    waited = 1 + has_left.astype(jnp.int32)
    if aside:
        waited += jnp.where(leads, len(helpers), 0) + lands.astype(jnp.int32)
    pl.semaphore_wait(barrier, waited)

    @pl.when(has_left)
    def _():
        pl.semaphore_signal(told_sem, inc=1, device_id=left, device_id_type=MESH)

    last = len(outs) - 1
    block = held[last].shape[1]
    tail = late_rows(block)
    groups = [(array, 0, w.shape[1]) for array, w in enumerate(held[:last])]
    groups.append((last, aside, block - tail - aside))
    if tail:
        groups.append((last, block - tail, tail))
    groups.append((len(outs), 0, 0))
    side_group = len(groups)
    if aside:
        groups.append((last, 0, aside))
    norm_group = len(outs) + (1 if tail else 0)
    late_group = norm_group - 1 if tail else -1

    def part(array, row, rows, origin):
        if array == len(outs):
            return norm_out.at[origin]
        out, w = outs[array], held[array]
        if array < last:
            size = w.shape[0]
            begin = pl.multiple_of(origin * size, LANES)
            return out.at[pl.ds(pl.multiple_of(row, LANES), rows), pl.ds(begin, size)]
        begin = pl.multiple_of(origin * block + row, ROW_UNIT)
        return out.at[pl.ds(begin, rows)]

    def copy(ref, device, semaphore, origin, group):
        return pltpu.make_async_remote_copy(
            src_ref=ref,
            dst_ref=ref,
            send_sem=semaphore,
            recv_sem=recv_sem.at[origin, group],
            device_id=device,
            device_id_type=MESH,
        )

    def forward(group, origin):
        ref = part(*groups[group], origin)
        return copy(ref, right, send_sem.at[origin, group], origin, group)

    def backward(group, origin, own=False):
        ref = part(*groups[group], origin)
        semaphore = back_sem.at[group] if own else send_sem.at[origin, group]
        return copy(ref, left, semaphore, origin, group)

    def compute(array, c):
        rows = pl.ds(pl.multiple_of(c * LANES, LANES), LANES)
        low_rank = lax.dot_general(
            high_refs[array][:, rows],
            low_refs[array][...],
            (((0,), (0,)), ((), ())),
            preferred_element_type=jnp.float32,
        )
        base = held[array][:, rows].T.astype(jnp.float32)
        part(array, c * LANES, LANES, me)[...] = (base + mix_rate * low_rank).astype(
            jnp.bfloat16
        )

    def send_left(ref, group):
        @pl.when(has_left)
        def _():
            copy(ref, left, back_sem.at[group], me, group).start()

    def send_right(ref, group):
        @pl.when(has_right)
        def _():
            copy(ref, right, send_sem.at[me, group], me, group).start()

    def send_both(ref, group):
        send_left(ref, group)
        send_right(ref, group)

    def hop(source, target, device, index, semaphore):
        return pltpu.make_async_remote_copy(
            src_ref=source,
            dst_ref=target,
            send_sem=detour_send.at[index],
            recv_sem=semaphore,
            device_id=device,
            device_id_type=MESH,
        )

    def lead(helper):
        source = part(last, (helper - 1) * DETOUR_ROWS, DETOUR_ROWS, me)
        line = {"shift": 0 * shift + helper}
        return hop(source, detour, line, helper - 1, detour_recv.at[0])

    def lift():
        return hop(detour, detour, left, 0, detour_recv.at[0])

    def land():
        target = part(last, (shift - 1) * DETOUR_ROWS, DETOUR_ROWS, me + 1)
        return hop(detour, target, {"shift": 0 * shift}, 0, recv_sem.at[1, side_group])

    def send_aside():
        ref = part(*groups[side_group], me)
        send_right(ref, side_group)

        @pl.when(jnp.logical_not(leads))
        def _():
            send_left(ref, side_group)

        @pl.when(leads)
        def _():
            for helper in helpers:
                lead(helper).start()

        @pl.when(lifts)
        def _():
            lift().wait_recv()
            lift().start()

    def open_right(rows):
        @pl.when(has_right)
        def _():
            pl.semaphore_wait(told_sem, 1)

        send_right(part(0, 0, rows, me), 0)

    def finish(array):
        if array == 0:
            rows = held[0].shape[1]
            if rows > LANES:
                send_left(part(0, rows - LANES, LANES, me), 0)
            if early:
                send_right(part(0, early, rows - early, me), 0)
            else:
                open_right(rows)
        else:
            send_both(part(*groups[array], me), array)

    for one in opening:
        one.wait()
    compute(0, 0)

    send_left(part(0, 0, LANES, me), 0)

    def exchange(side):
        return pltpu.make_async_remote_copy(
            src_ref=norm_out.at[me, side],
            dst_ref=norm_out.at[me, side],
            send_sem=pair_sem.at[0],
            recv_sem=pair_sem.at[1],
            device_id=partner,
            device_id_type=MESH,
        )

    early = (EARLY_PIECES - 1) * LANES if width > EARLY_PIECES * LANES else 0

    for array in range(len(outs)):
        for one in rest_of[array]:
            one.wait()
        count = held[array].shape[1] // LANES
        if array:
            compute(array, 0)
            finish(array - 1)
        if array == 1:
            for one in norm_loads:
                one.wait()
            norm_out[me, core] = copied[12][...] + copied[13][...]
        begin = 1
        if array == 0 and count > 1:
            compute(0, 1)
            begin = 2

        def step(c, carry, array=array):
            compute(array, c)
            if array == 0:
                send_left(part(0, (c - 1) * LANES, LANES, me), 0)
            return carry

        if array == 0 and early:
            lax.fori_loop(begin, EARLY_PIECES, step, 0)
            open_right(early)
            begin = EARLY_PIECES
        lax.fori_loop(begin, count, step, 0)
    exchange(core).start()
    if tail >= LANES:
        finish(last)
    exchange(core).wait_send()
    exchange(1 - core).wait_recv()
    if tail < LANES:
        finish(last)
    if tail:

        @pl.when(core != LATE_CORE)
        def _():
            send_both(part(*groups[late_group], me), late_group)

    send_both(part(*groups[norm_group], me), norm_group)
    if aside:
        send_aside()

    def each_group(act):
        for group in range(len(groups)):
            if group == late_group:

                @pl.when(core != LATE_CORE)
                def _(group=group):
                    act(group)
            else:
                act(group)

    def relay(k, carry):
        from_left, from_right = me - k, me + k

        def pass_on(group):
            @pl.when(from_left >= 0)
            def _():
                forward(group, from_left).wait_recv()

                @pl.when(has_right)
                def _():
                    forward(group, from_left).start()

            @pl.when(from_right < n)
            def _():
                backward(group, from_right).wait_recv()

                @pl.when(has_left)
                def _():
                    backward(group, from_right).start()

        each_group(pass_on)
        if aside:

            @pl.when(jnp.logical_and(lands, k == 1))
            def _():
                lift().wait_recv()
                land().start()

        return carry

    lax.fori_loop(1, n, relay, 0)

    def own_sent(group):
        @pl.when(has_right)
        def _():
            forward(group, me).wait_send()

        goes_left = has_left
        if group == side_group:
            goes_left = jnp.logical_and(has_left, jnp.logical_not(leads))

        @pl.when(goes_left)
        def _():
            backward(group, me, own=True).wait_send()

    each_group(own_sent)
    if aside:

        @pl.when(leads)
        def _():
            for helper in helpers:
                lead(helper).wait_send()

        @pl.when(lifts)
        def _():
            lift().wait_send()

        @pl.when(jnp.logical_and(lands, n > 1))
        def _():
            land().wait_send()

    def drain(k, carry):
        def sent(group):
            @pl.when(jnp.logical_and(me - k >= 0, has_right))
            def _():
                forward(group, me - k).wait_send()

            @pl.when(jnp.logical_and(me + k < n, has_left))
            def _():
                backward(group, me + k).wait_send()

        each_group(sent)
        return carry

    lax.fori_loop(1, n, drain, 0)


def body(n, shifts, *refs):
    kernel(n, shifts, refs[:14], refs[14:18], refs[18], refs[19:33], *refs[33:])


def store(n, cores, *refs):
    gathered, norm_ref, outs, norm_out, flat, rounded, sem, mixed_sem, norm_sem = (
        refs[:4],
        refs[4],
        refs[5:9],
        *refs[9:],
    )
    me, core = lax.axis_index("shard"), lax.axis_index("width")
    copies = []
    for source, out in zip(gathered[:3], outs[:3]):
        for row in range(0, source.shape[0], COPY_ROWS):
            rows = pl.ds(row, min(COPY_ROWS, source.shape[0] - row))
            copies.append(
                pltpu.make_async_copy(source.at[rows], out.at[rows], sem.at[len(copies)])
            )

    block = gathered[3].shape[0] // n
    tail = late_rows(block)

    def mixed(origin, row, size, part):
        rows = pl.ds(origin * block + row, size)
        return pltpu.make_async_copy(
            gathered[3].at[rows], outs[3].at[rows], mixed_sem.at[origin, part]
        )

    copies += [mixed(origin, 0, block - tail, 0) for origin in range(n)]

    def each_last(act):
        for origin in range(n if tail else 0):

            @pl.when(jnp.logical_or(core != LATE_CORE, me == origin))
            def _(origin=origin):
                act(mixed(origin, block - tail, tail, 1))

    for copy in copies:
        copy.start()
    each_last(lambda copy: copy.start())
    rows = norm_ref.shape[2]
    for origin in range(n):
        for side in range(cores):
            flat[pl.ds((origin * cores + side) * rows, rows)] = norm_ref[origin, side]
    rounded[...] = flat[...].astype(norm_out.dtype)
    norm_copy = pltpu.make_async_copy(rounded, norm_out, norm_sem)
    norm_copy.start()
    for copy in copies:
        copy.wait()
    each_last(lambda copy: copy.wait())
    norm_copy.wait()


def late(n, mixed, after, out, send_sem, recv_sem, told_sem):
    me = lax.axis_index("shard")
    core = lax.axis_index("width")
    has_left, has_right = me > 0, me < n - 1
    left, right = {"shard": me - 1}, {"shard": me + 1}
    block = mixed.shape[0] // n
    tail = late_rows(block)
    size = tail // LATE_STEPS

    def copy(origin, begin, rows, step, device, semaphore, own):
        first = pl.multiple_of(me * block + block - tail + begin, 16)
        dst = out.at[origin, pl.ds(pl.multiple_of(begin, 16), rows)]
        return pltpu.make_async_remote_copy(
            src_ref=mixed.at[pl.ds(first, rows)] if own else dst,
            dst_ref=dst,
            send_sem=send_sem.at[semaphore],
            recv_sem=recv_sem.at[origin, step],
            device_id=device,
            device_id_type=MESH,
        )

    def forward(origin, step, own=False):
        return copy(origin, step * size, size, step, right, origin, own)

    def backward(origin, step, own=False):
        return copy(origin, step * size, size, step, left, n if own else origin, own)

    def sent(origin, semaphore):
        copy(origin, 0, tail, 0, right, semaphore, True).wait_send()

    @pl.when(core == LATE_CORE)
    def _():
        barrier = pltpu.get_barrier_semaphore()

        @pl.when(has_right)
        def _():
            pl.semaphore_signal(barrier, inc=1, device_id=right, device_id_type=MESH)

        @pl.when(has_left)
        def _():
            pl.semaphore_wait(barrier, 1)
            for step in range(LATE_STEPS):
                backward(me, step, own=True).start()
            pl.semaphore_signal(told_sem, inc=1, device_id=left, device_id_type=MESH)

        @pl.when(has_right)
        def _():
            pl.semaphore_wait(told_sem, 1)
            for step in range(LATE_STEPS):
                forward(me, step, own=True).start()

        def relay(k, carry):
            for step in range(LATE_STEPS):

                @pl.when(me - k >= 0)
                def _(step=step):
                    forward(me - k, step).wait_recv()

                    @pl.when(has_right)
                    def _():
                        forward(me - k, step).start()

                @pl.when(me + k < n)
                def _(step=step):
                    backward(me + k, step).wait_recv()

                    @pl.when(has_left)
                    def _():
                        backward(me + k, step).start()

            return carry

        lax.fori_loop(1, n, relay, 0)

        @pl.when(has_right)
        def _():
            sent(me, me)

        @pl.when(has_left)
        def _():
            sent(me, n)

        def drain(k, carry):
            @pl.when(jnp.logical_and(me - k >= 0, has_right))
            def _():
                sent(me - k, me - k)

            @pl.when(jnp.logical_and(me + k < n, has_left))
            def _():
                sent(me + k, me + k)

            return carry

        lax.fori_loop(1, n, drain, 0)


def store_late(n, pieces, given, out, sem):
    me, core = lax.axis_index("shard"), lax.axis_index("width")
    block = out.shape[0] // n
    tail = late_rows(block)

    def each(act):
        for origin in range(n):

            @pl.when(jnp.logical_and(core == LATE_CORE, me != origin))
            def _(origin=origin):
                act(origin)

    def begin(origin):
        for row in range(0, tail, STORE_ROWS):
            rows = pl.ds((origin + 1) * block - tail + row, STORE_ROWS)
            source = pieces.at[origin, pl.ds(row, STORE_ROWS)]
            pltpu.make_async_copy(source, out.at[rows], sem.at[origin]).start()

    def end(origin):
        rows = pl.ds((origin + 1) * block - tail, tail)
        pltpu.make_async_copy(pieces.at[origin], out.at[rows], sem.at[origin]).wait()

    each(begin)
    each(end)


def on_device(n, cores, shifts, *args):
    weights, (norm_train, norm_step) = list(args[:12]), args[12:]
    bases = weights[0::3]
    (size,) = norm_train.shape
    sizes = [size, *(size for w in bases for size in w.shape)]
    if cores != 2 or any(size % LANES for size in sizes):
        return plain(*args)
    rows = size // LANES
    shapes = [(w.shape[1], w.shape[0] * n) for w in bases[:3]]
    shapes.append((bases[3].shape[1] * n, bases[3].shape[0]))
    in_hbm = pl.BlockSpec(memory_space=pltpu.HBM)
    in_vmem = pl.BlockSpec(memory_space=pltpu.VMEM)
    tail = late_rows(bases[3].shape[1])
    helpers = detours(shifts)
    groups = len(bases) + (2 if tail else 1) + (1 if helpers else 0)
    weights[1::3] = [low.T for low in weights[1::3]]
    norms = [norm_train.reshape(rows, LANES), norm_step.reshape(rows, LANES)]
    given = [pltpu.with_memory_space_constraint(array, pltpu.HBM) for array in weights + norms]
    gathered = pl.pallas_call(
        functools.partial(body, n, shifts),
        out_shape=[pltpu.VMEM(shape, jnp.bfloat16) for shape in shapes]
        + [pltpu.VMEM((n, cores, rows, LANES), jnp.float32)],
        in_specs=[in_hbm] * 14,
        out_specs=[in_vmem] * 5,
        scratch_shapes=[pltpu.VMEM(array.shape, array.dtype) for array in given]
        + [
            pltpu.SemaphoreType.DMA((15 + bases[0].shape[0] // LANES,)),
            pltpu.SemaphoreType.DMA((n, groups)),
            pltpu.SemaphoreType.DMA((groups,)),
            pltpu.SemaphoreType.DMA((n, groups)),
            pltpu.SemaphoreType.DMA((2,)),
            pltpu.SemaphoreType.REGULAR,
            pltpu.VMEM((DETOUR_ROWS, shapes[3][1]), jnp.bfloat16),
            pltpu.SemaphoreType.DMA((max(helpers, 1),)),
            pltpu.SemaphoreType.DMA((1,)),
        ],
        compiler_params=pltpu.CompilerParams(
            collective_id=0, has_side_effects=True, vmem_limit_bytes=40 * 2**20
        ),
        name="merge_gather",
    )(*given)
    norm_rows = n * cores * rows
    *finals, norm = pl.pallas_call(
        functools.partial(store, n, cores),
        out_shape=[jax.ShapeDtypeStruct(shape, jnp.bfloat16) for shape in shapes]
        + [jax.ShapeDtypeStruct((norm_rows, LANES), jnp.bfloat16)],
        in_specs=[in_vmem] * 5,
        out_specs=[in_hbm] * 5,
        scratch_shapes=[
            pltpu.VMEM((norm_rows, LANES), jnp.float32),
            pltpu.VMEM((norm_rows, LANES), jnp.bfloat16),
            pltpu.SemaphoreType.DMA((sum(-(-shape[0] // COPY_ROWS) for shape in shapes[:3]),)),
            pltpu.SemaphoreType.DMA((n, 2)),
            pltpu.SemaphoreType.DMA,
        ],
        compiler_params=pltpu.CompilerParams(vmem_limit_bytes=20 * 2**20),
        name="store",
    )(*gathered)
    norm = norm.reshape(-1)
    if not tail:
        return (*finals, norm)
    columns = shapes[3][1]
    pieces = pl.pallas_call(
        functools.partial(late, n),
        out_shape=pltpu.VMEM((n, tail, columns), jnp.bfloat16),
        in_specs=[in_vmem, in_hbm],
        out_specs=in_vmem,
        scratch_shapes=[
            pltpu.SemaphoreType.DMA((n + 1,)),
            pltpu.SemaphoreType.DMA((n, LATE_STEPS)),
            pltpu.SemaphoreType.REGULAR,
        ],
        compiler_params=pltpu.CompilerParams(
            collective_id=1, has_side_effects=True, vmem_limit_bytes=20 * 2**20
        ),
        name="late",
    )(gathered[3], pltpu.with_memory_space_constraint(finals[3], pltpu.HBM))
    finals[3] = pl.pallas_call(
        functools.partial(store_late, n),
        out_shape=jax.ShapeDtypeStruct(shapes[3], jnp.bfloat16),
        in_specs=[in_vmem, in_hbm],
        out_specs=in_hbm,
        input_output_aliases={1: 0},
        scratch_shapes=[pltpu.SemaphoreType.DMA((n,))],
        compiler_params=pltpu.CompilerParams(vmem_limit_bytes=20 * 2**20),
        name="store_late",
    )(pieces, finals[3])
    return (*finals, norm)


def solution(mesh):
    placed = (
        P(("shift", "shard"), "width"),
        P(("shift", "shard"), None),
        P("shift", "width"),
        P(("shift", "shard"), "width"),
        P(("shift", "shard"), None),
        P("shift", "width"),
        P(("shift", "shard"), "width"),
        P(("shift", "shard"), None),
        P("shift", "width"),
        P(("shift", "width"), "shard"),
        P(("shift", "width"), None),
        P("shift", "shard"),
        P(("shift", "shard", "width")),
        P(("shift", "shard", "width")),
    )
    return jax.shard_map(
        functools.partial(
            on_device, mesh.shape["shard"], mesh.shape["width"], mesh.shape["shift"]
        ),
        mesh=mesh,
        in_specs=placed,
        out_specs=(
            P(("shift", "width"), None),
            P(("shift", "width"), None),
            P(("shift", "width"), None),
            P("shift", "width"),
            P("shift"),
        ),
        check_vma=False,
    )
```

```python
import functools

import jax
import jax.numpy as jnp
from jax import lax
from jax.experimental import pallas as pl
from jax.experimental.pallas import tpu as pltpu
from jax.sharding import PartitionSpec as P

mix_rate = 0.5
MESH = pl.DeviceIdType.MESH
LANES = 128
COPY_ROWS = 256
LATE_STEPS = 2
LATE_CORE = 1
LATE_ROWS = 128
ROW_UNIT = 16
DETOURS = 2
DETOUR_ROWS = 16
EARLY_PIECES = 3
STORE_ROWS = 64


def plain(
    w_query,
    low_query,
    high_query,
    w_key,
    low_key,
    high_key,
    w_value,
    low_value,
    high_value,
    w_mixed,
    low_mixed,
    high_mixed,
    norm_train,
    norm_step,
):
    def merged(w, low, high):
        low_rank = jnp.dot(low, high, preferred_element_type=jnp.float32)
        return (w.astype(jnp.float32) + mix_rate * low_rank).astype(jnp.bfloat16)

    query = lax.all_gather(merged(w_query, low_query, high_query), "shard", axis=0, tiled=True)
    key = lax.all_gather(merged(w_key, low_key, high_key), "shard", axis=0, tiled=True)
    value = lax.all_gather(merged(w_value, low_value, high_value), "shard", axis=0, tiled=True)
    mixed = lax.all_gather(merged(w_mixed, low_mixed, high_mixed), "shard", axis=1, tiled=True)
    norm = lax.all_gather(
        (norm_train + norm_step).astype(jnp.bfloat16), ("shard", "width"), axis=0, tiled=True
    )
    return query.T, key.T, value.T, mixed.T, norm


def detours(shifts):
    return min(DETOURS, shifts - 1)


def short_rows(depth):
    rows = LANES * LANES // depth
    return rows if rows * depth == LANES * LANES and rows % ROW_UNIT == 0 and rows < LANES else 0


def late_rows(block):
    return LATE_ROWS if block > LATE_ROWS else 0


def kernel(
    n,
    shifts,
    given,
    outs,
    norm_out,
    copied,
    load_sem,
    send_sem,
    back_sem,
    recv_sem,
    pair_sem,
    told_sem,
    detour,
    detour_send,
    detour_recv,
    raw,
    raw_low,
    raw_send,
    raw_recv,
):
    me, shift = lax.axis_index("shard"), lax.axis_index("shift")
    core = lax.axis_index("width")
    has_left, has_right = me > 0, me < n - 1
    left, right = {"shard": me - 1}, {"shard": me + 1}
    partner = {"width": 1 - core}
    helpers = range(1, 1 + detours(shifts))
    aside = len(helpers) * DETOUR_ROWS

    def on_early(*conditions):
        return functools.reduce(jnp.logical_and, conditions, core != LATE_CORE)

    helps = jnp.logical_and(shift >= 1, shift <= len(helpers))
    leads, ends = on_early(shift == 0, me == 1), on_early(shift == 0, me == 0)
    lifts, lands = on_early(helps, me == 1), on_early(helps, me == 0)
    held, low_refs, high_refs = copied[0:12:3], copied[1:12:3], copied[2:12:3]
    depth, width = held[0].shape
    first, rest = pl.ds(0, LANES), pl.ds(LANES, width - LANES)
    bands = [pl.ds(row, LANES) for row in range(0, depth, LANES)]
    loads = []

    def load(source, target):
        loads.append(pltpu.make_async_copy(source, target, load_sem.at[len(loads)]))
        return loads[-1]

    opening = [load(given[1], copied[1]), load(given[2].at[:, first], copied[2].at[:, first])]
    opening += [load(given[0].at[rows, first], held[0].at[rows, first]) for rows in bands]
    others = []
    if width > LANES:
        others = [load(given[i].at[:, rest], copied[i].at[:, rest]) for i in (2, 0)]
    rest_of = [others] + [
        [load(given[i], copied[i]) for i in range(array, array + 3)] for array in (3, 6, 9)
    ]
    norm_loads = [load(given[i], copied[i]) for i in (12, 13)]
    for one in opening:
        one.start()

    barrier = pltpu.get_barrier_semaphore()
    pl.semaphore_signal(barrier, inc=1, device_id=partner, device_id_type=MESH)

    @pl.when(has_right)
    def _():
        pl.semaphore_signal(barrier, inc=1, device_id=right, device_id_type=MESH)

    if aside:

        @pl.when(lifts)
        def _():
            line = {"shift": 0 * shift}
            pl.semaphore_signal(barrier, inc=1, device_id=line, device_id_type=MESH)

        @pl.when(ends)
        def _():
            for helper in helpers:
                line = {"shift": 0 * shift + helper}
                pl.semaphore_signal(barrier, inc=1, device_id=line, device_id_type=MESH)

    for one in loads[len(opening) :]:
        one.start()
    waited = 1 + has_left.astype(jnp.int32)
    if aside:
        waited += jnp.where(leads, len(helpers), 0) + lands.astype(jnp.int32)
    pl.semaphore_wait(barrier, waited)

    @pl.when(has_left)
    def _():
        pl.semaphore_signal(told_sem, inc=1, device_id=left, device_id_type=MESH)

    last = len(outs) - 1
    block = held[last].shape[1]
    tail = late_rows(block)
    groups = [(array, 0, w.shape[1]) for array, w in enumerate(held[:last])]
    groups.append((last, aside, block - tail - aside))
    if tail:
        groups.append((last, block - tail, tail))
    groups.append((len(outs), 0, 0))
    side_group = len(groups)
    if aside:
        groups.append((last, 0, aside))
    norm_group = len(outs) + (1 if tail else 0)
    late_group = norm_group - 1 if tail else -1

    def part(array, row, rows, origin, band=None):
        if array == len(outs):
            return norm_out.at[origin]
        out, w = outs[array], held[array]
        if array < last:
            first, size = band or (0, w.shape[0])
            begin = pl.multiple_of(origin * w.shape[0] + first, LANES)
            return out.at[pl.ds(pl.multiple_of(row, LANES), rows), pl.ds(begin, size)]
        begin = pl.multiple_of(origin * block + row, ROW_UNIT)
        return out.at[pl.ds(begin, rows)]

    def copy(ref, device, semaphore, origin, group):
        return pltpu.make_async_remote_copy(
            src_ref=ref,
            dst_ref=ref,
            send_sem=semaphore,
            recv_sem=recv_sem.at[origin, group],
            device_id=device,
            device_id_type=MESH,
        )

    short = short_rows(depth)
    corner = pl.ds(0, LANES)

    def raw_copies():
        pairs = ((held[0].at[corner, corner], raw), (low_refs[0].at[:, corner], raw_low))
        return [
            pltpu.make_async_remote_copy(
                src_ref=source,
                dst_ref=target,
                send_sem=raw_send.at[i],
                recv_sem=raw_recv.at[i],
                device_id=left,
                device_id_type=MESH,
            )
            for i, (source, target) in enumerate(pairs)
        ]

    def near_query():
        ref = part(0, 0, width - short, me)
        return copy(ref, left, back_sem.at[0], me + 1, 0)

    def forward(group, origin):
        ref = part(*groups[group], origin)
        return copy(ref, right, send_sem.at[origin, group], origin, group)

    def backward(group, origin, own=False):
        ref = part(*groups[group], origin)
        semaphore = back_sem.at[group] if own else send_sem.at[origin, group]
        return copy(ref, left, semaphore, origin, group)

    def compute(array, c):
        rows = pl.ds(pl.multiple_of(c * LANES, LANES), LANES)
        low_rank = lax.dot_general(
            high_refs[array][:, rows],
            low_refs[array][...],
            (((0,), (0,)), ((), ())),
            preferred_element_type=jnp.float32,
        )
        base = held[array][:, rows].T.astype(jnp.float32)
        part(array, c * LANES, LANES, me)[...] = (base + mix_rate * low_rank).astype(
            jnp.bfloat16
        )

    def send_left(ref, group):
        @pl.when(has_left)
        def _():
            copy(ref, left, back_sem.at[group], me, group).start()

    def send_right(ref, group):
        @pl.when(has_right)
        def _():
            copy(ref, right, send_sem.at[me, group], me, group).start()

    def send_both(ref, group):
        send_left(ref, group)
        send_right(ref, group)

    def hop(source, target, device, index, semaphore):
        return pltpu.make_async_remote_copy(
            src_ref=source,
            dst_ref=target,
            send_sem=detour_send.at[index],
            recv_sem=semaphore,
            device_id=device,
            device_id_type=MESH,
        )

    def lead(helper):
        source = part(last, (helper - 1) * DETOUR_ROWS, DETOUR_ROWS, me)
        line = {"shift": 0 * shift + helper}
        return hop(source, detour, line, helper - 1, detour_recv.at[0])

    def lift():
        return hop(detour, detour, left, 0, detour_recv.at[0])

    def land():
        target = part(last, (shift - 1) * DETOUR_ROWS, DETOUR_ROWS, me + 1)
        return hop(detour, target, {"shift": 0 * shift}, 0, recv_sem.at[1, side_group])

    def send_aside():
        ref = part(*groups[side_group], me)
        send_right(ref, side_group)

        @pl.when(jnp.logical_not(leads))
        def _():
            send_left(ref, side_group)

        @pl.when(leads)
        def _():
            for helper in helpers:
                lead(helper).start()

        @pl.when(lifts)
        def _():
            lift().wait_recv()
            lift().start()

    def open_right(rows):
        @pl.when(has_right)
        def _():
            pl.semaphore_wait(told_sem, 1)

        send_right(part(0, 0, rows, me), 0)

    def finish(array):
        if array == 0:
            rows = held[0].shape[1]
            if rows > LANES:
                send_left(part(0, rows - LANES, LANES, me), 0)
            if early:
                send_right(part(0, early, rows - early, me), 0)
            else:
                open_right(rows)
        else:
            send_both(part(*groups[array], me), array)

    opening[0].wait()
    opening[2].wait()
    if short:

        @pl.when(has_left)
        def _():
            for one in raw_copies():
                one.start()

    for one in opening[1:2] + opening[3:]:
        one.wait()
    compute(0, 0)
    send_left(part(0, 0, LANES, me, (LANES, depth - LANES) if short else None), 0)

    def exchange(side):
        return pltpu.make_async_remote_copy(
            src_ref=norm_out.at[me, side],
            dst_ref=norm_out.at[me, side],
            send_sem=pair_sem.at[0],
            recv_sem=pair_sem.at[1],
            device_id=partner,
            device_id_type=MESH,
        )

    early = (EARLY_PIECES - 1) * LANES if width > EARLY_PIECES * LANES else 0

    for array in range(len(outs)):
        for one in rest_of[array]:
            one.wait()
        count = held[array].shape[1] // LANES
        if array:
            compute(array, 0)
            finish(array - 1)
        if array == 1:
            for one in norm_loads:
                one.wait()
            norm_out[me, core] = copied[12][...] + copied[13][...]
        begin = 1
        if array == 0 and count > 1:
            compute(0, 1)
            begin = 2

        def step(c, carry, array=array):
            compute(array, c)
            if array == 0:
                send_left(part(0, (c - 1) * LANES, LANES, me), 0)
            return carry

        if array == 0 and early:
            lax.fori_loop(begin, EARLY_PIECES, step, 0)
            open_right(early)
            begin = EARLY_PIECES
        lax.fori_loop(begin, count, step, 0)
    exchange(core).start()
    if tail >= LANES:
        finish(last)
    exchange(core).wait_send()
    exchange(1 - core).wait_recv()
    if tail < LANES:
        finish(last)
    if tail:

        @pl.when(core != LATE_CORE)
        def _():
            send_both(part(*groups[late_group], me), late_group)

    send_both(part(*groups[norm_group], me), norm_group)
    if aside:
        send_aside()

    if short:

        @pl.when(has_right)
        def _():
            for one in raw_copies():
                one.wait_recv()
            low_rank = lax.dot_general(
                high_refs[0][:, corner],
                raw_low[...],
                (((0,), (0,)), ((), ())),
                preferred_element_type=jnp.float32,
            )
            base = raw[...].T.astype(jnp.float32)
            part(0, 0, LANES, me + 1, (0, LANES))[...] = (base + mix_rate * low_rank).astype(
                jnp.bfloat16
            )

    def each_group(act):
        for group in range(len(groups)):
            if group == late_group:

                @pl.when(core != LATE_CORE)
                def _(group=group):
                    act(group)
            else:
                act(group)

    def relay(k, carry):
        from_left, from_right = me - k, me + k

        def pass_on(group):
            @pl.when(from_left >= 0)
            def _():
                forward(group, from_left).wait_recv()

                @pl.when(has_right)
                def _():
                    forward(group, from_left).start()

            @pl.when(from_right < n)
            def _():
                if group == 0 and short:

                    @pl.when(k == 1)
                    def _():
                        near_query().wait_recv()

                    @pl.when(k > 1)
                    def _():
                        backward(group, from_right).wait_recv()
                else:
                    backward(group, from_right).wait_recv()

                @pl.when(has_left)
                def _():
                    backward(group, from_right).start()

        each_group(pass_on)
        if aside:

            @pl.when(jnp.logical_and(lands, k == 1))
            def _():
                lift().wait_recv()
                land().start()

        return carry

    lax.fori_loop(1, n, relay, 0)

    def own_sent(group):
        @pl.when(has_right)
        def _():
            forward(group, me).wait_send()

        goes_left = has_left
        if group == side_group:
            goes_left = jnp.logical_and(has_left, jnp.logical_not(leads))

        @pl.when(goes_left)
        def _():
            if group == 0 and short:
                near_query().wait_send()
            else:
                backward(group, me, own=True).wait_send()

    each_group(own_sent)
    if short:

        @pl.when(has_left)
        def _():
            for one in raw_copies():
                one.wait_send()
    if aside:

        @pl.when(leads)
        def _():
            for helper in helpers:
                lead(helper).wait_send()

        @pl.when(lifts)
        def _():
            lift().wait_send()

        @pl.when(jnp.logical_and(lands, n > 1))
        def _():
            land().wait_send()

    def drain(k, carry):
        def sent(group):
            @pl.when(jnp.logical_and(me - k >= 0, has_right))
            def _():
                forward(group, me - k).wait_send()

            @pl.when(jnp.logical_and(me + k < n, has_left))
            def _():
                backward(group, me + k).wait_send()

        each_group(sent)
        return carry

    lax.fori_loop(1, n, drain, 0)


def body(n, shifts, *refs):
    kernel(n, shifts, refs[:14], refs[14:18], refs[18], refs[19:33], *refs[33:])


def store(n, cores, *refs):
    gathered, norm_ref, outs, norm_out, flat, rounded, sem, mixed_sem, norm_sem = (
        refs[:4],
        refs[4],
        refs[5:9],
        *refs[9:],
    )
    me, core = lax.axis_index("shard"), lax.axis_index("width")
    copies = []
    for source, out in zip(gathered[:3], outs[:3]):
        for row in range(0, source.shape[0], COPY_ROWS):
            rows = pl.ds(row, min(COPY_ROWS, source.shape[0] - row))
            copies.append(
                pltpu.make_async_copy(source.at[rows], out.at[rows], sem.at[len(copies)])
            )

    block = gathered[3].shape[0] // n
    tail = late_rows(block)

    def mixed(origin, row, size, part):
        rows = pl.ds(origin * block + row, size)
        return pltpu.make_async_copy(
            gathered[3].at[rows], outs[3].at[rows], mixed_sem.at[origin, part]
        )

    copies += [mixed(origin, 0, block - tail, 0) for origin in range(n)]

    def each_last(act):
        for origin in range(n if tail else 0):

            @pl.when(jnp.logical_or(core != LATE_CORE, me == origin))
            def _(origin=origin):
                act(mixed(origin, block - tail, tail, 1))

    for copy in copies:
        copy.start()
    each_last(lambda copy: copy.start())
    rows = norm_ref.shape[2]
    for origin in range(n):
        for side in range(cores):
            flat[pl.ds((origin * cores + side) * rows, rows)] = norm_ref[origin, side]
    rounded[...] = flat[...].astype(norm_out.dtype)
    norm_copy = pltpu.make_async_copy(rounded, norm_out, norm_sem)
    norm_copy.start()
    for copy in copies:
        copy.wait()
    each_last(lambda copy: copy.wait())
    norm_copy.wait()


def late(n, mixed, after, out, send_sem, recv_sem, told_sem):
    me = lax.axis_index("shard")
    core = lax.axis_index("width")
    has_left, has_right = me > 0, me < n - 1
    left, right = {"shard": me - 1}, {"shard": me + 1}
    block = mixed.shape[0] // n
    tail = late_rows(block)
    size = tail // LATE_STEPS

    def copy(origin, begin, rows, step, device, semaphore, own):
        first = pl.multiple_of(me * block + block - tail + begin, 16)
        dst = out.at[origin, pl.ds(pl.multiple_of(begin, 16), rows)]
        return pltpu.make_async_remote_copy(
            src_ref=mixed.at[pl.ds(first, rows)] if own else dst,
            dst_ref=dst,
            send_sem=send_sem.at[semaphore],
            recv_sem=recv_sem.at[origin, step],
            device_id=device,
            device_id_type=MESH,
        )

    def forward(origin, step, own=False):
        return copy(origin, step * size, size, step, right, origin, own)

    def backward(origin, step, own=False):
        return copy(origin, step * size, size, step, left, n if own else origin, own)

    def sent(origin, semaphore):
        copy(origin, 0, tail, 0, right, semaphore, True).wait_send()

    @pl.when(core == LATE_CORE)
    def _():
        barrier = pltpu.get_barrier_semaphore()

        @pl.when(has_right)
        def _():
            pl.semaphore_signal(barrier, inc=1, device_id=right, device_id_type=MESH)

        @pl.when(has_left)
        def _():
            pl.semaphore_wait(barrier, 1)
            for step in range(LATE_STEPS):
                backward(me, step, own=True).start()
            pl.semaphore_signal(told_sem, inc=1, device_id=left, device_id_type=MESH)

        @pl.when(has_right)
        def _():
            pl.semaphore_wait(told_sem, 1)
            for step in range(LATE_STEPS):
                forward(me, step, own=True).start()

        def relay(k, carry):
            for step in range(LATE_STEPS):

                @pl.when(me - k >= 0)
                def _(step=step):
                    forward(me - k, step).wait_recv()

                    @pl.when(has_right)
                    def _():
                        forward(me - k, step).start()

                @pl.when(me + k < n)
                def _(step=step):
                    backward(me + k, step).wait_recv()

                    @pl.when(has_left)
                    def _():
                        backward(me + k, step).start()

            return carry

        lax.fori_loop(1, n, relay, 0)

        @pl.when(has_right)
        def _():
            sent(me, me)

        @pl.when(has_left)
        def _():
            sent(me, n)

        def drain(k, carry):
            @pl.when(jnp.logical_and(me - k >= 0, has_right))
            def _():
                sent(me - k, me - k)

            @pl.when(jnp.logical_and(me + k < n, has_left))
            def _():
                sent(me + k, me + k)

            return carry

        lax.fori_loop(1, n, drain, 0)


def store_late(n, pieces, given, out, sem):
    me, core = lax.axis_index("shard"), lax.axis_index("width")
    block = out.shape[0] // n
    tail = late_rows(block)

    def each(act):
        for origin in range(n):

            @pl.when(jnp.logical_and(core == LATE_CORE, me != origin))
            def _(origin=origin):
                act(origin)

    def begin(origin):
        for row in range(0, tail, STORE_ROWS):
            rows = pl.ds((origin + 1) * block - tail + row, STORE_ROWS)
            source = pieces.at[origin, pl.ds(row, STORE_ROWS)]
            pltpu.make_async_copy(source, out.at[rows], sem.at[origin]).start()

    def end(origin):
        rows = pl.ds((origin + 1) * block - tail, tail)
        pltpu.make_async_copy(pieces.at[origin], out.at[rows], sem.at[origin]).wait()

    each(begin)
    each(end)


def on_device(n, cores, shifts, *args):
    weights, (norm_train, norm_step) = list(args[:12]), args[12:]
    bases = weights[0::3]
    (size,) = norm_train.shape
    sizes = [size, *(size for w in bases for size in w.shape)]
    if cores != 2 or any(size % LANES for size in sizes):
        return plain(*args)
    rows = size // LANES
    shapes = [(w.shape[1], w.shape[0] * n) for w in bases[:3]]
    shapes.append((bases[3].shape[1] * n, bases[3].shape[0]))
    in_hbm = pl.BlockSpec(memory_space=pltpu.HBM)
    in_vmem = pl.BlockSpec(memory_space=pltpu.VMEM)
    tail = late_rows(bases[3].shape[1])
    helpers = detours(shifts)
    groups = len(bases) + (2 if tail else 1) + (1 if helpers else 0)
    weights[1::3] = [low.T for low in weights[1::3]]
    norms = [norm_train.reshape(rows, LANES), norm_step.reshape(rows, LANES)]
    given = [pltpu.with_memory_space_constraint(array, pltpu.HBM) for array in weights + norms]
    gathered = pl.pallas_call(
        functools.partial(body, n, shifts),
        out_shape=[pltpu.VMEM(shape, jnp.bfloat16) for shape in shapes]
        + [pltpu.VMEM((n, cores, rows, LANES), jnp.float32)],
        in_specs=[in_hbm] * 14,
        out_specs=[in_vmem] * 5,
        scratch_shapes=[pltpu.VMEM(array.shape, array.dtype) for array in given]
        + [
            pltpu.SemaphoreType.DMA((15 + bases[0].shape[0] // LANES,)),
            pltpu.SemaphoreType.DMA((n, groups)),
            pltpu.SemaphoreType.DMA((groups,)),
            pltpu.SemaphoreType.DMA((n, groups)),
            pltpu.SemaphoreType.DMA((2,)),
            pltpu.SemaphoreType.REGULAR,
            pltpu.VMEM((DETOUR_ROWS, shapes[3][1]), jnp.bfloat16),
            pltpu.SemaphoreType.DMA((max(helpers, 1),)),
            pltpu.SemaphoreType.DMA((1,)),
            pltpu.VMEM((LANES, LANES), jnp.bfloat16),
            pltpu.VMEM((given[1].shape[0], LANES), jnp.bfloat16),
            pltpu.SemaphoreType.DMA((2,)),
            pltpu.SemaphoreType.DMA((2,)),
        ],
        compiler_params=pltpu.CompilerParams(
            collective_id=0, has_side_effects=True, vmem_limit_bytes=40 * 2**20
        ),
        name="merge_gather",
    )(*given)
    norm_rows = n * cores * rows
    *finals, norm = pl.pallas_call(
        functools.partial(store, n, cores),
        out_shape=[jax.ShapeDtypeStruct(shape, jnp.bfloat16) for shape in shapes]
        + [jax.ShapeDtypeStruct((norm_rows, LANES), jnp.bfloat16)],
        in_specs=[in_vmem] * 5,
        out_specs=[in_hbm] * 5,
        scratch_shapes=[
            pltpu.VMEM((norm_rows, LANES), jnp.float32),
            pltpu.VMEM((norm_rows, LANES), jnp.bfloat16),
            pltpu.SemaphoreType.DMA((sum(-(-shape[0] // COPY_ROWS) for shape in shapes[:3]),)),
            pltpu.SemaphoreType.DMA((n, 2)),
            pltpu.SemaphoreType.DMA,
        ],
        compiler_params=pltpu.CompilerParams(vmem_limit_bytes=20 * 2**20),
        name="store",
    )(*gathered)
    norm = norm.reshape(-1)
    if not tail:
        return (*finals, norm)
    columns = shapes[3][1]
    pieces = pl.pallas_call(
        functools.partial(late, n),
        out_shape=pltpu.VMEM((n, tail, columns), jnp.bfloat16),
        in_specs=[in_vmem, in_hbm],
        out_specs=in_vmem,
        scratch_shapes=[
            pltpu.SemaphoreType.DMA((n + 1,)),
            pltpu.SemaphoreType.DMA((n, LATE_STEPS)),
            pltpu.SemaphoreType.REGULAR,
        ],
        compiler_params=pltpu.CompilerParams(
            collective_id=1, has_side_effects=True, vmem_limit_bytes=20 * 2**20
        ),
        name="late",
    )(gathered[3], pltpu.with_memory_space_constraint(finals[3], pltpu.HBM))
    finals[3] = pl.pallas_call(
        functools.partial(store_late, n),
        out_shape=jax.ShapeDtypeStruct(shapes[3], jnp.bfloat16),
        in_specs=[in_vmem, in_hbm],
        out_specs=in_hbm,
        input_output_aliases={1: 0},
        scratch_shapes=[pltpu.SemaphoreType.DMA((n,))],
        compiler_params=pltpu.CompilerParams(vmem_limit_bytes=20 * 2**20),
        name="store_late",
    )(pieces, finals[3])
    return (*finals, norm)


def solution(mesh):
    placed = (
        P(("shift", "shard"), "width"),
        P(("shift", "shard"), None),
        P("shift", "width"),
        P(("shift", "shard"), "width"),
        P(("shift", "shard"), None),
        P("shift", "width"),
        P(("shift", "shard"), "width"),
        P(("shift", "shard"), None),
        P("shift", "width"),
        P(("shift", "width"), "shard"),
        P(("shift", "width"), None),
        P("shift", "shard"),
        P(("shift", "shard", "width")),
        P(("shift", "shard", "width")),
    )
    return jax.shard_map(
        functools.partial(
            on_device, mesh.shape["shard"], mesh.shape["width"], mesh.shape["shift"]
        ),
        mesh=mesh,
        in_specs=placed,
        out_specs=(
            P(("shift", "width"), None),
            P(("shift", "width"), None),
            P(("shift", "width"), None),
            P("shift", "width"),
            P("shift"),
        ),
        check_vma=False,
    )
```

```python
import functools

import jax
import jax.numpy as jnp
from jax import lax
from jax.experimental import pallas as pl
from jax.experimental.pallas import tpu as pltpu
from jax.sharding import PartitionSpec as P

mix_rate = 0.5
MESH = pl.DeviceIdType.MESH
LANES = 128
COPY_ROWS = 256
LATE_STEPS = 2
LATE_CORE = 1
LATE_ROWS = 160
ROW_UNIT = 16
DETOURS = 2
DETOUR_ROWS = 16
EARLY_PIECES = 3
STORE_ROWS = 32


def plain(
    w_query,
    low_query,
    high_query,
    w_key,
    low_key,
    high_key,
    w_value,
    low_value,
    high_value,
    w_mixed,
    low_mixed,
    high_mixed,
    norm_train,
    norm_step,
):
    def merged(w, low, high):
        low_rank = jnp.dot(low, high, preferred_element_type=jnp.float32)
        return (w.astype(jnp.float32) + mix_rate * low_rank).astype(jnp.bfloat16)

    query = lax.all_gather(merged(w_query, low_query, high_query), "shard", axis=0, tiled=True)
    key = lax.all_gather(merged(w_key, low_key, high_key), "shard", axis=0, tiled=True)
    value = lax.all_gather(merged(w_value, low_value, high_value), "shard", axis=0, tiled=True)
    mixed = lax.all_gather(merged(w_mixed, low_mixed, high_mixed), "shard", axis=1, tiled=True)
    norm = lax.all_gather(
        (norm_train + norm_step).astype(jnp.bfloat16), ("shard", "width"), axis=0, tiled=True
    )
    return query.T, key.T, value.T, mixed.T, norm


def detours(shifts):
    return min(DETOURS, shifts - 1)


def short_rows(depth):
    rows = LANES * LANES // depth
    return rows if rows * depth == LANES * LANES and rows % ROW_UNIT == 0 and rows < LANES else 0


def late_rows(block):
    return LATE_ROWS if block > LATE_ROWS else 0


def kernel(
    n,
    shifts,
    given,
    outs,
    norm_out,
    copied,
    load_sem,
    send_sem,
    back_sem,
    recv_sem,
    pair_sem,
    told_sem,
    detour,
    detour_send,
    detour_recv,
    raw,
    raw_low,
    raw_send,
    raw_recv,
):
    me, shift = lax.axis_index("shard"), lax.axis_index("shift")
    core = lax.axis_index("width")
    has_left, has_right = me > 0, me < n - 1
    left, right = {"shard": me - 1}, {"shard": me + 1}
    partner = {"width": 1 - core}
    helpers = range(1, 1 + detours(shifts))
    aside = len(helpers) * DETOUR_ROWS

    def on_early(*conditions):
        return functools.reduce(jnp.logical_and, conditions, core != LATE_CORE)

    helps = jnp.logical_and(shift >= 1, shift <= len(helpers))
    leads, ends = on_early(shift == 0, me == 1), on_early(shift == 0, me == 0)
    lifts, lands = on_early(helps, me == 1), on_early(helps, me == 0)
    held, low_refs, high_refs = copied[0:12:3], copied[1:12:3], copied[2:12:3]
    depth, width = held[0].shape
    first, rest = pl.ds(0, LANES), pl.ds(LANES, width - LANES)
    bands = [pl.ds(row, LANES) for row in range(0, depth, LANES)]
    loads = []

    def load(source, target):
        loads.append(pltpu.make_async_copy(source, target, load_sem.at[len(loads)]))
        return loads[-1]

    opening = [load(given[1], copied[1]), load(given[2].at[:, first], copied[2].at[:, first])]
    opening += [load(given[0].at[rows, first], held[0].at[rows, first]) for rows in bands]
    others = []
    if width > LANES:
        others = [load(given[i].at[:, rest], copied[i].at[:, rest]) for i in (2, 0)]
    rest_of = [others] + [
        [load(given[i], copied[i]) for i in range(array, array + 3)] for array in (3, 6, 9)
    ]
    norm_loads = [load(given[i], copied[i]) for i in (12, 13)]
    for one in opening:
        one.start()

    barrier = pltpu.get_barrier_semaphore()
    pl.semaphore_signal(barrier, inc=1, device_id=partner, device_id_type=MESH)

    @pl.when(has_right)
    def _():
        pl.semaphore_signal(barrier, inc=1, device_id=right, device_id_type=MESH)

    if aside:

        @pl.when(lifts)
        def _():
            line = {"shift": 0 * shift}
            pl.semaphore_signal(barrier, inc=1, device_id=line, device_id_type=MESH)

        @pl.when(ends)
        def _():
            for helper in helpers:
                line = {"shift": 0 * shift + helper}
                pl.semaphore_signal(barrier, inc=1, device_id=line, device_id_type=MESH)

    for one in loads[len(opening) :]:
        one.start()
    waited = 1 + has_left.astype(jnp.int32)
    if aside:
        waited += jnp.where(leads, len(helpers), 0) + lands.astype(jnp.int32)
    pl.semaphore_wait(barrier, waited)

    @pl.when(has_left)
    def _():
        pl.semaphore_signal(told_sem, inc=1, device_id=left, device_id_type=MESH)

    last = len(outs) - 1
    block = held[last].shape[1]
    tail = late_rows(block)
    groups = [(array, 0, w.shape[1]) for array, w in enumerate(held[:last])]
    groups.append((last, aside, block - tail - aside))
    if tail:
        groups.append((last, block - tail, tail))
    groups.append((len(outs), 0, 0))
    side_group = len(groups)
    if aside:
        groups.append((last, 0, aside))
    norm_group = len(outs) + (1 if tail else 0)
    late_group = norm_group - 1 if tail else -1

    def part(array, row, rows, origin, band=None):
        if array == len(outs):
            return norm_out.at[origin]
        out, w = outs[array], held[array]
        if array < last:
            first, size = band or (0, w.shape[0])
            begin = pl.multiple_of(origin * w.shape[0] + first, LANES)
            return out.at[pl.ds(pl.multiple_of(row, LANES), rows), pl.ds(begin, size)]
        begin = pl.multiple_of(origin * block + row, ROW_UNIT)
        return out.at[pl.ds(begin, rows)]

    def copy(ref, device, semaphore, origin, group):
        return pltpu.make_async_remote_copy(
            src_ref=ref,
            dst_ref=ref,
            send_sem=semaphore,
            recv_sem=recv_sem.at[origin, group],
            device_id=device,
            device_id_type=MESH,
        )

    short = short_rows(depth)
    corner = pl.ds(0, LANES)

    def raw_copies():
        pairs = ((held[0].at[corner, corner], raw), (low_refs[0].at[:, corner], raw_low))
        return [
            pltpu.make_async_remote_copy(
                src_ref=source,
                dst_ref=target,
                send_sem=raw_send.at[i],
                recv_sem=raw_recv.at[i],
                device_id=left,
                device_id_type=MESH,
            )
            for i, (source, target) in enumerate(pairs)
        ]

    def near_query():
        ref = part(0, 0, width - short, me)
        return copy(ref, left, back_sem.at[0], me + 1, 0)

    def forward(group, origin):
        ref = part(*groups[group], origin)
        return copy(ref, right, send_sem.at[origin, group], origin, group)

    def backward(group, origin, own=False):
        ref = part(*groups[group], origin)
        semaphore = back_sem.at[group] if own else send_sem.at[origin, group]
        return copy(ref, left, semaphore, origin, group)

    def compute(array, c):
        rows = pl.ds(pl.multiple_of(c * LANES, LANES), LANES)
        low_rank = lax.dot_general(
            high_refs[array][:, rows],
            low_refs[array][...],
            (((0,), (0,)), ((), ())),
            preferred_element_type=jnp.float32,
        )
        base = held[array][:, rows].T.astype(jnp.float32)
        part(array, c * LANES, LANES, me)[...] = (base + mix_rate * low_rank).astype(
            jnp.bfloat16
        )

    def send_left(ref, group):
        @pl.when(has_left)
        def _():
            copy(ref, left, back_sem.at[group], me, group).start()

    def send_right(ref, group):
        @pl.when(has_right)
        def _():
            copy(ref, right, send_sem.at[me, group], me, group).start()

    def send_both(ref, group):
        send_left(ref, group)
        send_right(ref, group)

    def hop(source, target, device, index, semaphore):
        return pltpu.make_async_remote_copy(
            src_ref=source,
            dst_ref=target,
            send_sem=detour_send.at[index],
            recv_sem=semaphore,
            device_id=device,
            device_id_type=MESH,
        )

    def lead(helper):
        source = part(last, (helper - 1) * DETOUR_ROWS, DETOUR_ROWS, me)
        line = {"shift": 0 * shift + helper}
        return hop(source, detour, line, helper - 1, detour_recv.at[0])

    def lift():
        return hop(detour, detour, left, 0, detour_recv.at[0])

    def land():
        target = part(last, (shift - 1) * DETOUR_ROWS, DETOUR_ROWS, me + 1)
        return hop(detour, target, {"shift": 0 * shift}, 0, recv_sem.at[1, side_group])

    def send_aside():
        ref = part(*groups[side_group], me)
        send_right(ref, side_group)

        @pl.when(jnp.logical_not(leads))
        def _():
            send_left(ref, side_group)

        @pl.when(leads)
        def _():
            for helper in helpers:
                lead(helper).start()

        @pl.when(lifts)
        def _():
            lift().wait_recv()
            lift().start()

    def open_right(rows):
        @pl.when(has_right)
        def _():
            pl.semaphore_wait(told_sem, 1)

        send_right(part(0, 0, rows, me), 0)

    def finish(array):
        if array == 0:
            rows = held[0].shape[1]
            if rows > LANES:
                send_left(part(0, rows - LANES, LANES, me), 0)
            if early:
                send_right(part(0, early, rows - early, me), 0)
            else:
                open_right(rows)
        else:
            send_both(part(*groups[array], me), array)

    opening[0].wait()
    opening[2].wait()
    if short:

        @pl.when(has_left)
        def _():
            for one in raw_copies():
                one.start()

    for one in opening[1:2] + opening[3:]:
        one.wait()
    compute(0, 0)
    send_left(part(0, 0, LANES, me, (LANES, depth - LANES) if short else None), 0)

    def exchange(side):
        return pltpu.make_async_remote_copy(
            src_ref=norm_out.at[me, side],
            dst_ref=norm_out.at[me, side],
            send_sem=pair_sem.at[0],
            recv_sem=pair_sem.at[1],
            device_id=partner,
            device_id_type=MESH,
        )

    early = (EARLY_PIECES - 1) * LANES if width > EARLY_PIECES * LANES else 0

    for array in range(len(outs)):
        for one in rest_of[array]:
            one.wait()
        count = held[array].shape[1] // LANES
        if array:
            compute(array, 0)
            finish(array - 1)
        if array == 1:
            for one in norm_loads:
                one.wait()
            norm_out[me, core] = copied[12][...] + copied[13][...]
        begin = 1
        if array == 0 and count > 1:
            compute(0, 1)
            begin = 2

        def step(c, carry, array=array):
            compute(array, c)
            if array == 0:
                send_left(part(0, (c - 1) * LANES, LANES, me), 0)
            return carry

        if array == 0 and early:
            lax.fori_loop(begin, EARLY_PIECES, step, 0)
            open_right(early)
            begin = EARLY_PIECES
        lax.fori_loop(begin, count, step, 0)
    exchange(core).start()
    if tail >= LANES:
        finish(last)
    exchange(core).wait_send()
    exchange(1 - core).wait_recv()
    if tail < LANES:
        finish(last)
    if tail:

        @pl.when(core != LATE_CORE)
        def _():
            send_both(part(*groups[late_group], me), late_group)

    send_both(part(*groups[norm_group], me), norm_group)
    if aside:
        send_aside()

    if short:

        @pl.when(has_right)
        def _():
            for one in raw_copies():
                one.wait_recv()
            low_rank = lax.dot_general(
                high_refs[0][:, corner],
                raw_low[...],
                (((0,), (0,)), ((), ())),
                preferred_element_type=jnp.float32,
            )
            base = raw[...].T.astype(jnp.float32)
            part(0, 0, LANES, me + 1, (0, LANES))[...] = (base + mix_rate * low_rank).astype(
                jnp.bfloat16
            )

    def each_group(act):
        for group in range(len(groups)):
            if group == late_group:

                @pl.when(core != LATE_CORE)
                def _(group=group):
                    act(group)
            else:
                act(group)

    def relay(k, carry):
        from_left, from_right = me - k, me + k

        def pass_on(group):
            @pl.when(from_left >= 0)
            def _():
                forward(group, from_left).wait_recv()

                @pl.when(has_right)
                def _():
                    forward(group, from_left).start()

            @pl.when(from_right < n)
            def _():
                if group == 0 and short:

                    @pl.when(k == 1)
                    def _():
                        near_query().wait_recv()

                    @pl.when(k > 1)
                    def _():
                        backward(group, from_right).wait_recv()
                else:
                    backward(group, from_right).wait_recv()

                @pl.when(has_left)
                def _():
                    backward(group, from_right).start()

        each_group(pass_on)
        if aside:

            @pl.when(jnp.logical_and(lands, k == 1))
            def _():
                lift().wait_recv()
                land().start()

        return carry

    lax.fori_loop(1, n, relay, 0)

    def own_sent(group):
        @pl.when(has_right)
        def _():
            forward(group, me).wait_send()

        goes_left = has_left
        if group == side_group:
            goes_left = jnp.logical_and(has_left, jnp.logical_not(leads))

        @pl.when(goes_left)
        def _():
            if group == 0 and short:
                near_query().wait_send()
            else:
                backward(group, me, own=True).wait_send()

    each_group(own_sent)
    if short:

        @pl.when(has_left)
        def _():
            for one in raw_copies():
                one.wait_send()
    if aside:

        @pl.when(leads)
        def _():
            for helper in helpers:
                lead(helper).wait_send()

        @pl.when(lifts)
        def _():
            lift().wait_send()

        @pl.when(jnp.logical_and(lands, n > 1))
        def _():
            land().wait_send()

    def drain(k, carry):
        def sent(group):
            @pl.when(jnp.logical_and(me - k >= 0, has_right))
            def _():
                forward(group, me - k).wait_send()

            @pl.when(jnp.logical_and(me + k < n, has_left))
            def _():
                backward(group, me + k).wait_send()

        each_group(sent)
        return carry

    lax.fori_loop(1, n, drain, 0)


def body(n, shifts, *refs):
    kernel(n, shifts, refs[:14], refs[14:18], refs[18], refs[19:33], *refs[33:])


def store(n, cores, *refs):
    gathered, norm_ref, outs, norm_out, flat, rounded, sem, mixed_sem, norm_sem = (
        refs[:4],
        refs[4],
        refs[5:9],
        *refs[9:],
    )
    me, core = lax.axis_index("shard"), lax.axis_index("width")
    copies = []
    for source, out in zip(gathered[:3], outs[:3]):
        for row in range(0, source.shape[0], COPY_ROWS):
            rows = pl.ds(row, min(COPY_ROWS, source.shape[0] - row))
            copies.append(
                pltpu.make_async_copy(source.at[rows], out.at[rows], sem.at[len(copies)])
            )

    block = gathered[3].shape[0] // n
    tail = late_rows(block)

    def mixed(origin, row, size, part):
        rows = pl.ds(origin * block + row, size)
        return pltpu.make_async_copy(
            gathered[3].at[rows], outs[3].at[rows], mixed_sem.at[origin, part]
        )

    copies += [mixed(origin, 0, block - tail, 0) for origin in range(n)]

    def each_last(act):
        for origin in range(n if tail else 0):

            @pl.when(jnp.logical_or(core != LATE_CORE, me == origin))
            def _(origin=origin):
                act(mixed(origin, block - tail, tail, 1))

    for copy in copies:
        copy.start()
    each_last(lambda copy: copy.start())
    rows = norm_ref.shape[2]
    for origin in range(n):
        for side in range(cores):
            flat[pl.ds((origin * cores + side) * rows, rows)] = norm_ref[origin, side]
    rounded[...] = flat[...].astype(norm_out.dtype)
    norm_copy = pltpu.make_async_copy(rounded, norm_out, norm_sem)
    norm_copy.start()
    for copy in copies:
        copy.wait()
    each_last(lambda copy: copy.wait())
    norm_copy.wait()


def late(n, mixed, after, out, send_sem, recv_sem, told_sem):
    me = lax.axis_index("shard")
    core = lax.axis_index("width")
    has_left, has_right = me > 0, me < n - 1
    left, right = {"shard": me - 1}, {"shard": me + 1}
    block = mixed.shape[0] // n
    tail = late_rows(block)
    size = tail // LATE_STEPS

    def copy(origin, begin, rows, step, device, semaphore, own):
        first = pl.multiple_of(me * block + block - tail + begin, 16)
        dst = out.at[origin, pl.ds(pl.multiple_of(begin, 16), rows)]
        return pltpu.make_async_remote_copy(
            src_ref=mixed.at[pl.ds(first, rows)] if own else dst,
            dst_ref=dst,
            send_sem=send_sem.at[semaphore],
            recv_sem=recv_sem.at[origin, step],
            device_id=device,
            device_id_type=MESH,
        )

    def forward(origin, step, own=False):
        return copy(origin, step * size, size, step, right, origin, own)

    def backward(origin, step, own=False):
        return copy(origin, step * size, size, step, left, n if own else origin, own)

    def sent(origin, semaphore):
        copy(origin, 0, tail, 0, right, semaphore, True).wait_send()

    @pl.when(core == LATE_CORE)
    def _():
        barrier = pltpu.get_barrier_semaphore()

        @pl.when(has_right)
        def _():
            pl.semaphore_signal(barrier, inc=1, device_id=right, device_id_type=MESH)

        @pl.when(has_left)
        def _():
            pl.semaphore_wait(barrier, 1)
            for step in range(LATE_STEPS):
                backward(me, step, own=True).start()
            pl.semaphore_signal(told_sem, inc=1, device_id=left, device_id_type=MESH)

        @pl.when(has_right)
        def _():
            pl.semaphore_wait(told_sem, 1)
            for step in range(LATE_STEPS):
                forward(me, step, own=True).start()

        def relay(k, carry):
            for step in range(LATE_STEPS):

                @pl.when(me - k >= 0)
                def _(step=step):
                    forward(me - k, step).wait_recv()

                    @pl.when(has_right)
                    def _():
                        forward(me - k, step).start()

                @pl.when(me + k < n)
                def _(step=step):
                    backward(me + k, step).wait_recv()

                    @pl.when(has_left)
                    def _():
                        backward(me + k, step).start()

            return carry

        lax.fori_loop(1, n, relay, 0)

        @pl.when(has_right)
        def _():
            sent(me, me)

        @pl.when(has_left)
        def _():
            sent(me, n)

        def drain(k, carry):
            @pl.when(jnp.logical_and(me - k >= 0, has_right))
            def _():
                sent(me - k, me - k)

            @pl.when(jnp.logical_and(me + k < n, has_left))
            def _():
                sent(me + k, me + k)

            return carry

        lax.fori_loop(1, n, drain, 0)


def store_late(n, pieces, given, out, sem):
    me, core = lax.axis_index("shard"), lax.axis_index("width")
    block = out.shape[0] // n
    tail = late_rows(block)

    def each(act):
        for origin in range(n):

            @pl.when(jnp.logical_and(core == LATE_CORE, me != origin))
            def _(origin=origin):
                act(origin)

    def begin(origin):
        for row in range(0, tail, STORE_ROWS):
            rows = pl.ds((origin + 1) * block - tail + row, STORE_ROWS)
            source = pieces.at[origin, pl.ds(row, STORE_ROWS)]
            pltpu.make_async_copy(source, out.at[rows], sem.at[origin]).start()

    def end(origin):
        rows = pl.ds((origin + 1) * block - tail, tail)
        pltpu.make_async_copy(pieces.at[origin], out.at[rows], sem.at[origin]).wait()

    each(begin)
    each(end)


def on_device(n, cores, shifts, *args):
    weights, (norm_train, norm_step) = list(args[:12]), args[12:]
    bases = weights[0::3]
    (size,) = norm_train.shape
    sizes = [size, *(size for w in bases for size in w.shape)]
    if cores != 2 or any(size % LANES for size in sizes):
        return plain(*args)
    rows = size // LANES
    shapes = [(w.shape[1], w.shape[0] * n) for w in bases[:3]]
    shapes.append((bases[3].shape[1] * n, bases[3].shape[0]))
    in_hbm = pl.BlockSpec(memory_space=pltpu.HBM)
    in_vmem = pl.BlockSpec(memory_space=pltpu.VMEM)
    tail = late_rows(bases[3].shape[1])
    helpers = detours(shifts)
    groups = len(bases) + (2 if tail else 1) + (1 if helpers else 0)
    weights[1::3] = [low.T for low in weights[1::3]]
    norms = [norm_train.reshape(rows, LANES), norm_step.reshape(rows, LANES)]
    given = [pltpu.with_memory_space_constraint(array, pltpu.HBM) for array in weights + norms]
    gathered = pl.pallas_call(
        functools.partial(body, n, shifts),
        out_shape=[pltpu.VMEM(shape, jnp.bfloat16) for shape in shapes]
        + [pltpu.VMEM((n, cores, rows, LANES), jnp.float32)],
        in_specs=[in_hbm] * 14,
        out_specs=[in_vmem] * 5,
        scratch_shapes=[pltpu.VMEM(array.shape, array.dtype) for array in given]
        + [
            pltpu.SemaphoreType.DMA((15 + bases[0].shape[0] // LANES,)),
            pltpu.SemaphoreType.DMA((n, groups)),
            pltpu.SemaphoreType.DMA((groups,)),
            pltpu.SemaphoreType.DMA((n, groups)),
            pltpu.SemaphoreType.DMA((2,)),
            pltpu.SemaphoreType.REGULAR,
            pltpu.VMEM((DETOUR_ROWS, shapes[3][1]), jnp.bfloat16),
            pltpu.SemaphoreType.DMA((max(helpers, 1),)),
            pltpu.SemaphoreType.DMA((1,)),
            pltpu.VMEM((LANES, LANES), jnp.bfloat16),
            pltpu.VMEM((given[1].shape[0], LANES), jnp.bfloat16),
            pltpu.SemaphoreType.DMA((2,)),
            pltpu.SemaphoreType.DMA((2,)),
        ],
        compiler_params=pltpu.CompilerParams(
            collective_id=0, has_side_effects=True, vmem_limit_bytes=40 * 2**20
        ),
        name="merge_gather",
    )(*given)
    norm_rows = n * cores * rows
    *finals, norm = pl.pallas_call(
        functools.partial(store, n, cores),
        out_shape=[jax.ShapeDtypeStruct(shape, jnp.bfloat16) for shape in shapes]
        + [jax.ShapeDtypeStruct((norm_rows, LANES), jnp.bfloat16)],
        in_specs=[in_vmem] * 5,
        out_specs=[in_hbm] * 5,
        scratch_shapes=[
            pltpu.VMEM((norm_rows, LANES), jnp.float32),
            pltpu.VMEM((norm_rows, LANES), jnp.bfloat16),
            pltpu.SemaphoreType.DMA((sum(-(-shape[0] // COPY_ROWS) for shape in shapes[:3]),)),
            pltpu.SemaphoreType.DMA((n, 2)),
            pltpu.SemaphoreType.DMA,
        ],
        compiler_params=pltpu.CompilerParams(vmem_limit_bytes=20 * 2**20),
        name="store",
    )(*gathered)
    norm = norm.reshape(-1)
    if not tail:
        return (*finals, norm)
    columns = shapes[3][1]
    pieces = pl.pallas_call(
        functools.partial(late, n),
        out_shape=pltpu.VMEM((n, tail, columns), jnp.bfloat16),
        in_specs=[in_vmem, in_hbm],
        out_specs=in_vmem,
        scratch_shapes=[
            pltpu.SemaphoreType.DMA((n + 1,)),
            pltpu.SemaphoreType.DMA((n, LATE_STEPS)),
            pltpu.SemaphoreType.REGULAR,
        ],
        compiler_params=pltpu.CompilerParams(
            collective_id=1, has_side_effects=True, vmem_limit_bytes=20 * 2**20
        ),
        name="late",
    )(gathered[3], pltpu.with_memory_space_constraint(finals[3], pltpu.HBM))
    finals[3] = pl.pallas_call(
        functools.partial(store_late, n),
        out_shape=jax.ShapeDtypeStruct(shapes[3], jnp.bfloat16),
        in_specs=[in_vmem, in_hbm],
        out_specs=in_hbm,
        input_output_aliases={1: 0},
        scratch_shapes=[pltpu.SemaphoreType.DMA((n,))],
        compiler_params=pltpu.CompilerParams(vmem_limit_bytes=20 * 2**20),
        name="store_late",
    )(pieces, finals[3])
    return (*finals, norm)


def solution(mesh):
    placed = (
        P(("shift", "shard"), "width"),
        P(("shift", "shard"), None),
        P("shift", "width"),
        P(("shift", "shard"), "width"),
        P(("shift", "shard"), None),
        P("shift", "width"),
        P(("shift", "shard"), "width"),
        P(("shift", "shard"), None),
        P("shift", "width"),
        P(("shift", "width"), "shard"),
        P(("shift", "width"), None),
        P("shift", "shard"),
        P(("shift", "shard", "width")),
        P(("shift", "shard", "width")),
    )
    return jax.shard_map(
        functools.partial(
            on_device, mesh.shape["shard"], mesh.shape["width"], mesh.shape["shift"]
        ),
        mesh=mesh,
        in_specs=placed,
        out_specs=(
            P(("shift", "width"), None),
            P(("shift", "width"), None),
            P(("shift", "width"), None),
            P("shift", "width"),
            P("shift"),
        ),
        check_vma=False,
    )
```

```python
import functools

import jax
import jax.numpy as jnp
from jax import lax
from jax.experimental import pallas as pl
from jax.experimental.pallas import tpu as pltpu
from jax.sharding import PartitionSpec as P

mix_rate = 0.5
MESH = pl.DeviceIdType.MESH
LANES = 128
COPY_ROWS = 256
LATE_STEPS = 2
LATE_CORE = 1
LATE_ROWS = 160
ROW_UNIT = 8
DETOURS = 3
DETOUR_ROWS = 8
EARLY_PIECES = 3
STORE_ROWS = 32


def plain(
    w_query,
    low_query,
    high_query,
    w_key,
    low_key,
    high_key,
    w_value,
    low_value,
    high_value,
    w_mixed,
    low_mixed,
    high_mixed,
    norm_train,
    norm_step,
):
    def merged(w, low, high):
        low_rank = jnp.dot(low, high, preferred_element_type=jnp.float32)
        return (w.astype(jnp.float32) + mix_rate * low_rank).astype(jnp.bfloat16)

    query = lax.all_gather(merged(w_query, low_query, high_query), "shard", axis=0, tiled=True)
    key = lax.all_gather(merged(w_key, low_key, high_key), "shard", axis=0, tiled=True)
    value = lax.all_gather(merged(w_value, low_value, high_value), "shard", axis=0, tiled=True)
    mixed = lax.all_gather(merged(w_mixed, low_mixed, high_mixed), "shard", axis=1, tiled=True)
    norm = lax.all_gather(
        (norm_train + norm_step).astype(jnp.bfloat16), ("shard", "width"), axis=0, tiled=True
    )
    return query.T, key.T, value.T, mixed.T, norm


def detours(shifts):
    return min(DETOURS, shifts - 1)


def short_rows(depth):
    rows = LANES * LANES // depth
    return rows if rows * depth == LANES * LANES and rows % ROW_UNIT == 0 and rows < LANES else 0


def late_rows(block):
    return LATE_ROWS if block > LATE_ROWS else 0


def kernel(
    n,
    shifts,
    given,
    outs,
    norm_out,
    copied,
    load_sem,
    send_sem,
    back_sem,
    recv_sem,
    pair_sem,
    told_sem,
    detour,
    detour_send,
    detour_recv,
    raw,
    raw_low,
    raw_send,
    raw_recv,
):
    me, shift = lax.axis_index("shard"), lax.axis_index("shift")
    core = lax.axis_index("width")
    has_left, has_right = me > 0, me < n - 1
    left, right = {"shard": me - 1}, {"shard": me + 1}
    partner = {"width": 1 - core}
    helpers = range(1, 1 + detours(shifts))
    aside = len(helpers) * DETOUR_ROWS

    def on_early(*conditions):
        return functools.reduce(jnp.logical_and, conditions, core != LATE_CORE)

    helps = jnp.logical_and(shift >= 1, shift <= len(helpers))
    leads, ends = on_early(shift == 0, me == 1), on_early(shift == 0, me == 0)
    lifts, lands = on_early(helps, me == 1), on_early(helps, me == 0)
    held, low_refs, high_refs = copied[0:12:3], copied[1:12:3], copied[2:12:3]
    depth, width = held[0].shape
    first, rest = pl.ds(0, LANES), pl.ds(LANES, width - LANES)
    bands = [pl.ds(row, LANES) for row in range(0, depth, LANES)]
    loads = []

    def load(source, target):
        loads.append(pltpu.make_async_copy(source, target, load_sem.at[len(loads)]))
        return loads[-1]

    opening = [load(given[1], copied[1]), load(given[2].at[:, first], copied[2].at[:, first])]
    opening += [load(given[0].at[rows, first], held[0].at[rows, first]) for rows in bands]
    others = []
    if width > LANES:
        others = [load(given[i].at[:, rest], copied[i].at[:, rest]) for i in (2, 0)]
    rest_of = [others] + [
        [load(given[i], copied[i]) for i in range(array, array + 3)] for array in (3, 6, 9)
    ]
    norm_loads = [load(given[i], copied[i]) for i in (12, 13)]
    for one in opening:
        one.start()

    barrier = pltpu.get_barrier_semaphore()
    pl.semaphore_signal(barrier, inc=1, device_id=partner, device_id_type=MESH)

    @pl.when(has_right)
    def _():
        pl.semaphore_signal(barrier, inc=1, device_id=right, device_id_type=MESH)

    if aside:

        @pl.when(lifts)
        def _():
            line = {"shift": 0 * shift}
            pl.semaphore_signal(barrier, inc=1, device_id=line, device_id_type=MESH)

        @pl.when(ends)
        def _():
            for helper in helpers:
                line = {"shift": 0 * shift + helper}
                pl.semaphore_signal(barrier, inc=1, device_id=line, device_id_type=MESH)

    for one in loads[len(opening) :]:
        one.start()
    waited = 1 + has_left.astype(jnp.int32)
    if aside:
        waited += jnp.where(leads, len(helpers), 0) + lands.astype(jnp.int32)
    pl.semaphore_wait(barrier, waited)

    @pl.when(has_left)
    def _():
        pl.semaphore_signal(told_sem, inc=1, device_id=left, device_id_type=MESH)

    last = len(outs) - 1
    block = held[last].shape[1]
    tail = late_rows(block)
    groups = [(array, 0, w.shape[1]) for array, w in enumerate(held[:last])]
    groups.append((last, aside, block - tail - aside))
    if tail:
        groups.append((last, block - tail, tail))
    groups.append((len(outs), 0, 0))
    side_group = len(groups)
    if aside:
        groups.append((last, 0, aside))
    norm_group = len(outs) + (1 if tail else 0)
    late_group = norm_group - 1 if tail else -1

    def part(array, row, rows, origin, band=None):
        if array == len(outs):
            return norm_out.at[origin]
        out, w = outs[array], held[array]
        if array < last:
            first, size = band or (0, w.shape[0])
            begin = pl.multiple_of(origin * w.shape[0] + first, LANES)
            return out.at[pl.ds(pl.multiple_of(row, LANES), rows), pl.ds(begin, size)]
        begin = pl.multiple_of(origin * block + row, ROW_UNIT)
        return out.at[pl.ds(begin, rows)]

    def copy(ref, device, semaphore, origin, group):
        return pltpu.make_async_remote_copy(
            src_ref=ref,
            dst_ref=ref,
            send_sem=semaphore,
            recv_sem=recv_sem.at[origin, group],
            device_id=device,
            device_id_type=MESH,
        )

    short = short_rows(depth)
    corner = pl.ds(0, LANES)

    def raw_copies():
        pairs = ((held[0].at[corner, corner], raw), (low_refs[0].at[:, corner], raw_low))
        return [
            pltpu.make_async_remote_copy(
                src_ref=source,
                dst_ref=target,
                send_sem=raw_send.at[i],
                recv_sem=raw_recv.at[i],
                device_id=left,
                device_id_type=MESH,
            )
            for i, (source, target) in enumerate(pairs)
        ]

    def near_query():
        ref = part(0, 0, width - short, me)
        return copy(ref, left, back_sem.at[0], me + 1, 0)

    def forward(group, origin):
        ref = part(*groups[group], origin)
        return copy(ref, right, send_sem.at[origin, group], origin, group)

    def backward(group, origin, own=False):
        ref = part(*groups[group], origin)
        semaphore = back_sem.at[group] if own else send_sem.at[origin, group]
        return copy(ref, left, semaphore, origin, group)

    def compute(array, c):
        rows = pl.ds(pl.multiple_of(c * LANES, LANES), LANES)
        low_rank = lax.dot_general(
            high_refs[array][:, rows],
            low_refs[array][...],
            (((0,), (0,)), ((), ())),
            preferred_element_type=jnp.float32,
        )
        base = held[array][:, rows].T.astype(jnp.float32)
        part(array, c * LANES, LANES, me)[...] = (base + mix_rate * low_rank).astype(
            jnp.bfloat16
        )

    def send_left(ref, group):
        @pl.when(has_left)
        def _():
            copy(ref, left, back_sem.at[group], me, group).start()

    def send_right(ref, group):
        @pl.when(has_right)
        def _():
            copy(ref, right, send_sem.at[me, group], me, group).start()

    def send_both(ref, group):
        send_left(ref, group)
        send_right(ref, group)

    def hop(source, target, device, index, semaphore):
        return pltpu.make_async_remote_copy(
            src_ref=source,
            dst_ref=target,
            send_sem=detour_send.at[index],
            recv_sem=semaphore,
            device_id=device,
            device_id_type=MESH,
        )

    def lead(helper):
        source = part(last, (helper - 1) * DETOUR_ROWS, DETOUR_ROWS, me)
        line = {"shift": 0 * shift + helper}
        return hop(source, detour, line, helper - 1, detour_recv.at[0])

    def lift():
        return hop(detour, detour, left, 0, detour_recv.at[0])

    def land():
        target = part(last, (shift - 1) * DETOUR_ROWS, DETOUR_ROWS, me + 1)
        return hop(detour, target, {"shift": 0 * shift}, 0, recv_sem.at[1, side_group])

    def send_aside():
        ref = part(*groups[side_group], me)
        send_right(ref, side_group)

        @pl.when(jnp.logical_not(leads))
        def _():
            send_left(ref, side_group)

        @pl.when(leads)
        def _():
            for helper in helpers:
                lead(helper).start()

        @pl.when(lifts)
        def _():
            lift().wait_recv()
            lift().start()

    def open_right(rows):
        @pl.when(has_right)
        def _():
            pl.semaphore_wait(told_sem, 1)

        send_right(part(0, 0, rows, me), 0)

    def finish(array):
        if array == 0:
            rows = held[0].shape[1]
            if rows > LANES:
                send_left(part(0, rows - LANES, LANES, me), 0)
            if early:
                send_right(part(0, early, rows - early, me), 0)
            else:
                open_right(rows)
        else:
            send_both(part(*groups[array], me), array)

    opening[0].wait()
    opening[2].wait()
    if short:

        @pl.when(has_left)
        def _():
            for one in raw_copies():
                one.start()

    for one in opening[1:2] + opening[3:]:
        one.wait()
    compute(0, 0)
    send_left(part(0, 0, LANES, me, (LANES, depth - LANES) if short else None), 0)

    def exchange(side):
        return pltpu.make_async_remote_copy(
            src_ref=norm_out.at[me, side],
            dst_ref=norm_out.at[me, side],
            send_sem=pair_sem.at[0],
            recv_sem=pair_sem.at[1],
            device_id=partner,
            device_id_type=MESH,
        )

    early = (EARLY_PIECES - 1) * LANES if width > EARLY_PIECES * LANES else 0

    for array in range(len(outs)):
        for one in rest_of[array]:
            one.wait()
        count = held[array].shape[1] // LANES
        if array:
            compute(array, 0)
            finish(array - 1)
        if array == 1:
            for one in norm_loads:
                one.wait()
            norm_out[me, core] = copied[12][...] + copied[13][...]
        begin = 1
        if array == 0 and count > 1:
            compute(0, 1)
            begin = 2

        def step(c, carry, array=array):
            compute(array, c)
            if array == 0:
                send_left(part(0, (c - 1) * LANES, LANES, me), 0)
            return carry

        if array == 0 and early:
            lax.fori_loop(begin, EARLY_PIECES, step, 0)
            open_right(early)
            begin = EARLY_PIECES
        lax.fori_loop(begin, count, step, 0)
    exchange(core).start()
    if tail >= LANES:
        finish(last)
    exchange(core).wait_send()
    exchange(1 - core).wait_recv()
    if tail < LANES:
        finish(last)
    if tail:

        @pl.when(core != LATE_CORE)
        def _():
            send_both(part(*groups[late_group], me), late_group)

    send_both(part(*groups[norm_group], me), norm_group)
    if aside:
        send_aside()

    if short:

        @pl.when(has_right)
        def _():
            for one in raw_copies():
                one.wait_recv()
            low_rank = lax.dot_general(
                high_refs[0][:, corner],
                raw_low[...],
                (((0,), (0,)), ((), ())),
                preferred_element_type=jnp.float32,
            )
            base = raw[...].T.astype(jnp.float32)
            part(0, 0, LANES, me + 1, (0, LANES))[...] = (base + mix_rate * low_rank).astype(
                jnp.bfloat16
            )

    def each_group(act):
        for group in range(len(groups)):
            if group == late_group:

                @pl.when(core != LATE_CORE)
                def _(group=group):
                    act(group)
            else:
                act(group)

    def relay(k, carry):
        from_left, from_right = me - k, me + k

        def pass_on(group):
            @pl.when(from_left >= 0)
            def _():
                forward(group, from_left).wait_recv()

                @pl.when(has_right)
                def _():
                    forward(group, from_left).start()

            @pl.when(from_right < n)
            def _():
                if group == 0 and short:

                    @pl.when(k == 1)
                    def _():
                        near_query().wait_recv()

                    @pl.when(k > 1)
                    def _():
                        backward(group, from_right).wait_recv()
                else:
                    backward(group, from_right).wait_recv()

                @pl.when(has_left)
                def _():
                    backward(group, from_right).start()

        each_group(pass_on)
        if aside:

            @pl.when(jnp.logical_and(lands, k == 1))
            def _():
                lift().wait_recv()
                land().start()

        return carry

    lax.fori_loop(1, n, relay, 0)

    def own_sent(group):
        @pl.when(has_right)
        def _():
            forward(group, me).wait_send()

        goes_left = has_left
        if group == side_group:
            goes_left = jnp.logical_and(has_left, jnp.logical_not(leads))

        @pl.when(goes_left)
        def _():
            if group == 0 and short:
                near_query().wait_send()
            else:
                backward(group, me, own=True).wait_send()

    each_group(own_sent)
    if short:

        @pl.when(has_left)
        def _():
            for one in raw_copies():
                one.wait_send()
    if aside:

        @pl.when(leads)
        def _():
            for helper in helpers:
                lead(helper).wait_send()

        @pl.when(lifts)
        def _():
            lift().wait_send()

        @pl.when(jnp.logical_and(lands, n > 1))
        def _():
            land().wait_send()

    def drain(k, carry):
        def sent(group):
            @pl.when(jnp.logical_and(me - k >= 0, has_right))
            def _():
                forward(group, me - k).wait_send()

            @pl.when(jnp.logical_and(me + k < n, has_left))
            def _():
                backward(group, me + k).wait_send()

        each_group(sent)
        return carry

    lax.fori_loop(1, n, drain, 0)


def body(n, shifts, *refs):
    kernel(n, shifts, refs[:14], refs[14:18], refs[18], refs[19:33], *refs[33:])


def store(n, cores, *refs):
    gathered, norm_ref, outs, norm_out, flat, rounded, sem, mixed_sem, norm_sem = (
        refs[:4],
        refs[4],
        refs[5:9],
        *refs[9:],
    )
    me, core = lax.axis_index("shard"), lax.axis_index("width")
    copies = []
    for source, out in zip(gathered[:3], outs[:3]):
        for row in range(0, source.shape[0], COPY_ROWS):
            rows = pl.ds(row, min(COPY_ROWS, source.shape[0] - row))
            copies.append(
                pltpu.make_async_copy(source.at[rows], out.at[rows], sem.at[len(copies)])
            )

    block = gathered[3].shape[0] // n
    tail = late_rows(block)

    def mixed(origin, row, size, part):
        rows = pl.ds(origin * block + row, size)
        return pltpu.make_async_copy(
            gathered[3].at[rows], outs[3].at[rows], mixed_sem.at[origin, part]
        )

    copies += [mixed(origin, 0, block - tail, 0) for origin in range(n)]

    def each_last(act):
        for origin in range(n if tail else 0):

            @pl.when(jnp.logical_or(core != LATE_CORE, me == origin))
            def _(origin=origin):
                act(mixed(origin, block - tail, tail, 1))

    for copy in copies:
        copy.start()
    each_last(lambda copy: copy.start())
    rows = norm_ref.shape[2]
    for origin in range(n):
        for side in range(cores):
            flat[pl.ds((origin * cores + side) * rows, rows)] = norm_ref[origin, side]
    rounded[...] = flat[...].astype(norm_out.dtype)
    norm_copy = pltpu.make_async_copy(rounded, norm_out, norm_sem)
    norm_copy.start()
    for copy in copies:
        copy.wait()
    each_last(lambda copy: copy.wait())
    norm_copy.wait()


def late(n, mixed, after, out, send_sem, recv_sem, told_sem):
    me = lax.axis_index("shard")
    core = lax.axis_index("width")
    has_left, has_right = me > 0, me < n - 1
    left, right = {"shard": me - 1}, {"shard": me + 1}
    block = mixed.shape[0] // n
    tail = late_rows(block)
    size = tail // LATE_STEPS

    def copy(origin, begin, rows, step, device, semaphore, own):
        first = pl.multiple_of(me * block + block - tail + begin, 16)
        dst = out.at[origin, pl.ds(pl.multiple_of(begin, 16), rows)]
        return pltpu.make_async_remote_copy(
            src_ref=mixed.at[pl.ds(first, rows)] if own else dst,
            dst_ref=dst,
            send_sem=send_sem.at[semaphore],
            recv_sem=recv_sem.at[origin, step],
            device_id=device,
            device_id_type=MESH,
        )

    def forward(origin, step, own=False):
        return copy(origin, step * size, size, step, right, origin, own)

    def backward(origin, step, own=False):
        return copy(origin, step * size, size, step, left, n if own else origin, own)

    def sent(origin, semaphore):
        copy(origin, 0, tail, 0, right, semaphore, True).wait_send()

    @pl.when(core == LATE_CORE)
    def _():
        barrier = pltpu.get_barrier_semaphore()

        @pl.when(has_right)
        def _():
            pl.semaphore_signal(barrier, inc=1, device_id=right, device_id_type=MESH)

        @pl.when(has_left)
        def _():
            pl.semaphore_wait(barrier, 1)
            for step in range(LATE_STEPS):
                backward(me, step, own=True).start()
            pl.semaphore_signal(told_sem, inc=1, device_id=left, device_id_type=MESH)

        @pl.when(has_right)
        def _():
            pl.semaphore_wait(told_sem, 1)
            for step in range(LATE_STEPS):
                forward(me, step, own=True).start()

        def relay(k, carry):
            for step in range(LATE_STEPS):

                @pl.when(me - k >= 0)
                def _(step=step):
                    forward(me - k, step).wait_recv()

                    @pl.when(has_right)
                    def _():
                        forward(me - k, step).start()

                @pl.when(me + k < n)
                def _(step=step):
                    backward(me + k, step).wait_recv()

                    @pl.when(has_left)
                    def _():
                        backward(me + k, step).start()

            return carry

        lax.fori_loop(1, n, relay, 0)

        @pl.when(has_right)
        def _():
            sent(me, me)

        @pl.when(has_left)
        def _():
            sent(me, n)

        def drain(k, carry):
            @pl.when(jnp.logical_and(me - k >= 0, has_right))
            def _():
                sent(me - k, me - k)

            @pl.when(jnp.logical_and(me + k < n, has_left))
            def _():
                sent(me + k, me + k)

            return carry

        lax.fori_loop(1, n, drain, 0)


def store_late(n, pieces, given, out, sem):
    me, core = lax.axis_index("shard"), lax.axis_index("width")
    block = out.shape[0] // n
    tail = late_rows(block)

    def each(act):
        for origin in range(n):

            @pl.when(jnp.logical_and(core == LATE_CORE, me != origin))
            def _(origin=origin):
                act(origin)

    def begin(origin):
        for row in range(0, tail, STORE_ROWS):
            rows = pl.ds((origin + 1) * block - tail + row, STORE_ROWS)
            source = pieces.at[origin, pl.ds(row, STORE_ROWS)]
            pltpu.make_async_copy(source, out.at[rows], sem.at[origin]).start()

    def end(origin):
        rows = pl.ds((origin + 1) * block - tail, tail)
        pltpu.make_async_copy(pieces.at[origin], out.at[rows], sem.at[origin]).wait()

    each(begin)
    each(end)


def on_device(n, cores, shifts, *args):
    weights, (norm_train, norm_step) = list(args[:12]), args[12:]
    bases = weights[0::3]
    (size,) = norm_train.shape
    sizes = [size, *(size for w in bases for size in w.shape)]
    if cores != 2 or any(size % LANES for size in sizes):
        return plain(*args)
    rows = size // LANES
    shapes = [(w.shape[1], w.shape[0] * n) for w in bases[:3]]
    shapes.append((bases[3].shape[1] * n, bases[3].shape[0]))
    in_hbm = pl.BlockSpec(memory_space=pltpu.HBM)
    in_vmem = pl.BlockSpec(memory_space=pltpu.VMEM)
    tail = late_rows(bases[3].shape[1])
    helpers = detours(shifts)
    groups = len(bases) + (2 if tail else 1) + (1 if helpers else 0)
    weights[1::3] = [low.T for low in weights[1::3]]
    norms = [norm_train.reshape(rows, LANES), norm_step.reshape(rows, LANES)]
    given = [pltpu.with_memory_space_constraint(array, pltpu.HBM) for array in weights + norms]
    gathered = pl.pallas_call(
        functools.partial(body, n, shifts),
        out_shape=[pltpu.VMEM(shape, jnp.bfloat16) for shape in shapes]
        + [pltpu.VMEM((n, cores, rows, LANES), jnp.float32)],
        in_specs=[in_hbm] * 14,
        out_specs=[in_vmem] * 5,
        scratch_shapes=[pltpu.VMEM(array.shape, array.dtype) for array in given]
        + [
            pltpu.SemaphoreType.DMA((15 + bases[0].shape[0] // LANES,)),
            pltpu.SemaphoreType.DMA((n, groups)),
            pltpu.SemaphoreType.DMA((groups,)),
            pltpu.SemaphoreType.DMA((n, groups)),
            pltpu.SemaphoreType.DMA((2,)),
            pltpu.SemaphoreType.REGULAR,
            pltpu.VMEM((DETOUR_ROWS, shapes[3][1]), jnp.bfloat16),
            pltpu.SemaphoreType.DMA((max(helpers, 1),)),
            pltpu.SemaphoreType.DMA((1,)),
            pltpu.VMEM((LANES, LANES), jnp.bfloat16),
            pltpu.VMEM((given[1].shape[0], LANES), jnp.bfloat16),
            pltpu.SemaphoreType.DMA((2,)),
            pltpu.SemaphoreType.DMA((2,)),
        ],
        compiler_params=pltpu.CompilerParams(
            collective_id=0, has_side_effects=True, vmem_limit_bytes=40 * 2**20
        ),
        name="merge_gather",
    )(*given)
    norm_rows = n * cores * rows
    *finals, norm = pl.pallas_call(
        functools.partial(store, n, cores),
        out_shape=[jax.ShapeDtypeStruct(shape, jnp.bfloat16) for shape in shapes]
        + [jax.ShapeDtypeStruct((norm_rows, LANES), jnp.bfloat16)],
        in_specs=[in_vmem] * 5,
        out_specs=[in_hbm] * 5,
        scratch_shapes=[
            pltpu.VMEM((norm_rows, LANES), jnp.float32),
            pltpu.VMEM((norm_rows, LANES), jnp.bfloat16),
            pltpu.SemaphoreType.DMA((sum(-(-shape[0] // COPY_ROWS) for shape in shapes[:3]),)),
            pltpu.SemaphoreType.DMA((n, 2)),
            pltpu.SemaphoreType.DMA,
        ],
        compiler_params=pltpu.CompilerParams(vmem_limit_bytes=20 * 2**20),
        name="store",
    )(*gathered)
    norm = norm.reshape(-1)
    if not tail:
        return (*finals, norm)
    columns = shapes[3][1]
    pieces = pl.pallas_call(
        functools.partial(late, n),
        out_shape=pltpu.VMEM((n, tail, columns), jnp.bfloat16),
        in_specs=[in_vmem, in_hbm],
        out_specs=in_vmem,
        scratch_shapes=[
            pltpu.SemaphoreType.DMA((n + 1,)),
            pltpu.SemaphoreType.DMA((n, LATE_STEPS)),
            pltpu.SemaphoreType.REGULAR,
        ],
        compiler_params=pltpu.CompilerParams(
            collective_id=1, has_side_effects=True, vmem_limit_bytes=20 * 2**20
        ),
        name="late",
    )(gathered[3], pltpu.with_memory_space_constraint(finals[3], pltpu.HBM))
    finals[3] = pl.pallas_call(
        functools.partial(store_late, n),
        out_shape=jax.ShapeDtypeStruct(shapes[3], jnp.bfloat16),
        in_specs=[in_vmem, in_hbm],
        out_specs=in_hbm,
        input_output_aliases={1: 0},
        scratch_shapes=[pltpu.SemaphoreType.DMA((n,))],
        compiler_params=pltpu.CompilerParams(vmem_limit_bytes=20 * 2**20),
        name="store_late",
    )(pieces, finals[3])
    return (*finals, norm)


def solution(mesh):
    placed = (
        P(("shift", "shard"), "width"),
        P(("shift", "shard"), None),
        P("shift", "width"),
        P(("shift", "shard"), "width"),
        P(("shift", "shard"), None),
        P("shift", "width"),
        P(("shift", "shard"), "width"),
        P(("shift", "shard"), None),
        P("shift", "width"),
        P(("shift", "width"), "shard"),
        P(("shift", "width"), None),
        P("shift", "shard"),
        P(("shift", "shard", "width")),
        P(("shift", "shard", "width")),
    )
    return jax.shard_map(
        functools.partial(
            on_device, mesh.shape["shard"], mesh.shape["width"], mesh.shape["shift"]
        ),
        mesh=mesh,
        in_specs=placed,
        out_specs=(
            P(("shift", "width"), None),
            P(("shift", "width"), None),
            P(("shift", "width"), None),
            P("shift", "width"),
            P("shift"),
        ),
        check_vma=False,
    )
```

```python
import functools

import jax
import jax.numpy as jnp
from jax import lax
from jax.experimental import pallas as pl
from jax.experimental.pallas import tpu as pltpu
from jax.sharding import PartitionSpec as P

mix_rate = 0.5
MESH = pl.DeviceIdType.MESH
LANES = 128
COPY_ROWS = 256
LATE_STEPS = 3
LATE_CORE = 1
LATE_ROWS = 144
ROW_UNIT = 8
DETOURS = 3
DETOUR_ROWS = 8
EARLY_PIECES = 3
STORE_ROWS = 48


def plain(
    w_query,
    low_query,
    high_query,
    w_key,
    low_key,
    high_key,
    w_value,
    low_value,
    high_value,
    w_mixed,
    low_mixed,
    high_mixed,
    norm_train,
    norm_step,
):
    def merged(w, low, high):
        low_rank = jnp.dot(low, high, preferred_element_type=jnp.float32)
        return (w.astype(jnp.float32) + mix_rate * low_rank).astype(jnp.bfloat16)

    query = lax.all_gather(merged(w_query, low_query, high_query), "shard", axis=0, tiled=True)
    key = lax.all_gather(merged(w_key, low_key, high_key), "shard", axis=0, tiled=True)
    value = lax.all_gather(merged(w_value, low_value, high_value), "shard", axis=0, tiled=True)
    mixed = lax.all_gather(merged(w_mixed, low_mixed, high_mixed), "shard", axis=1, tiled=True)
    norm = lax.all_gather(
        (norm_train + norm_step).astype(jnp.bfloat16), ("shard", "width"), axis=0, tiled=True
    )
    return query.T, key.T, value.T, mixed.T, norm


def detours(shifts):
    return min(DETOURS, shifts - 1)


def short_rows(depth):
    rows = LANES * LANES // depth
    return rows if rows * depth == LANES * LANES and rows % ROW_UNIT == 0 and rows < LANES else 0


def late_rows(block):
    return LATE_ROWS if block > LATE_ROWS else 0


def kernel(
    n,
    shifts,
    given,
    outs,
    norm_out,
    copied,
    load_sem,
    send_sem,
    back_sem,
    recv_sem,
    pair_sem,
    told_sem,
    detour,
    detour_send,
    detour_recv,
    raw,
    raw_low,
    raw_send,
    raw_recv,
):
    me, shift = lax.axis_index("shard"), lax.axis_index("shift")
    core = lax.axis_index("width")
    has_left, has_right = me > 0, me < n - 1
    left, right = {"shard": me - 1}, {"shard": me + 1}
    partner = {"width": 1 - core}
    helpers = range(1, 1 + detours(shifts))
    aside = len(helpers) * DETOUR_ROWS

    def on_early(*conditions):
        return functools.reduce(jnp.logical_and, conditions, core != LATE_CORE)

    helps = jnp.logical_and(shift >= 1, shift <= len(helpers))
    leads, ends = on_early(shift == 0, me == 1), on_early(shift == 0, me == 0)
    lifts, lands = on_early(helps, me == 1), on_early(helps, me == 0)
    held, low_refs, high_refs = copied[0:12:3], copied[1:12:3], copied[2:12:3]
    depth, width = held[0].shape
    first, rest = pl.ds(0, LANES), pl.ds(LANES, width - LANES)
    bands = [pl.ds(row, LANES) for row in range(0, depth, LANES)]
    loads = []

    def load(source, target):
        loads.append(pltpu.make_async_copy(source, target, load_sem.at[len(loads)]))
        return loads[-1]

    opening = [load(given[1], copied[1]), load(given[2].at[:, first], copied[2].at[:, first])]
    opening += [load(given[0].at[rows, first], held[0].at[rows, first]) for rows in bands]
    others = []
    if width > LANES:
        others = [load(given[i].at[:, rest], copied[i].at[:, rest]) for i in (2, 0)]
    rest_of = [others] + [
        [load(given[i], copied[i]) for i in range(array, array + 3)] for array in (3, 6, 9)
    ]
    norm_loads = [load(given[i], copied[i]) for i in (12, 13)]
    for one in (opening[2], *opening[:2], *opening[3:]):
        one.start()

    barrier = pltpu.get_barrier_semaphore()
    pl.semaphore_signal(barrier, inc=1, device_id=partner, device_id_type=MESH)

    @pl.when(has_right)
    def _():
        pl.semaphore_signal(barrier, inc=1, device_id=right, device_id_type=MESH)

    if aside:

        @pl.when(lifts)
        def _():
            line = {"shift": 0 * shift}
            pl.semaphore_signal(barrier, inc=1, device_id=line, device_id_type=MESH)

        @pl.when(ends)
        def _():
            for helper in helpers:
                line = {"shift": 0 * shift + helper}
                pl.semaphore_signal(barrier, inc=1, device_id=line, device_id_type=MESH)

    for one in loads[len(opening) :]:
        one.start()
    waited = 1 + has_left.astype(jnp.int32)
    if aside:
        waited += jnp.where(leads, len(helpers), 0) + lands.astype(jnp.int32)
    pl.semaphore_wait(barrier, waited)

    @pl.when(has_left)
    def _():
        pl.semaphore_signal(told_sem, inc=1, device_id=left, device_id_type=MESH)

    last = len(outs) - 1
    block = held[last].shape[1]
    tail = late_rows(block)
    groups = [(array, 0, w.shape[1]) for array, w in enumerate(held[:last])]
    groups.append((last, aside, block - tail - aside))
    if tail:
        groups.append((last, block - tail, tail))
    groups.append((len(outs), 0, 0))
    side_group = len(groups)
    if aside:
        groups.append((last, 0, aside))
    norm_group = len(outs) + (1 if tail else 0)
    late_group = norm_group - 1 if tail else -1

    def part(array, row, rows, origin, band=None):
        if array == len(outs):
            return norm_out.at[origin]
        out, w = outs[array], held[array]
        if array < last:
            first, size = band or (0, w.shape[0])
            begin = pl.multiple_of(origin * w.shape[0] + first, LANES)
            return out.at[pl.ds(pl.multiple_of(row, LANES), rows), pl.ds(begin, size)]
        begin = pl.multiple_of(origin * block + row, ROW_UNIT)
        return out.at[pl.ds(begin, rows)]

    def copy(ref, device, semaphore, origin, group):
        return pltpu.make_async_remote_copy(
            src_ref=ref,
            dst_ref=ref,
            send_sem=semaphore,
            recv_sem=recv_sem.at[origin, group],
            device_id=device,
            device_id_type=MESH,
        )

    short = short_rows(depth)
    corner = pl.ds(0, LANES)

    def raw_copies():
        pairs = ((held[0].at[corner, corner], raw), (low_refs[0].at[:, corner], raw_low))
        return [
            pltpu.make_async_remote_copy(
                src_ref=source,
                dst_ref=target,
                send_sem=raw_send.at[i],
                recv_sem=raw_recv.at[i],
                device_id=left,
                device_id_type=MESH,
            )
            for i, (source, target) in enumerate(pairs)
        ]

    def near_query():
        ref = part(0, 0, width - short, me)
        return copy(ref, left, back_sem.at[0], me + 1, 0)

    def forward(group, origin):
        ref = part(*groups[group], origin)
        return copy(ref, right, send_sem.at[origin, group], origin, group)

    def backward(group, origin, own=False):
        ref = part(*groups[group], origin)
        semaphore = back_sem.at[group] if own else send_sem.at[origin, group]
        return copy(ref, left, semaphore, origin, group)

    def compute(array, c):
        rows = pl.ds(pl.multiple_of(c * LANES, LANES), LANES)
        low_rank = lax.dot_general(
            high_refs[array][:, rows],
            low_refs[array][...],
            (((0,), (0,)), ((), ())),
            preferred_element_type=jnp.float32,
        )
        base = held[array][:, rows].T.astype(jnp.float32)
        part(array, c * LANES, LANES, me)[...] = (base + mix_rate * low_rank).astype(
            jnp.bfloat16
        )

    def send_left(ref, group):
        @pl.when(has_left)
        def _():
            copy(ref, left, back_sem.at[group], me, group).start()

    def send_right(ref, group):
        @pl.when(has_right)
        def _():
            copy(ref, right, send_sem.at[me, group], me, group).start()

    def send_both(ref, group):
        send_left(ref, group)
        send_right(ref, group)

    def hop(source, target, device, index, semaphore):
        return pltpu.make_async_remote_copy(
            src_ref=source,
            dst_ref=target,
            send_sem=detour_send.at[index],
            recv_sem=semaphore,
            device_id=device,
            device_id_type=MESH,
        )

    def lead(helper):
        source = part(last, (helper - 1) * DETOUR_ROWS, DETOUR_ROWS, me)
        line = {"shift": 0 * shift + helper}
        return hop(source, detour, line, helper - 1, detour_recv.at[0])

    def lift():
        return hop(detour, detour, left, 0, detour_recv.at[0])

    def land():
        target = part(last, (shift - 1) * DETOUR_ROWS, DETOUR_ROWS, me + 1)
        return hop(detour, target, {"shift": 0 * shift}, 0, recv_sem.at[1, side_group])

    def send_aside():
        ref = part(*groups[side_group], me)
        send_right(ref, side_group)

        @pl.when(jnp.logical_not(leads))
        def _():
            send_left(ref, side_group)

        @pl.when(leads)
        def _():
            for helper in helpers:
                lead(helper).start()

        @pl.when(lifts)
        def _():
            lift().wait_recv()
            lift().start()

    def open_right(rows):
        @pl.when(has_right)
        def _():
            pl.semaphore_wait(told_sem, 1)

        send_right(part(0, 0, rows, me), 0)

    def finish(array):
        if array == 0:
            rows = held[0].shape[1]
            if rows > LANES:
                send_left(part(0, rows - LANES, LANES, me), 0)
            if early:
                send_right(part(0, early, rows - early, me), 0)
            else:
                open_right(rows)
        else:
            send_both(part(*groups[array], me), array)

    opening[0].wait()
    opening[2].wait()
    if short:

        @pl.when(has_left)
        def _():
            for one in raw_copies():
                one.start()

    for one in opening[1:2] + opening[3:]:
        one.wait()
    compute(0, 0)
    send_left(part(0, 0, LANES, me, (LANES, depth - LANES) if short else None), 0)

    def exchange(side):
        return pltpu.make_async_remote_copy(
            src_ref=norm_out.at[me, side],
            dst_ref=norm_out.at[me, side],
            send_sem=pair_sem.at[0],
            recv_sem=pair_sem.at[1],
            device_id=partner,
            device_id_type=MESH,
        )

    early = (EARLY_PIECES - 1) * LANES if width > EARLY_PIECES * LANES else 0

    for array in range(len(outs)):
        for one in rest_of[array]:
            one.wait()
        count = held[array].shape[1] // LANES
        if array:
            compute(array, 0)
            finish(array - 1)
        if array == 1:
            for one in norm_loads:
                one.wait()
            norm_out[me, core] = copied[12][...] + copied[13][...]
        begin = 1
        if array == 0 and count > 1:
            compute(0, 1)
            begin = 2

        def step(c, carry, array=array):
            compute(array, c)
            if array == 0:
                send_left(part(0, (c - 1) * LANES, LANES, me), 0)
            return carry

        if array == 0 and early:
            lax.fori_loop(begin, EARLY_PIECES, step, 0)
            open_right(early)
            begin = EARLY_PIECES
        lax.fori_loop(begin, count, step, 0)
    exchange(core).start()
    if tail >= LANES:
        finish(last)
    exchange(core).wait_send()
    exchange(1 - core).wait_recv()
    if tail < LANES:
        finish(last)
    if tail:

        @pl.when(core != LATE_CORE)
        def _():
            send_both(part(*groups[late_group], me), late_group)

    send_both(part(*groups[norm_group], me), norm_group)
    if aside:
        send_aside()

    if short:

        @pl.when(has_right)
        def _():
            for one in raw_copies():
                one.wait_recv()
            low_rank = lax.dot_general(
                high_refs[0][:, corner],
                raw_low[...],
                (((0,), (0,)), ((), ())),
                preferred_element_type=jnp.float32,
            )
            base = raw[...].T.astype(jnp.float32)
            part(0, 0, LANES, me + 1, (0, LANES))[...] = (base + mix_rate * low_rank).astype(
                jnp.bfloat16
            )

    def each_group(act):
        for group in range(len(groups)):
            if group == late_group:

                @pl.when(core != LATE_CORE)
                def _(group=group):
                    act(group)
            else:
                act(group)

    def relay(k, carry):
        from_left, from_right = me - k, me + k

        def pass_on(group):
            @pl.when(from_left >= 0)
            def _():
                forward(group, from_left).wait_recv()

                @pl.when(has_right)
                def _():
                    forward(group, from_left).start()

            @pl.when(from_right < n)
            def _():
                if group == 0 and short:

                    @pl.when(k == 1)
                    def _():
                        near_query().wait_recv()

                    @pl.when(k > 1)
                    def _():
                        backward(group, from_right).wait_recv()
                else:
                    backward(group, from_right).wait_recv()

                @pl.when(has_left)
                def _():
                    backward(group, from_right).start()

        each_group(pass_on)
        if aside:

            @pl.when(jnp.logical_and(lands, k == 1))
            def _():
                lift().wait_recv()
                land().start()

        return carry

    lax.fori_loop(1, n, relay, 0)

    def own_sent(group):
        @pl.when(has_right)
        def _():
            forward(group, me).wait_send()

        goes_left = has_left
        if group == side_group:
            goes_left = jnp.logical_and(has_left, jnp.logical_not(leads))

        @pl.when(goes_left)
        def _():
            if group == 0 and short:
                near_query().wait_send()
            else:
                backward(group, me, own=True).wait_send()

    each_group(own_sent)
    if short:

        @pl.when(has_left)
        def _():
            for one in raw_copies():
                one.wait_send()
    if aside:

        @pl.when(leads)
        def _():
            for helper in helpers:
                lead(helper).wait_send()

        @pl.when(lifts)
        def _():
            lift().wait_send()

        @pl.when(jnp.logical_and(lands, n > 1))
        def _():
            land().wait_send()

    def drain(k, carry):
        def sent(group):
            @pl.when(jnp.logical_and(me - k >= 0, has_right))
            def _():
                forward(group, me - k).wait_send()

            @pl.when(jnp.logical_and(me + k < n, has_left))
            def _():
                backward(group, me + k).wait_send()

        each_group(sent)
        return carry

    lax.fori_loop(1, n, drain, 0)


def body(n, shifts, *refs):
    kernel(n, shifts, refs[:14], refs[14:18], refs[18], refs[19:33], *refs[33:])


def store(n, cores, *refs):
    gathered, norm_ref, outs, norm_out, flat, rounded, sem, mixed_sem, norm_sem = (
        refs[:4],
        refs[4],
        refs[5:9],
        *refs[9:],
    )
    me, core = lax.axis_index("shard"), lax.axis_index("width")
    copies = []
    for source, out in zip(gathered[:3], outs[:3]):
        for row in range(0, source.shape[0], COPY_ROWS):
            rows = pl.ds(row, min(COPY_ROWS, source.shape[0] - row))
            copies.append(
                pltpu.make_async_copy(source.at[rows], out.at[rows], sem.at[len(copies)])
            )

    block = gathered[3].shape[0] // n
    tail = late_rows(block)

    def mixed(origin, row, size, part):
        rows = pl.ds(origin * block + row, size)
        return pltpu.make_async_copy(
            gathered[3].at[rows], outs[3].at[rows], mixed_sem.at[origin, part]
        )

    copies += [mixed(origin, 0, block - tail, 0) for origin in range(n)]

    def each_last(act):
        for origin in range(n if tail else 0):

            @pl.when(jnp.logical_or(core != LATE_CORE, me == origin))
            def _(origin=origin):
                act(mixed(origin, block - tail, tail, 1))

    for copy in copies:
        copy.start()
    each_last(lambda copy: copy.start())
    rows = norm_ref.shape[2]
    for origin in range(n):
        for side in range(cores):
            flat[pl.ds((origin * cores + side) * rows, rows)] = norm_ref[origin, side]
    rounded[...] = flat[...].astype(norm_out.dtype)
    norm_copy = pltpu.make_async_copy(rounded, norm_out, norm_sem)
    norm_copy.start()
    for copy in copies:
        copy.wait()
    each_last(lambda copy: copy.wait())
    norm_copy.wait()


def late(n, mixed, after, out, send_sem, recv_sem, told_sem):
    me = lax.axis_index("shard")
    core = lax.axis_index("width")
    has_left, has_right = me > 0, me < n - 1
    left, right = {"shard": me - 1}, {"shard": me + 1}
    block = mixed.shape[0] // n
    tail = late_rows(block)
    size = tail // LATE_STEPS

    def copy(origin, begin, rows, step, device, semaphore, own):
        first = pl.multiple_of(me * block + block - tail + begin, 16)
        dst = out.at[origin, pl.ds(pl.multiple_of(begin, 16), rows)]
        return pltpu.make_async_remote_copy(
            src_ref=mixed.at[pl.ds(first, rows)] if own else dst,
            dst_ref=dst,
            send_sem=send_sem.at[semaphore],
            recv_sem=recv_sem.at[origin, step],
            device_id=device,
            device_id_type=MESH,
        )

    def forward(origin, step, own=False):
        return copy(origin, step * size, size, step, right, origin, own)

    def backward(origin, step, own=False):
        return copy(origin, step * size, size, step, left, n if own else origin, own)

    def sent(origin, semaphore):
        copy(origin, 0, tail, 0, right, semaphore, True).wait_send()

    @pl.when(core == LATE_CORE)
    def _():
        barrier = pltpu.get_barrier_semaphore()

        @pl.when(has_right)
        def _():
            pl.semaphore_signal(barrier, inc=1, device_id=right, device_id_type=MESH)

        @pl.when(has_left)
        def _():
            pl.semaphore_wait(barrier, 1)
            for step in range(LATE_STEPS):
                backward(me, step, own=True).start()
            pl.semaphore_signal(told_sem, inc=1, device_id=left, device_id_type=MESH)

        @pl.when(has_right)
        def _():
            pl.semaphore_wait(told_sem, 1)
            for step in range(LATE_STEPS):
                forward(me, step, own=True).start()

        def relay(k, carry):
            for step in range(LATE_STEPS):

                @pl.when(me - k >= 0)
                def _(step=step):
                    forward(me - k, step).wait_recv()

                    @pl.when(has_right)
                    def _():
                        forward(me - k, step).start()

                @pl.when(me + k < n)
                def _(step=step):
                    backward(me + k, step).wait_recv()

                    @pl.when(has_left)
                    def _():
                        backward(me + k, step).start()

            return carry

        lax.fori_loop(1, n, relay, 0)

        @pl.when(has_right)
        def _():
            sent(me, me)

        @pl.when(has_left)
        def _():
            sent(me, n)

        def drain(k, carry):
            @pl.when(jnp.logical_and(me - k >= 0, has_right))
            def _():
                sent(me - k, me - k)

            @pl.when(jnp.logical_and(me + k < n, has_left))
            def _():
                sent(me + k, me + k)

            return carry

        lax.fori_loop(1, n, drain, 0)


def store_late(n, pieces, given, out, sem):
    me, core = lax.axis_index("shard"), lax.axis_index("width")
    block = out.shape[0] // n
    tail = late_rows(block)

    def each(act):
        for origin in range(n):

            @pl.when(jnp.logical_and(core == LATE_CORE, me != origin))
            def _(origin=origin):
                act(origin)

    def begin(origin):
        for row in range(0, tail, STORE_ROWS):
            rows = pl.ds((origin + 1) * block - tail + row, STORE_ROWS)
            source = pieces.at[origin, pl.ds(row, STORE_ROWS)]
            pltpu.make_async_copy(source, out.at[rows], sem.at[origin]).start()

    def end(origin):
        rows = pl.ds((origin + 1) * block - tail, tail)
        pltpu.make_async_copy(pieces.at[origin], out.at[rows], sem.at[origin]).wait()

    each(begin)
    each(end)


def on_device(n, cores, shifts, *args):
    weights, (norm_train, norm_step) = list(args[:12]), args[12:]
    bases = weights[0::3]
    (size,) = norm_train.shape
    sizes = [size, *(size for w in bases for size in w.shape)]
    if cores != 2 or any(size % LANES for size in sizes):
        return plain(*args)
    rows = size // LANES
    shapes = [(w.shape[1], w.shape[0] * n) for w in bases[:3]]
    shapes.append((bases[3].shape[1] * n, bases[3].shape[0]))
    in_hbm = pl.BlockSpec(memory_space=pltpu.HBM)
    in_vmem = pl.BlockSpec(memory_space=pltpu.VMEM)
    tail = late_rows(bases[3].shape[1])
    helpers = detours(shifts)
    groups = len(bases) + (2 if tail else 1) + (1 if helpers else 0)
    weights[1::3] = [low.T for low in weights[1::3]]
    norms = [norm_train.reshape(rows, LANES), norm_step.reshape(rows, LANES)]
    given = [pltpu.with_memory_space_constraint(array, pltpu.HBM) for array in weights + norms]
    gathered = pl.pallas_call(
        functools.partial(body, n, shifts),
        out_shape=[pltpu.VMEM(shape, jnp.bfloat16) for shape in shapes]
        + [pltpu.VMEM((n, cores, rows, LANES), jnp.float32)],
        in_specs=[in_hbm] * 14,
        out_specs=[in_vmem] * 5,
        scratch_shapes=[pltpu.VMEM(array.shape, array.dtype) for array in given]
        + [
            pltpu.SemaphoreType.DMA((15 + bases[0].shape[0] // LANES,)),
            pltpu.SemaphoreType.DMA((n, groups)),
            pltpu.SemaphoreType.DMA((groups,)),
            pltpu.SemaphoreType.DMA((n, groups)),
            pltpu.SemaphoreType.DMA((2,)),
            pltpu.SemaphoreType.REGULAR,
            pltpu.VMEM((DETOUR_ROWS, shapes[3][1]), jnp.bfloat16),
            pltpu.SemaphoreType.DMA((max(helpers, 1),)),
            pltpu.SemaphoreType.DMA((1,)),
            pltpu.VMEM((LANES, LANES), jnp.bfloat16),
            pltpu.VMEM((given[1].shape[0], LANES), jnp.bfloat16),
            pltpu.SemaphoreType.DMA((2,)),
            pltpu.SemaphoreType.DMA((2,)),
        ],
        compiler_params=pltpu.CompilerParams(
            collective_id=0, has_side_effects=True, vmem_limit_bytes=40 * 2**20
        ),
        name="merge_gather",
    )(*given)
    norm_rows = n * cores * rows
    *finals, norm = pl.pallas_call(
        functools.partial(store, n, cores),
        out_shape=[jax.ShapeDtypeStruct(shape, jnp.bfloat16) for shape in shapes]
        + [jax.ShapeDtypeStruct((norm_rows, LANES), jnp.bfloat16)],
        in_specs=[in_vmem] * 5,
        out_specs=[in_hbm] * 5,
        scratch_shapes=[
            pltpu.VMEM((norm_rows, LANES), jnp.float32),
            pltpu.VMEM((norm_rows, LANES), jnp.bfloat16),
            pltpu.SemaphoreType.DMA((sum(-(-shape[0] // COPY_ROWS) for shape in shapes[:3]),)),
            pltpu.SemaphoreType.DMA((n, 2)),
            pltpu.SemaphoreType.DMA,
        ],
        compiler_params=pltpu.CompilerParams(vmem_limit_bytes=20 * 2**20),
        name="store",
    )(*gathered)
    norm = norm.reshape(-1)
    if not tail:
        return (*finals, norm)
    columns = shapes[3][1]
    pieces = pl.pallas_call(
        functools.partial(late, n),
        out_shape=pltpu.VMEM((n, tail, columns), jnp.bfloat16),
        in_specs=[in_vmem, in_hbm],
        out_specs=in_vmem,
        scratch_shapes=[
            pltpu.SemaphoreType.DMA((n + 1,)),
            pltpu.SemaphoreType.DMA((n, LATE_STEPS)),
            pltpu.SemaphoreType.REGULAR,
        ],
        compiler_params=pltpu.CompilerParams(
            collective_id=1, has_side_effects=True, vmem_limit_bytes=20 * 2**20
        ),
        name="late",
    )(gathered[3], pltpu.with_memory_space_constraint(finals[3], pltpu.HBM))
    finals[3] = pl.pallas_call(
        functools.partial(store_late, n),
        out_shape=jax.ShapeDtypeStruct(shapes[3], jnp.bfloat16),
        in_specs=[in_vmem, in_hbm],
        out_specs=in_hbm,
        input_output_aliases={1: 0},
        scratch_shapes=[pltpu.SemaphoreType.DMA((n,))],
        compiler_params=pltpu.CompilerParams(vmem_limit_bytes=20 * 2**20),
        name="store_late",
    )(pieces, finals[3])
    return (*finals, norm)


def solution(mesh):
    placed = (
        P(("shift", "shard"), "width"),
        P(("shift", "shard"), None),
        P("shift", "width"),
        P(("shift", "shard"), "width"),
        P(("shift", "shard"), None),
        P("shift", "width"),
        P(("shift", "shard"), "width"),
        P(("shift", "shard"), None),
        P("shift", "width"),
        P(("shift", "width"), "shard"),
        P(("shift", "width"), None),
        P("shift", "shard"),
        P(("shift", "shard", "width")),
        P(("shift", "shard", "width")),
    )
    return jax.shard_map(
        functools.partial(
            on_device, mesh.shape["shard"], mesh.shape["width"], mesh.shape["shift"]
        ),
        mesh=mesh,
        in_specs=placed,
        out_specs=(
            P(("shift", "width"), None),
            P(("shift", "width"), None),
            P(("shift", "width"), None),
            P("shift", "width"),
            P("shift"),
        ),
        check_vma=False,
    )
```
